32 devices in a mesh: ctx: 8 (over z, x), fsdp: 4 (over y, core).
Axes of the slice: x: 2, y: 2, z: 4, core: 2. Of those that a mesh axis runs over, the one named last changes fastest.
Arguments:
- layer_input: bfloat16 [4, 1024, 896], P('fsdp', 'ctx'), may hold values from -6 to 6
- seq_ids: int32 [4, 1024], P('fsdp', 'ctx'), may hold values from 0 to 1, as said below
- positions: int32 [4, 1024], P('fsdp', 'ctx'), may hold values from 0 to 895, as said below
- norm_gain: bfloat16 [896], P('fsdp'), may hold values from 0.5 to 1.5
- w_query: bfloat16 [896, 896], P('fsdp'), may hold values from -0.1875 to 0.1875
- b_query: bfloat16 [896], P('fsdp'), may hold values from -3 to 3
- w_key: bfloat16 [896, 128], P('fsdp'), may hold values from -0.1875 to 0.1875
- b_key: bfloat16 [128], P('fsdp'), may hold values from -3 to 3
- w_value: bfloat16 [896, 128], P('fsdp'), may hold values from -0.1875 to 0.1875
- b_value: bfloat16 [128], P('fsdp'), may hold values from -3 to 3
- w_output: bfloat16 [896, 896], P('fsdp'), may hold values from -2 to 2
- mlp_gain: bfloat16 [896], P('fsdp'), may hold values from 0.5 to 1.5
- w_gate: bfloat16 [896, 4864], P(None, 'fsdp'), may hold values from -0.1875 to 0.1875
- w_up: bfloat16 [896, 4864], P(None, 'fsdp'), may hold values from -0.1875 to 0.1875
- w_down: bfloat16 [4864, 896], P('fsdp'), may hold values from -0.078125 to 0.078125
- cotangent: bfloat16 [4, 1024, 896], P('fsdp', 'ctx'), may hold values from -6 to 6
Outputs:
- block_out: bfloat16 [4, 1024, 896], P('fsdp', 'ctx')
- input_grad: bfloat16 [4, 1024, 896], P('fsdp', 'ctx')
- norm_gain_grad: float32 [896], P('fsdp')
- w_query_grad: float32 [896, 896], P('fsdp')
- b_query_grad: float32 [896], P('fsdp')
- w_key_grad: float32 [896, 128], P('fsdp')
- b_key_grad: float32 [128], P('fsdp')
- w_value_grad: float32 [896, 128], P('fsdp')
- b_value_grad: float32 [128], P('fsdp')
- w_output_grad: float32 [896, 896], P('fsdp')
- mlp_gain_grad: float32 [896], P('fsdp')
- w_gate_grad: float32 [896, 4864], P(None, 'fsdp')
- w_up_grad: float32 [896, 4864], P(None, 'fsdp')
- w_down_grad: float32 [4864, 896], P('fsdp')
- lse: float32 [4, 14, 1024], P('fsdp', None, 'ctx')
The draws below stay inside these ranges and needn't reach their ends.
Inputs may be any that keep to these rules, and one draw needn't show every extreme that they name: Each row holds two documents: seq_ids is 0 on its first r positions and 1 on the rest, with 128 <= r <= 256; in the first row r = 128. positions count from 0 at the start of each document of the row.
All inputs are finite; a program needn't handle non-finite values.
Results may differ from the reference program's by a relative error of at most 0.035.
Values may be sent and summed in bfloat16 or wider, within the bound.
A program may use at most 256 MiB of HBM per device.

```python
import math
import jax
import jax.numpy as jnp
from jax import lax

D = 896
H = 14
KV = 2
HD = 64
FF = 4864
SEQ_LEN = 1024
SEQS = 4


def split_point(key):
    drawn = jax.random.randint(jax.random.fold_in(key, 11), (SEQS,), SEQ_LEN // 8, SEQ_LEN // 4 + 1)
    return drawn.at[0].set(SEQ_LEN // 8).astype(jnp.int32)


def draw_seq_ids(key, part):
    boundary = split_point(key)
    offsets = jnp.arange(SEQ_LEN, dtype=jnp.int32)
    return (offsets[None, :] >= boundary[:, None]).astype(jnp.int32)


def draw_positions(key, part):
    boundary = split_point(key)
    offsets = jnp.arange(SEQ_LEN, dtype=jnp.int32)
    later = offsets[None, :] >= boundary[:, None]
    return jnp.where(later, offsets[None, :] - boundary[:, None], offsets[None, :]).astype(jnp.int32)


def level_of(key, extent, shards, low, top_value):
    loudness, own = 1.0, jax.random.fold_in(key, 6)
    for axis_at, shards_of in shards:
        heights = jnp.exp(jax.random.uniform(jax.random.fold_in(own, axis_at), (shards_of,), jnp.float32, low / len(shards), top_value / len(shards)))
        loudness = loudness * jnp.repeat(heights, extent[axis_at] // shards_of).reshape([-1 if axis == axis_at else 1 for axis in range(len(extent))])
    return loudness


def scatter_about(own_key, extent, deviation, most, shards=(), held_as=jnp.bfloat16):
    values = jax.random.normal(own_key, extent, jnp.float32) * deviation
    if len(shards) > 0:
        values = level_of(own_key, extent, shards, -0.22, 0.18) * values
    return jnp.clip(values, min=-most, max=most).astype(held_as)


def setup_inputs(seed: int = 0) -> dict:
    arg_keys = jax.random.split(jax.random.key(seed), 17)
    layer_input = scatter_about(arg_keys[0], (SEQS, SEQ_LEN, D), 1.0, 6.0, ((0, 4), (1, 8)))
    seq_ids = draw_seq_ids(jax.random.fold_in(arg_keys[16], 71), 0)
    positions = draw_positions(jax.random.fold_in(arg_keys[16], 71), 0)
    norm_gain = jnp.clip(1.0 + 0.1 * jax.random.normal(arg_keys[3], (D,), jnp.float32), 0.5, 1.5).astype(jnp.bfloat16)
    w_query = scatter_about(arg_keys[4], (D, H * HD), D ** -0.5, 0.1875, ((0, 4),))
    b_query = scatter_about(arg_keys[5], (H * HD,), 0.5, 3.0, ((0, 4),))
    w_key = scatter_about(arg_keys[6], (D, KV * HD), D ** -0.5, 0.1875, ((0, 4),))
    b_key = scatter_about(arg_keys[7], (KV * HD,), 0.5, 3.0, ((0, 4),))
    w_value = scatter_about(arg_keys[8], (D, KV * HD), D ** -0.5, 0.1875, ((0, 4),))
    b_value = scatter_about(arg_keys[9], (KV * HD,), 0.5, 3.0, ((0, 4),))
    w_output = scatter_about(arg_keys[10], (H * HD, D), (max(1, H * HD // 128)) ** -0.5, 2.0, ((0, 4),))
    mlp_gain = jnp.clip(1.0 + 0.1 * jax.random.normal(arg_keys[11], (D,), jnp.float32), 0.5, 1.5).astype(jnp.bfloat16)
    w_gate = scatter_about(arg_keys[12], (D, FF), D ** -0.5, 0.1875, ((1, 4),))
    w_up = scatter_about(arg_keys[13], (D, FF), D ** -0.5, 0.1875, ((1, 4),))
    w_down = scatter_about(arg_keys[14], (FF, D), FF ** -0.5, 0.078125, ((0, 4),))
    cotangent = scatter_about(arg_keys[15], (SEQS, SEQ_LEN, D), 1.0, 6.0, ((0, 4), (1, 8)))
    return dict(layer_input=layer_input, seq_ids=seq_ids, positions=positions, norm_gain=norm_gain, w_query=w_query, b_query=b_query, w_key=w_key, b_key=b_key, w_value=w_value, b_value=b_value, w_output=w_output, mlp_gain=mlp_gain, w_gate=w_gate, w_up=w_up, w_down=w_down, cotangent=cotangent)


EPSILON = 1e-06
ROPE_BASE = 1000000.0
MASK_FILL = -1e+30
HIGHEST = lax.Precision.HIGHEST

@jax.custom_vjp
def low(v):
    return lax.optimization_barrier(v.astype(jnp.bfloat16)).astype(jnp.float32)

@jax.custom_vjp
def low_back(v):
    return v

def low_keep(v):
    return (low(v), None)

def low_pass(kept, grad):
    return (grad,)

def back_keep(v):
    return (v, None)

def back_low(kept, grad):
    return (low(grad),)
low.defvjp(low_keep, low_pass)
low_back.defvjp(back_keep, back_low)

def matmul_hi(left, right):
    return jnp.dot(left, right, precision=HIGHEST, preferred_element_type=jnp.float32)

def rms_norm(values, gain):
    inverse = lax.rsqrt(lax.optimization_barrier(jnp.mean(values * values, -1, keepdims=True)) + EPSILON)
    return values * inverse * gain

def rope_tables(positions, head_dim):
    half = head_dim // 2
    freq = ROPE_BASE ** (-(jnp.arange(half, dtype=jnp.float32) * 2.0 / head_dim))
    angle = positions.astype(jnp.float32)[:, None] * freq[None, :]
    return (jnp.cos(angle)[:, None, :], jnp.sin(angle)[:, None, :])

def rotate(values, cosine, sine_table):
    half = values.shape[-1] // 2
    leading, trailing = (values[..., :half], values[..., half:])
    return jnp.concatenate([leading * cosine - trailing * sine_table, trailing * cosine + leading * sine_table], -1)

def attend(query, keys, values, segments):
    length = SEQ_LEN
    block_rows = math.gcd(length, 512)
    blocks = length // block_rows
    key_index = jnp.arange(length, dtype=jnp.int32)
    score_scale = HD ** (-0.5)

    def one_block(block_id):
        begin = (block_id * block_rows).astype(jnp.int32)
        query_block = lax.dynamic_slice_in_dim(query, begin, block_rows, 0)
        query_segs = lax.dynamic_slice_in_dim(segments, begin, block_rows, 0)
        query_rows = begin + jnp.arange(block_rows, dtype=jnp.int32)
        scores = low_back(jnp.einsum('tkgd,nkd->kgtn', query_block, keys, precision=HIGHEST) * score_scale)
        allowed = (key_index[None, :] <= query_rows[:, None]) & (segments[None, :] == query_segs[:, None])
        scores = jnp.where(allowed, scores, MASK_FILL)
        highest = lax.optimization_barrier(jnp.max(scores, -1, keepdims=True))
        expos = jnp.exp(scores - highest)
        totals = lax.optimization_barrier(jnp.sum(expos, -1, keepdims=True))
        probs = low(expos / totals)
        result = jnp.einsum('kgtn,nkd->tkgd', probs, values, precision=HIGHEST)
        return (result, (highest + jnp.log(totals))[..., 0])
    results, log_totals = lax.map(jax.checkpoint(one_block), jnp.arange(blocks, dtype=jnp.int32))
    results = results.reshape(length, H * HD)
    log_totals = jnp.transpose(log_totals, (1, 2, 0, 3)).reshape(H, length)
    return (results, log_totals)

def block_layer(tokens, segments, positions, params):
    norm_gain, w_query, b_query, w_key, b_key, w_value, b_value, w_output, mlp_gain, w_gate, w_up, w_down = params
    length = SEQ_LEN
    normed1 = low(rms_norm(tokens, norm_gain))
    q_pre = low_back(matmul_hi(normed1, w_query) + b_query)
    k_pre = low_back(matmul_hi(normed1, w_key) + b_key)
    v_pre = low_back(matmul_hi(normed1, w_value) + b_value)
    cosine, sine_table = rope_tables(positions, HD)
    query = low(rotate(q_pre.reshape(length, H, HD), cosine, sine_table)).reshape(length, KV, H // KV, HD)
    keys = low(rotate(k_pre.reshape(length, KV, HD), cosine, sine_table))
    values = low(v_pre.reshape(length, KV, HD))
    attention, log_totals = attend(query, keys, values, segments)
    attention = low(low_back(attention))
    hidden = tokens + low_back(matmul_hi(attention, w_output))
    normed2 = low(rms_norm(hidden, mlp_gain))
    gate = low_back(matmul_hi(normed2, w_gate))
    up_act = low_back(matmul_hi(normed2, w_up))
    act = low(jax.nn.silu(gate) * up_act)
    return (hidden + low_back(matmul_hi(act, w_down)), log_totals)

def reference(layer_input, seq_ids, positions, norm_gain, w_query, b_query, w_key, b_key, w_value, b_value, w_output, mlp_gain, w_gate, w_up, w_down, cotangent):
    params = tuple((param.astype(jnp.float32) for param in (norm_gain, w_query, b_query, w_key, b_key, w_value, b_value, w_output, mlp_gain, w_gate, w_up, w_down)))
    inputs = layer_input.astype(jnp.float32)
    layer_saved = jax.checkpoint(block_layer)

    def forward(inputs, params):

        def one_seq(state_now, items):
            out_seq, total_seq = layer_saved(items[0], items[1], items[2], params)
            return (state_now, (out_seq, total_seq))
        unused, (outputs, totals) = lax.scan(one_seq, jnp.zeros((), jnp.float32), (inputs, seq_ids, positions))
        return (outputs, totals)
    outputs, pullback, totals = jax.vjp(forward, inputs, params, has_aux=True)
    grad_in, grads = pullback(cotangent.astype(jnp.float32))
    return (outputs.astype(jnp.bfloat16), grad_in.astype(jnp.bfloat16), grads[0], grads[1], grads[2], grads[3], grads[4], grads[5], grads[6], grads[7], grads[8], grads[9], grads[10], grads[11], totals)
```

```python
import functools
import math

import jax
import jax.numpy as jnp
from jax import lax
from jax.experimental import pallas as pl
from jax.experimental.pallas import tpu as pltpu
from jax.sharding import PartitionSpec as P

H = 14
KV = 2
HD = 64


EPSILON = 1e-06
ROPE_BASE = 1000000.0
MASK_FILL = -1e30
MESH = pl.DeviceIdType.MESH
VMEM = pl.BlockSpec(memory_space=pltpu.VMEM)
f32 = jnp.float32
bf16 = jnp.bfloat16


def rope_tables(positions, head_dim):
    half = head_dim // 2
    freq = ROPE_BASE ** (-(jnp.arange(half, dtype=jnp.float32) * 2.0 / head_dim))
    angle = positions.astype(jnp.float32)[:, None] * freq[None, :]
    return (jnp.cos(angle)[:, None, :], jnp.sin(angle)[:, None, :])


def rotate(values, cosine, sine_table):
    half = values.shape[-1] // 2
    leading, trailing = (values[..., :half], values[..., half:])
    return jnp.concatenate(
        [leading * cosine - trailing * sine_table, trailing * cosine + leading * sine_table], -1
    )


def rotate_back(grads, cosine, sine_table):
    half = grads.shape[-1] // 2
    leading, trailing = (grads[..., :half], grads[..., half:])
    return jnp.concatenate(
        [leading * cosine + trailing * sine_table, trailing * cosine - leading * sine_table], -1
    )


def norm_back(values, inverse, gain, grads):
    scaled = values * inverse
    weighted = grads * gain
    grad_values = inverse * (weighted - scaled * jnp.mean(weighted * scaled, -1, keepdims=True))
    return (grad_values, jnp.sum(grads * scaled, 0))


def remote(src, dst, send_sem, recv_sem, device):
    return pltpu.make_async_remote_copy(
        src_ref=src, dst_ref=dst, send_sem=send_sem, recv_sem=recv_sem, device_id=device,
        device_id_type=MESH,
    )


def where_am_i():
    c, f = lax.axis_index("ctx"), lax.axis_index("fsdp")
    c2 = c + 1 - 2 * (c % 2)
    m = f + 1 - 2 * (f % 2)
    n = (f + 2) % 4
    return c, f, c2, m, n


def greet(devices):
    barrier = pltpu.get_barrier_semaphore()
    for device in devices:
        pl.semaphore_signal(barrier, inc=1, device_id=device, device_id_type=MESH)
    pl.semaphore_wait(barrier, len(devices))


def gather_start(items, ss, rs, place):
    c, f, c2, m, n = place
    h = c % 2
    for i, (src, dst) in enumerate(items):
        half = src.shape[0] // 2
        rows = pl.ds(h * half, half)
        remote(src.at[rows], dst(f).at[rows], ss.at[i, 1], rs.at[i, 1], (c, n)).start()
    for i, (src, dst) in enumerate(items):
        remote(src, dst(f), ss.at[i, 0], rs.at[i, 0], (c, m)).start()
        dst(f)[...] = src[...]


def gather_finish(items, ss, rs, place):
    c, f, c2, m, n = place
    h = c % 2
    far = (m + 2) % 4
    for i, (src, dst) in enumerate(items):
        half = src.shape[0] // 2
        mine = dst(n).at[pl.ds(h * half, half)]
        remote(mine, mine, ss.at[i, 1], rs.at[i, 1], (c, n)).wait_recv()
        remote(mine, mine, ss.at[i, 2], rs.at[i, 2], (c2, f)).start()
        remote(mine, mine, ss.at[i, 3], rs.at[i, 3], (c, m)).start()
    for i, (src, dst) in enumerate(items):
        half = src.shape[0] // 2
        other = dst(n).at[pl.ds((1 - h) * half, half)]
        remote(other, other, ss.at[i, 2], rs.at[i, 2], (c2, f)).wait_recv()
        remote(other, other, ss.at[i, 4], rs.at[i, 4], (c, m)).start()
    for i, (src, dst) in enumerate(items):
        half = src.shape[0] // 2
        mine, other = pl.ds(h * half, half), pl.ds((1 - h) * half, half)
        remote(src, dst(m), ss.at[i, 0], rs.at[i, 0], (c, m)).wait()
        remote(src.at[mine], dst(f).at[mine], ss.at[i, 1], rs.at[i, 1], (c, n)).wait_send()
        remote(src.at[mine], dst(n).at[mine], ss.at[i, 2], rs.at[i, 2], (c2, f)).wait_send()
        remote(src.at[mine], dst(far).at[mine], ss.at[i, 3], rs.at[i, 3], (c, m)).wait()
        remote(src.at[other], dst(far).at[other], ss.at[i, 4], rs.at[i, 4], (c, m)).wait()


def tokens_start(items, ss, rs, place):
    c, f, c2, m, n = place
    for i, (src, dst) in enumerate(items):
        half = src.shape[0] // 2
        for j in range(2):
            rows = pl.ds(j * half, half)
            remote(src.at[rows], dst(f, rows), ss.at[i, 1 + j], rs.at[i, 1 + j], (c, n)).start()
    for i, (src, dst) in enumerate(items):
        rows = pl.ds(0, src.shape[0])
        remote(src, dst(f, rows), ss.at[i, 0], rs.at[i, 0], (c, m)).start()
        dst(f, rows)[...] = src[...]


def tokens_finish(items, ss, rs, place):
    c, f, c2, m, n = place
    far = (m + 2) % 4
    for i, (src, dst) in enumerate(items):
        half = src.shape[0] // 2
        for j in range(2):
            here = dst(n, pl.ds(j * half, half))
            remote(here, here, ss.at[i, 1 + j], rs.at[i, 1 + j], (c, n)).wait_recv()
            remote(here, here, ss.at[i, 3 + j], rs.at[i, 3 + j], (c, m)).start()
    for i, (src, dst) in enumerate(items):
        half = src.shape[0] // 2
        remote(src, dst(m, pl.ds(0, src.shape[0])), ss.at[i, 0], rs.at[i, 0], (c, m)).wait()
        for j in range(2):
            rows = pl.ds(j * half, half)
            remote(src.at[rows], dst(f, rows), ss.at[i, 1 + j], rs.at[i, 1 + j], (c, n)).wait_send()
            remote(src.at[rows], dst(far, rows), ss.at[i, 3 + j], rs.at[i, 3 + j], (c, m)).wait()


def gather_sems(count):
    return [pltpu.SemaphoreType.DMA((count, 5)), pltpu.SemaphoreType.DMA((count, 5))]


def comm_call(body, out_shape, scratch, ident, name):
    def call(*args):
        return pl.pallas_call(
            body,
            out_shape=out_shape,
            in_specs=[VMEM] * len(args),
            out_specs=jax.tree.map(lambda _: VMEM, out_shape),
            scratch_shapes=scratch,
            compiler_params=pltpu.CompilerParams(
                collective_id=ident, has_side_effects=True, vmem_limit_bytes=48 << 20
            ),
            name=name,
        )(*args)

    return call


def front_body(
    ctx, depth, wq, wk, wv, wo, small, seg, wp_o, wo_o, small_o, seg_o, ss, rs, small_ss, small_rs, seg_ss, seg_rs
):
    place = where_am_i()
    c, f, c2, m, n = place
    far = (m + 2) % 4
    peers = [lax.rem(c + k, ctx) for k in range(1, ctx)]
    greet([(p, f) for p in peers] + [(c, m), (c, n), (c, far)])
    width = wq.shape[1]
    narrow = wk.shape[1]

    def rows(g):
        return pl.ds(pl.multiple_of(g * depth, 16), depth)

    items = [
        (wq, lambda g: wp_o.at[rows(g), pl.ds(0, width)]),
        (wk, lambda g: wp_o.at[rows(g), pl.ds(width, narrow)]),
        (wv, lambda g: wp_o.at[rows(g), pl.ds(width + narrow, narrow)]),
        (wo, lambda g: wo_o.at[rows(g)]),
    ]
    copies = [
        remote(small, small_o.at[f], small_ss.at[k], small_rs.at[k], (c, g)) for k, g in enumerate((m, n, far))
    ]
    for copy in copies:
        copy.start()
    for k, p in enumerate(peers):
        remote(seg, seg_o.at[c], seg_ss.at[k], seg_rs.at[k], (p, f)).start()
    gather_start(items, ss, rs, place)
    small_o[f] = small[...]
    seg_o[c] = seg[...]
    gather_finish(items, ss, rs, place)
    for k, g in enumerate((m, n, far)):
        remote(small, small_o.at[g], small_ss.at[k], small_rs.at[k], (c, g)).wait()
    for k, p in enumerate(peers):
        giver = lax.rem(c + ctx - 1 - k, ctx)
        remote(seg, seg_o.at[giver], seg_ss.at[k], seg_rs.at[k], (p, f)).wait()


def spread_start(src, dst, ss, rs, place, lines):
    c, f, c2, m, n = place
    for k in range(1, lines):
        p = lax.rem(c // 2 + k, lines) * 2 + c % 2
        remote(src, dst.at[c], ss.at[0, k], rs.at[0, k], (p, f)).start()
    remote(src, dst.at[c], ss.at[1, 0], rs.at[1, 0], (c2, f)).start()


def spread_finish(src, dst, ss, rs, place, lines):
    c, f, c2, m, n = place
    for k in range(1, lines):
        giver = lax.rem(c // 2 + lines - k, lines) * 2 + c % 2
        block = dst.at[giver]
        remote(block, block, ss.at[0, k], rs.at[0, k], (c2, f)).wait_recv()
        remote(block, block, ss.at[1, k], rs.at[1, k], (c2, f)).start()
    for k in range(lines):
        giver = lax.rem(c2 // 2 + lines - k, lines) * 2 + c2 % 2
        remote(src, dst.at[giver], ss.at[1, k], rs.at[1, k], (c2, f)).wait()
        if k:
            remote(src, dst.at[c], ss.at[0, k], rs.at[0, k], (c2, f)).wait_send()


def line_devices(place, lines):
    c, f, c2, m, n = place
    return [(lax.rem(c // 2 + k, lines) * 2 + c % 2, f) for k in range(1, lines)] + [(c2, f)]


def kv_body(lines, kv, kv_o, ss, rs):
    place = where_am_i()
    greet(line_devices(place, lines))
    spread_start(kv, kv_o, ss, rs, place, lines)
    kv_o[place[0]] = kv[...]
    spread_finish(kv, kv_o, ss, rs, place, lines)


def ag_body(x, x_o, ss, rs):
    place = where_am_i()
    c, f, c2, m, n = place
    greet([(c, m), (c, n)])
    items = [(x, lambda g, rows: x_o.at[g, rows])]
    tokens_start(items, ss, rs, place)
    tokens_finish(items, ss, rs, place)


def rs_body(part, out, near, sums, far_in, ss, rs):
    c, f, c2, m, n = where_am_i()
    far = (m + 2) % 4
    greet([(c, m), (c, n)])
    first = remote(part.at[far], near.at[0], ss.at[0], rs.at[0], (c, m))
    second = remote(part.at[m], near.at[1], ss.at[1], rs.at[1], (c, m))
    first.start()
    second.start()
    first.wait()
    sums[...] = (part[n].astype(f32) + near[0].astype(f32)).astype(bf16)
    across = remote(sums, far_in, ss.at[2], rs.at[2], (c, n))
    across.start()
    second.wait()
    mine = part[f].astype(f32) + near[1].astype(f32)
    across.wait()
    out[...] = mine + far_in[...].astype(f32)


def dkv_body(ctx, part, ghl, sl, out, ghl_o, sl_o, held, ss, rs, gs, gr, as_, ar):
    place = where_am_i()
    c, f, c2, m, n = place
    far = (m + 2) % 4
    peers = [lax.rem(c + k, ctx) for k in range(1, ctx)]
    greet([(p, f) for p in peers] + [(c, m), (c, n), (c, far)])
    for k, p in enumerate(peers):
        remote(part.at[p], held.at[k], ss.at[k], rs.at[k], (p, f)).start()
    for k, g in enumerate((n, far, m)):
        remote(sl.at[g], sl_o.at[f], as_.at[k], ar.at[k], (c, g)).start()
    items = [(ghl, lambda g, rows: ghl_o.at[g, rows])]
    tokens_start(items, gs, gr, place)
    sl_o[f] = sl[f]
    total = part[c].astype(f32)
    tokens_finish(items, gs, gr, place)
    for k, p in enumerate(peers):
        remote(part.at[p], held.at[k], ss.at[k], rs.at[k], (p, f)).wait()
        total = total + held[k].astype(f32)
    for k, g in enumerate((n, far, m)):
        remote(sl.at[g], sl_o.at[g], as_.at[k], ar.at[k], (c, g)).wait()
    out[...] = total


def shards(
    layer_input,
    seq_ids,
    positions,
    norm_gain,
    w_query,
    b_query,
    w_key,
    b_key,
    w_value,
    b_value,
    w_output,
    mlp_gain,
    w_gate,
    w_up,
    w_down,
    cotangent,
):
    tok = layer_input.shape[1]
    width = layer_input.shape[2]
    group = H // KV
    query_width = H * HD
    key_width = KV * HD
    score_scale = HD ** (-0.5)
    ctx = lax.axis_size("ctx")
    fsdp = lax.axis_size("fsdp")
    depth = width // fsdp
    lines = ctx // 2
    c, f = lax.axis_index("ctx"), lax.axis_index("fsdp")
    seq_length = ctx * tok
    dma = pltpu.SemaphoreType.DMA
    sds = jax.ShapeDtypeStruct
    input_rows = layer_input[0]
    grad_out = cotangent[0]
    own_segment = seq_ids[0]
    own_positions = positions[0]
    query_rows = c * tok + jnp.arange(tok, dtype=jnp.int32)

    cot_all = lax.all_gather(grad_out, ("ctx", "fsdp"), axis=0, tiled=True)

    def padded(v):
        return jnp.pad(v, (0, 256 - v.shape[0]))

    small = jnp.stack([padded(v) for v in (norm_gain, mlp_gain, b_query, b_key, b_value)])
    small = jnp.pad(small, ((0, 11), (0, 0)))
    seg_tile = jnp.broadcast_to(own_segment[None], (8, tok))
    w_project, wo_full, small_all, seg_all = comm_call(
        functools.partial(front_body, ctx, depth),
        (
            sds((width, query_width + 2 * key_width), bf16),
            sds((query_width, width), bf16),
            sds((fsdp, 16, 256), bf16),
            sds((ctx, 8, tok), jnp.int32),
        ),
        gather_sems(4) + [dma((3,)), dma((3,)), dma((ctx - 1,)), dma((ctx - 1,))],
        0,
        "front",
    )(w_query, w_key, w_value, w_output, small, seg_tile)
    all_segments = seg_all[:, 0].reshape(seq_length)
    small_all = small_all.astype(f32)
    gain_first = small_all[:, 0, :depth].reshape(width)
    gain_second = small_all[:, 1, :depth].reshape(width)
    kd = key_width // fsdp
    b_project = jnp.concatenate(
        [
            small_all[:, 2, :depth].reshape(query_width),
            small_all[:, 3, :kd].reshape(key_width),
            small_all[:, 4, :kd].reshape(key_width),
        ]
    )
    residual_in = input_rows.astype(f32)
    inverse_first = lax.rsqrt(jnp.mean(residual_in * residual_in, -1, keepdims=True) + EPSILON)
    normed_first = (residual_in * inverse_first * gain_first).astype(bf16)
    projected = jnp.dot(normed_first, w_project, preferred_element_type=f32) + b_project
    cosine, sine_table = rope_tables(own_positions, HD)
    query = rotate(projected[:, :query_width].reshape(tok, H, HD), cosine, sine_table)
    query = query.astype(bf16).reshape(tok, KV, group, HD)
    key_rot = rotate(
        projected[:, query_width : query_width + key_width].reshape(tok, KV, HD), cosine, sine_table
    )
    value_low = projected[:, query_width + key_width :].astype(bf16)
    key_value = jnp.concatenate([key_rot.astype(bf16).reshape(tok, key_width), value_low], 1)
    kv_all = comm_call(
        functools.partial(kv_body, lines),
        sds((ctx, tok, 2 * key_width), bf16),
        [dma((2, lines)), dma((2, lines))],
        1,
        "kv_gather",
    )(key_value).reshape(seq_length, 2 * key_width)
    keys = kv_all[:, :key_width].reshape(seq_length, KV, HD)
    values = kv_all[:, key_width:].reshape(seq_length, KV, HD)
    key_rows = jnp.arange(seq_length, dtype=jnp.int32)
    allowed = (key_rows[None, :] <= query_rows[:, None]) & (all_segments[None, :] == own_segment[:, None])
    raw_scores = jnp.einsum("tkgd,nkd->kgtn", query, keys, preferred_element_type=f32) * score_scale
    highest = jnp.max(jnp.where(allowed, raw_scores, MASK_FILL), -1)
    exp_scores = jnp.where(allowed, jnp.exp(raw_scores - highest[..., None]), 0.0)
    running_sum = jnp.sum(exp_scores, -1)
    accumulated = jnp.einsum("kgtn,nkd->tkgd", exp_scores.astype(bf16), values, preferred_element_type=f32)
    log_total = highest + jnp.log(running_sum)
    attention = accumulated / jnp.transpose(running_sum, (2, 0, 1))[..., None]
    attention_low = attention.reshape(tok, query_width).astype(bf16)
    hidden_state = residual_in + jnp.dot(attention_low, wo_full, preferred_element_type=f32)
    inverse_second = lax.rsqrt(jnp.mean(hidden_state * hidden_state, -1, keepdims=True) + EPSILON)
    normed_second = (hidden_state * inverse_second * gain_second).astype(bf16)
    x_all = lax.all_gather(normed_second, ("ctx", "fsdp"), axis=0, tiled=True)
    x_group = comm_call(
        ag_body, sds((fsdp, tok, width), bf16), gather_sems(1), 2, "normed_gather"
    )(normed_second).reshape(fsdp * tok, width)
    cot_group = lax.dynamic_slice_in_dim(cot_all, c * fsdp * tok, fsdp * tok, 0)

    def ffn(x, cot):
        gate = jnp.dot(x, w_gate, preferred_element_type=f32)
        up = jnp.dot(x, w_up, preferred_element_type=f32)
        g_act = lax.dot_general(cot, w_down, (((1,), (1,)), ((), ())), preferred_element_type=f32)
        sg = jax.nn.sigmoid(gate)
        act = (gate * sg * up).astype(bf16)
        g_gate = (g_act * up * sg * (1.0 + gate * (1.0 - sg))).astype(bf16)
        g_up = (g_act * gate * sg).astype(bf16)
        return act, g_gate, g_up

    def over_last(a, b):
        return lax.dot_general(a, b, (((1,), (1,)), ((), ())), preferred_element_type=f32)

    def over_first(a, b):
        return lax.dot_general(a, b, (((0,), (0,)), ((), ())), preferred_element_type=f32)

    act, g_gate, g_up = ffn(x_group, cot_group)
    g_normed_part = (over_last(g_gate, w_gate) + over_last(g_up, w_up)).astype(bf16)
    grad_normed2 = comm_call(
        rs_body,
        sds((tok, width), f32),
        [
            pltpu.VMEM((2, tok, width), bf16),
            pltpu.VMEM((tok, width), bf16),
            pltpu.VMEM((tok, width), bf16),
            dma((3,)),
            dma((3,)),
        ],
        3,
        "normed_scatter",
    )(g_normed_part.reshape(fsdp, tok, width))
    down_part = jnp.dot(act, w_down, preferred_element_type=f32).astype(bf16)
    down_out = lax.psum_scatter(down_part, "fsdp", scatter_dimension=0, tiled=True).astype(f32)
    block_out = (hidden_state + down_out).astype(bf16)[None]

    hidden_back, second_gain_grad = norm_back(hidden_state, inverse_second, gain_second, grad_normed2)
    grad_hidden = grad_out.astype(f32) + hidden_back
    grad_hidden_low = grad_hidden.astype(bf16)
    grad_attention = over_last(grad_hidden_low, wo_full).astype(bf16)
    grad_attention = grad_attention.reshape(tok, KV, group, HD)
    delta_rows = jnp.einsum("tkgd,tkgd->kgt", grad_attention.astype(f32), attention)
    probs = jnp.where(allowed, jnp.exp(raw_scores - log_total[..., None]), 0.0)
    grad_values = jnp.einsum("kgtn,tkgd->nkd", probs.astype(bf16), grad_attention, preferred_element_type=f32)
    grad_probs = jnp.einsum("tkgd,nkd->kgtn", grad_attention, values, preferred_element_type=f32)
    grad_scores = (probs * (grad_probs - delta_rows[..., None])).astype(bf16)
    grad_query = jnp.einsum("kgtn,nkd->tkgd", grad_scores, keys, preferred_element_type=f32) * score_scale
    grad_keys = jnp.einsum("kgtn,tkgd->nkd", grad_scores, query, preferred_element_type=f32) * score_scale
    grad_pairs = jnp.concatenate(
        [grad_keys.reshape(seq_length, key_width), grad_values.reshape(seq_length, key_width)], 1
    ).astype(bf16)
    slices = jnp.concatenate(
        [
            normed_first.reshape(tok, fsdp, depth).transpose(1, 0, 2),
            attention_low.reshape(tok, fsdp, depth).transpose(1, 0, 2),
        ],
        1,
    )
    grad_pairs, ghl_group, slice_group = comm_call(
        functools.partial(dkv_body, ctx),
        (
            sds((tok, 2 * key_width), f32),
            sds((fsdp, tok, width), bf16),
            sds((fsdp, 2 * tok, depth), bf16),
        ),
        [pltpu.VMEM((ctx - 1, tok, 2 * key_width), bf16), dma((ctx - 1,)), dma((ctx - 1,))]
        + gather_sems(1)
        + [dma((3,)), dma((3,))],
        4,
        "dkv_scatter",
    )(grad_pairs.reshape(ctx, tok, 2 * key_width), grad_hidden_low, slices)
    grad_q_pre = (
        rotate_back(grad_query.reshape(tok, H, HD), cosine, sine_table).reshape(tok, query_width).astype(bf16)
    )
    grad_k_pre = (
        rotate_back(grad_pairs[:, :key_width].reshape(tok, KV, HD), cosine, sine_table)
        .reshape(tok, key_width)
        .astype(bf16)
    )
    grad_v_pre = grad_pairs[:, key_width:].astype(bf16)
    grad_project = jnp.concatenate([grad_q_pre, grad_k_pre, grad_v_pre], 1)
    gp_group = comm_call(
        ag_body, sds((fsdp, tok, grad_project.shape[1]), bf16), gather_sems(1), 5, "project_gather"
    )(grad_project).reshape(fsdp * tok, grad_project.shape[1])
    normed_slice = slice_group[:, :tok].reshape(fsdp * tok, depth)
    attention_slice = slice_group[:, tok:].reshape(fsdp * tok, depth)
    project_grad = over_first(normed_slice, gp_group)
    output_grad = over_first(attention_slice, ghl_group.reshape(fsdp * tok, width))
    weight_grads = jnp.concatenate([project_grad, output_grad], 1).astype(bf16)
    x_all, cot_all, weight_grads = lax.optimization_barrier((x_all, cot_all, weight_grads))
    weight_grads = lax.psum(weight_grads, "ctx").astype(f32)

    grad_normed1 = over_last(grad_project, w_project)
    bias_grad = jnp.sum(grad_project.astype(f32), 0)
    input_back, first_gain_grad = norm_back(residual_in, inverse_first, gain_first, grad_normed1)
    input_grad = (grad_hidden + input_back).astype(bf16)[None]
    vectors = jnp.concatenate([first_gain_grad, second_gain_grad, bias_grad])
    vectors = lax.psum(vectors, ("ctx", "fsdp"))

    def piece(start, size):
        share = size // fsdp
        return lax.dynamic_slice_in_dim(vectors, start + f * share, share, 0)

    def hidden_grads(x, cot):
        act, g_gate, g_up = ffn(x, cot)
        return over_first(x, g_gate), over_first(x, g_up), over_first(act, cot)

    rows = x_all.shape[0]
    step = math.gcd(rows, 4096)
    if rows == step:
        gate_grad, up_grad, down_grad = hidden_grads(x_all, cot_all)
    else:

        def add_step(i, totals):
            x = lax.dynamic_slice_in_dim(x_all, i * step, step, 0)
            cot = lax.dynamic_slice_in_dim(cot_all, i * step, step, 0)
            return jax.tree.map(jnp.add, totals, hidden_grads(x, cot))

        start = (jnp.zeros(w_gate.shape, f32), jnp.zeros(w_up.shape, f32), jnp.zeros(w_down.shape, f32))
        gate_grad, up_grad, down_grad = lax.fori_loop(0, rows // step, add_step, start)
    return (
        block_out,
        input_grad,
        piece(0, width),
        weight_grads[:, :query_width],
        piece(2 * width, query_width),
        weight_grads[:, query_width : query_width + key_width],
        piece(2 * width + query_width, key_width),
        weight_grads[:, query_width + key_width : query_width + 2 * key_width],
        piece(2 * width + query_width + key_width, key_width),
        weight_grads[:, query_width + 2 * key_width :],
        piece(width, width),
        gate_grad,
        up_grad,
        down_grad,
        log_total.reshape(H, tok)[None],
    )


def solution(mesh):
    in_specs = (
        P("fsdp", "ctx", None),
        P("fsdp", "ctx"),
        P("fsdp", "ctx"),
        P("fsdp"),
        P("fsdp", None),
        P("fsdp"),
        P("fsdp", None),
        P("fsdp"),
        P("fsdp", None),
        P("fsdp"),
        P("fsdp", None),
        P("fsdp"),
        P(None, "fsdp"),
        P(None, "fsdp"),
        P("fsdp", None),
        P("fsdp", "ctx", None),
    )
    out_specs = (
        P("fsdp", "ctx", None),
        P("fsdp", "ctx", None),
        P("fsdp"),
        P("fsdp", None),
        P("fsdp"),
        P("fsdp", None),
        P("fsdp"),
        P("fsdp", None),
        P("fsdp"),
        P("fsdp", None),
        P("fsdp"),
        P(None, "fsdp"),
        P(None, "fsdp"),
        P("fsdp", None),
        P("fsdp", None, "ctx"),
    )
    return jax.shard_map(shards, mesh=mesh, in_specs=in_specs, out_specs=out_specs, check_vma=False)
```

```python
import functools
import math

import jax
import jax.numpy as jnp
from jax import lax
from jax.experimental import pallas as pl
from jax.experimental.pallas import tpu as pltpu
from jax.sharding import PartitionSpec as P

H = 14
KV = 2
HD = 64


EPSILON = 1e-06
ROPE_BASE = 1000000.0
MASK_FILL = -1e30
MESH = pl.DeviceIdType.MESH
VMEM = pl.BlockSpec(memory_space=pltpu.VMEM)
f32 = jnp.float32
bf16 = jnp.bfloat16


def rope_tables(positions, head_dim):
    half = head_dim // 2
    freq = ROPE_BASE ** (-(jnp.arange(half, dtype=jnp.float32) * 2.0 / head_dim))
    angle = positions.astype(jnp.float32)[:, None] * freq[None, :]
    return (jnp.cos(angle)[:, None, :], jnp.sin(angle)[:, None, :])


def rotate(values, cosine, sine_table):
    half = values.shape[-1] // 2
    leading, trailing = (values[..., :half], values[..., half:])
    return jnp.concatenate(
        [leading * cosine - trailing * sine_table, trailing * cosine + leading * sine_table], -1
    )


def rotate_back(grads, cosine, sine_table):
    half = grads.shape[-1] // 2
    leading, trailing = (grads[..., :half], grads[..., half:])
    return jnp.concatenate(
        [leading * cosine + trailing * sine_table, trailing * cosine - leading * sine_table], -1
    )


def norm_back(values, inverse, gain, grads):
    scaled = values * inverse
    weighted = grads * gain
    grad_values = inverse * (weighted - scaled * jnp.mean(weighted * scaled, -1, keepdims=True))
    return (grad_values, jnp.sum(grads * scaled, 0))


def remote(src, dst, send_sem, recv_sem, device):
    return pltpu.make_async_remote_copy(
        src_ref=src, dst_ref=dst, send_sem=send_sem, recv_sem=recv_sem, device_id=device,
        device_id_type=MESH,
    )


def where_am_i():
    c, f = lax.axis_index("ctx"), lax.axis_index("fsdp")
    c2 = c + 1 - 2 * (c % 2)
    m = f + 1 - 2 * (f % 2)
    n = (f + 2) % 4
    return c, f, c2, m, n


def greet(devices):
    barrier = pltpu.get_barrier_semaphore()
    for device in devices:
        pl.semaphore_signal(barrier, inc=1, device_id=device, device_id_type=MESH)
    pl.semaphore_wait(barrier, len(devices))


def gather_start(items, ss, rs, place):
    c, f, _, m, n = place
    h = c % 2
    for i, (src, dst) in enumerate(items):
        half = src.shape[0] // 2
        rows = pl.ds(h * half, half)
        remote(src.at[rows], dst(f).at[rows], ss.at[i, 1], rs.at[i, 1], (c, n)).start()
    for i, (src, dst) in enumerate(items):
        remote(src, dst(f), ss.at[i, 0], rs.at[i, 0], (c, m)).start()
        dst(f)[...] = src[...]


def gather_finish(items, ss, rs, place):
    c, f, c2, m, n = place
    h = c % 2
    far = (m + 2) % 4
    for i, (src, dst) in enumerate(items):
        half = src.shape[0] // 2
        mine = dst(n).at[pl.ds(h * half, half)]
        remote(mine, mine, ss.at[i, 1], rs.at[i, 1], (c, n)).wait_recv()
        remote(mine, mine, ss.at[i, 2], rs.at[i, 2], (c2, f)).start()
        remote(mine, mine, ss.at[i, 3], rs.at[i, 3], (c, m)).start()
    for i, (src, dst) in enumerate(items):
        half = src.shape[0] // 2
        other = dst(n).at[pl.ds((1 - h) * half, half)]
        remote(other, other, ss.at[i, 2], rs.at[i, 2], (c2, f)).wait_recv()
        remote(other, other, ss.at[i, 4], rs.at[i, 4], (c, m)).start()
    for i, (src, dst) in enumerate(items):
        half = src.shape[0] // 2
        mine, other = pl.ds(h * half, half), pl.ds((1 - h) * half, half)
        remote(src, dst(m), ss.at[i, 0], rs.at[i, 0], (c, m)).wait()
        remote(src.at[mine], dst(f).at[mine], ss.at[i, 1], rs.at[i, 1], (c, n)).wait_send()
        remote(src.at[mine], dst(n).at[mine], ss.at[i, 2], rs.at[i, 2], (c2, f)).wait_send()
        remote(src.at[mine], dst(far).at[mine], ss.at[i, 3], rs.at[i, 3], (c, m)).wait()
        remote(src.at[other], dst(far).at[other], ss.at[i, 4], rs.at[i, 4], (c, m)).wait()


def tokens_start(items, ss, rs, place):
    c, f, _, m, n = place
    for i, (src, dst) in enumerate(items):
        half = src.shape[0] // 2
        for j in range(2):
            rows = pl.ds(j * half, half)
            remote(src.at[rows], dst(f, rows), ss.at[i, 1 + j], rs.at[i, 1 + j], (c, n)).start()
    for i, (src, dst) in enumerate(items):
        rows = pl.ds(0, src.shape[0])
        remote(src, dst(f, rows), ss.at[i, 0], rs.at[i, 0], (c, m)).start()
        dst(f, rows)[...] = src[...]


def tokens_finish(items, ss, rs, place):
    c, f, _, m, n = place
    far = (m + 2) % 4
    for i, (src, dst) in enumerate(items):
        half = src.shape[0] // 2
        for j in range(2):
            here = dst(n, pl.ds(j * half, half))
            remote(here, here, ss.at[i, 1 + j], rs.at[i, 1 + j], (c, n)).wait_recv()
            remote(here, here, ss.at[i, 3 + j], rs.at[i, 3 + j], (c, m)).start()
    for i, (src, dst) in enumerate(items):
        half = src.shape[0] // 2
        remote(src, dst(m, pl.ds(0, src.shape[0])), ss.at[i, 0], rs.at[i, 0], (c, m)).wait()
        for j in range(2):
            rows = pl.ds(j * half, half)
            remote(src.at[rows], dst(f, rows), ss.at[i, 1 + j], rs.at[i, 1 + j], (c, n)).wait_send()
            remote(src.at[rows], dst(far, rows), ss.at[i, 3 + j], rs.at[i, 3 + j], (c, m)).wait()


def gather_sems(count):
    return [pltpu.SemaphoreType.DMA((count, 5)), pltpu.SemaphoreType.DMA((count, 5))]


def comm_call(body, out_shape, scratch, ident):
    def call(*args):
        return pl.pallas_call(
            body,
            out_shape=out_shape,
            in_specs=[VMEM] * len(args),
            out_specs=jax.tree.map(lambda _: VMEM, out_shape),
            scratch_shapes=scratch,
            compiler_params=pltpu.CompilerParams(
                collective_id=ident, has_side_effects=True, vmem_limit_bytes=48 << 20
            ),
        )(*args)

    return call


def front_body(
    ctx, depth, wq, wk, wv, wo, small, seg, wp_o, wo_o, small_o, seg_o, ss, rs, small_ss, small_rs, seg_ss, seg_rs
):
    place = where_am_i()
    c, f, _, m, n = place
    far = (m + 2) % 4
    peers = [lax.rem(c + k, ctx) for k in range(1, ctx)]
    greet([(p, f) for p in peers] + [(c, m), (c, n), (c, far)])
    width = wq.shape[1]
    narrow = wk.shape[1]

    def rows(g):
        return pl.ds(pl.multiple_of(g * depth, 16), depth)

    items = [
        (wq, lambda g: wp_o.at[rows(g), pl.ds(0, width)]),
        (wk, lambda g: wp_o.at[rows(g), pl.ds(width, narrow)]),
        (wv, lambda g: wp_o.at[rows(g), pl.ds(width + narrow, narrow)]),
        (wo, lambda g: wo_o.at[rows(g)]),
    ]
    copies = [
        remote(small, small_o.at[f], small_ss.at[k], small_rs.at[k], (c, g)) for k, g in enumerate((m, n, far))
    ]
    for copy in copies:
        copy.start()
    for k, p in enumerate(peers):
        remote(seg, seg_o.at[c], seg_ss.at[k], seg_rs.at[k], (p, f)).start()
    gather_start(items, ss, rs, place)
    small_o[f] = small[...]
    seg_o[c] = seg[...]
    gather_finish(items, ss, rs, place)
    for k, g in enumerate((m, n, far)):
        remote(small, small_o.at[g], small_ss.at[k], small_rs.at[k], (c, g)).wait()
    for k, p in enumerate(peers):
        giver = lax.rem(c + ctx - 1 - k, ctx)
        remote(seg, seg_o.at[giver], seg_ss.at[k], seg_rs.at[k], (p, f)).wait()


def spread_start(src, dst, ss, rs, place, lines):
    c, f, c2, _, _ = place
    for k in range(1, lines):
        p = lax.rem(c // 2 + k, lines) * 2 + c % 2
        remote(src, dst.at[c], ss.at[0, k], rs.at[0, k], (p, f)).start()
    remote(src, dst.at[c], ss.at[1, 0], rs.at[1, 0], (c2, f)).start()


def spread_finish(src, dst, ss, rs, place, lines):
    c, f, c2, _, _ = place
    for k in range(1, lines):
        giver = lax.rem(c // 2 + lines - k, lines) * 2 + c % 2
        block = dst.at[giver]
        remote(block, block, ss.at[0, k], rs.at[0, k], (c2, f)).wait_recv()
        remote(block, block, ss.at[1, k], rs.at[1, k], (c2, f)).start()
    for k in range(lines):
        giver = lax.rem(c2 // 2 + lines - k, lines) * 2 + c2 % 2
        remote(src, dst.at[giver], ss.at[1, k], rs.at[1, k], (c2, f)).wait()
        if k:
            remote(src, dst.at[c], ss.at[0, k], rs.at[0, k], (c2, f)).wait_send()


def line_devices(place, lines):
    c, f, c2, _, _ = place
    return [(lax.rem(c // 2 + k, lines) * 2 + c % 2, f) for k in range(1, lines)] + [(c2, f)]


def kv_body(lines, kv, kv_o, ss, rs):
    place = where_am_i()
    greet(line_devices(place, lines))
    spread_start(kv, kv_o, ss, rs, place, lines)
    kv_o[place[0]] = kv[...]
    spread_finish(kv, kv_o, ss, rs, place, lines)


def ag_body(x, x_o, ss, rs):
    place = where_am_i()
    c, _, _, m, n = place
    greet([(c, m), (c, n)])
    items = [(x, lambda g, rows: x_o.at[g, rows])]
    tokens_start(items, ss, rs, place)
    tokens_finish(items, ss, rs, place)


def project_body(x, vec, x_o, vec_o, ss, rs, held, vs, vr):
    place = where_am_i()
    c, _, _, m, n = place
    far = (m + 2) % 4
    greet([(c, m), (c, n), (c, far)])
    items = [(x, lambda g, rows: x_o.at[g, rows])]
    tokens_start(items, ss, rs, place)
    copies = [remote(vec, held.at[k], vs.at[k], vr.at[k], (c, g)) for k, g in enumerate((m, n, far))]
    for copy in copies:
        copy.start()
    tokens_finish(items, ss, rs, place)
    total = vec[...]
    for k, copy in enumerate(copies):
        copy.wait()
        total = total + held[k]
    vec_o[...] = total


def rs_body(part, out, near, sums, far_in, ss, rs):
    c, f, _, m, n = where_am_i()
    far = (m + 2) % 4
    greet([(c, m), (c, n)])
    first = remote(part.at[far], near.at[0], ss.at[0], rs.at[0], (c, m))
    second = remote(part.at[m], near.at[1], ss.at[1], rs.at[1], (c, m))
    first.start()
    second.start()
    first.wait()
    sums[...] = (part[n].astype(f32) + near[0].astype(f32)).astype(bf16)
    across = remote(sums, far_in, ss.at[2], rs.at[2], (c, n))
    across.start()
    second.wait()
    mine = part[f].astype(f32) + near[1].astype(f32)
    across.wait()
    out[...] = mine + far_in[...].astype(f32)


def dkv_body(ctx, part, ghl, sl, out, ghl_o, sl_o, held, ss, rs, gs, gr, as_, ar):
    place = where_am_i()
    c, f, _, m, n = place
    far = (m + 2) % 4
    peers = [lax.rem(c + k, ctx) for k in range(1, ctx)]
    greet([(p, f) for p in peers] + [(c, m), (c, n), (c, far)])
    for k, p in enumerate(peers):
        remote(part.at[p], held.at[k], ss.at[k], rs.at[k], (p, f)).start()
    for k, g in enumerate((n, far, m)):
        remote(sl.at[g], sl_o.at[f], as_.at[k], ar.at[k], (c, g)).start()
    items = [(ghl, lambda g, rows: ghl_o.at[g, rows])]
    tokens_start(items, gs, gr, place)
    sl_o[f] = sl[f]
    total = part[c].astype(f32)
    tokens_finish(items, gs, gr, place)
    for k, p in enumerate(peers):
        remote(part.at[p], held.at[k], ss.at[k], rs.at[k], (p, f)).wait()
        total = total + held[k].astype(f32)
    for k, g in enumerate((n, far, m)):
        remote(sl.at[g], sl_o.at[g], as_.at[k], ar.at[k], (c, g)).wait()
    out[...] = total


def over_last(a, b):
    return lax.dot_general(a, b, (((1,), (1,)), ((), ())), preferred_element_type=f32)


def over_first(a, b):
    return lax.dot_general(a, b, (((0,), (0,)), ((), ())), preferred_element_type=f32)


def plain_dot(a, b):
    return jnp.dot(a, b, preferred_element_type=f32)


def hidden_units(x, cot, wg, wu, wd):
    gate, up, g_act = over_last(wg, x), over_last(wu, x), over_last(wd, cot)
    sg = jax.nn.sigmoid(gate)
    silu = gate * sg
    act = (silu * up).astype(bf16)
    g_gate = (g_act * up * (sg * (1.0 + gate * (1.0 - sg)))).astype(bf16)
    g_up = (g_act * silu).astype(bf16)
    return act, g_gate, g_up


def hidden_body(
    chunk, block, x_h, c_h, wg_h, wu_h, wd_h, og_h, ou_h, od_h, xs, cs, wg, wu, wd, acc, in_sem, w_sem, out_sem
):
    rows = x_h.shape[0]
    steps, blocks, held = rows // chunk, wg.shape[0] // block, xs.shape[0] // chunk
    loads = [
        pltpu.make_async_copy(src, dst, w_sem.at[j])
        for j, (src, dst) in enumerate(((wg_h, wg), (wu_h, wu), (wd_h, wd)))
    ]

    def tokens(i):
        src = pl.ds(pl.multiple_of(i * chunk, chunk), chunk)
        dst = pl.ds(pl.multiple_of(i % held * chunk, chunk), chunk)
        return [
            pltpu.make_async_copy(x_h.at[src], xs.at[dst], in_sem.at[i % held, 0]),
            pltpu.make_async_copy(c_h.at[src], cs.at[dst], in_sem.at[i % held, 1]),
        ]

    def results(b, slot):
        at = pl.ds(pl.multiple_of(b * block, 16), block)
        return [
            pltpu.make_async_copy(acc.at[slot, j], out.at[at], out_sem.at[slot, j])
            for j, out in enumerate((og_h, ou_h, od_h))
        ]

    resident = held == steps
    for copy in tokens(0) + loads:
        copy.start()
    for i in range(1, held if resident else 1):
        for copy in tokens(i):
            copy.start()
    for copy in loads:
        copy.wait()
    slots = acc.shape[0]

    @pl.loop(0, blocks)
    def _(b):
        slot = b % slots
        at = pl.ds(pl.multiple_of(b * block, 16), block)

        @pl.when(b >= slots)
        def _():
            for copy in results(b - slots, slot):
                copy.wait()

        @pl.loop(0, steps)
        def _(i):
            if resident:

                @pl.when(b == 0)
                def _():
                    for copy in tokens(i):
                        copy.wait()

            else:
                for copy in tokens(i):
                    copy.wait()

                @pl.when((i + 1 < steps) | (b + 1 < blocks))
                def _():
                    for copy in tokens(lax.rem(i + 1, steps)):
                        copy.start()

            t = pl.ds(pl.multiple_of(i % held * chunk, chunk), chunk)
            x, cot = xs[t], cs[t]
            act, g_gate, g_up = hidden_units(x, cot, wg[at], wu[at], wd[at])

            @pl.when(i == 0)
            def _():
                acc[slot, 0] = plain_dot(g_gate, x)
                acc[slot, 1] = plain_dot(g_up, x)
                acc[slot, 2] = plain_dot(act, cot)

            @pl.when(i > 0)
            def _():
                acc[slot, 0] += plain_dot(g_gate, x)
                acc[slot, 1] += plain_dot(g_up, x)
                acc[slot, 2] += plain_dot(act, cot)

        for copy in results(b, slot):
            copy.start()

    for b in range(max(0, blocks - slots), blocks):
        for copy in results(b, b % slots):
            copy.wait()


def hidden_grads(x, cot, wg, wu, wd):
    rows, width = x.shape
    units = wg.shape[0]
    chunk = math.gcd(rows, 1024)
    block = units // 2
    held = min(rows // chunk, 4)
    any_spec = pl.BlockSpec(memory_space=pl.ANY)
    dma = pltpu.SemaphoreType.DMA
    return pl.pallas_call(
        functools.partial(hidden_body, chunk, block),
        out_shape=(jax.ShapeDtypeStruct((units, width), f32),) * 3,
        in_specs=[any_spec] * 5,
        out_specs=(any_spec,) * 3,
        scratch_shapes=[pltpu.VMEM((held * chunk, width), bf16)] * 2
        + [pltpu.VMEM((units, width), bf16)] * 3
        + [pltpu.VMEM((2, 3, block, width), f32), dma((held, 2)), dma((3,)), dma((2, 3))],
        compiler_params=pltpu.CompilerParams(vmem_limit_bytes=60 << 20),
        cost_estimate=pl.CostEstimate(
            flops=12 * rows * width * units, bytes_accessed=4 * rows * width + 18 * units * width, transcendentals=0
        ),
        name="hidden_grads",
    )(x, cot, wg, wu, wd)


def shards(
    layer_input,
    seq_ids,
    positions,
    norm_gain,
    w_query,
    b_query,
    w_key,
    b_key,
    w_value,
    b_value,
    w_output,
    mlp_gain,
    w_gate,
    w_up,
    w_down,
    cotangent,
):
    tok = layer_input.shape[1]
    width = layer_input.shape[2]
    group = H // KV
    query_width = H * HD
    key_width = KV * HD
    score_scale = HD ** (-0.5)
    ctx = lax.axis_size("ctx")
    fsdp = lax.axis_size("fsdp")
    depth = width // fsdp
    lines = ctx // 2
    c, f = lax.axis_index("ctx"), lax.axis_index("fsdp")
    seq_length = ctx * tok
    dma = pltpu.SemaphoreType.DMA
    sds = jax.ShapeDtypeStruct
    input_rows = layer_input[0]
    grad_out = cotangent[0]
    own_segment = seq_ids[0]
    own_positions = positions[0]
    query_rows = c * tok + jnp.arange(tok, dtype=jnp.int32)

    cot_all = lax.all_gather(grad_out, ("ctx", "fsdp"), axis=0, tiled=True)

    def padded(v):
        return jnp.pad(v, (0, 256 - v.shape[0]))

    small = jnp.stack([padded(v) for v in (norm_gain, mlp_gain, b_query, b_key, b_value)])
    small = jnp.pad(small, ((0, 11), (0, 0)))
    seg_tile = jnp.broadcast_to(own_segment[None], (8, tok))
    w_project, wo_full, small_all, seg_all = comm_call(
        functools.partial(front_body, ctx, depth),
        (
            sds((width, query_width + 2 * key_width), bf16),
            sds((query_width, width), bf16),
            sds((fsdp, 16, 256), bf16),
            sds((ctx, 8, tok), jnp.int32),
        ),
        gather_sems(4) + [dma((3,)), dma((3,)), dma((ctx - 1,)), dma((ctx - 1,))],
        0,
    )(w_query, w_key, w_value, w_output, small, seg_tile)
    all_segments = seg_all[:, 0].reshape(seq_length)
    small_all = small_all.astype(f32)
    gain_first = small_all[:, 0, :depth].reshape(width)
    gain_second = small_all[:, 1, :depth].reshape(width)
    kd = key_width // fsdp
    b_project = jnp.concatenate(
        [
            small_all[:, 2, :depth].reshape(query_width),
            small_all[:, 3, :kd].reshape(key_width),
            small_all[:, 4, :kd].reshape(key_width),
        ]
    )
    residual_in = input_rows.astype(f32)
    inverse_first = lax.rsqrt(jnp.mean(residual_in * residual_in, -1, keepdims=True) + EPSILON)
    normed_first = (residual_in * inverse_first * gain_first).astype(bf16)
    projected = jnp.dot(normed_first, w_project, preferred_element_type=f32) + b_project
    cosine, sine_table = rope_tables(own_positions, HD)
    query = rotate(projected[:, :query_width].reshape(tok, H, HD), cosine, sine_table)
    query = query.astype(bf16).reshape(tok, KV, group, HD)
    key_rot = rotate(
        projected[:, query_width : query_width + key_width].reshape(tok, KV, HD), cosine, sine_table
    )
    value_low = projected[:, query_width + key_width :].astype(bf16)
    key_value = jnp.concatenate([key_rot.astype(bf16).reshape(tok, key_width), value_low], 1)
    kv_all = comm_call(
        functools.partial(kv_body, lines), sds((ctx, tok, 2 * key_width), bf16), [dma((2, lines)), dma((2, lines))], 1
    )(key_value).reshape(seq_length, 2 * key_width)
    keys = kv_all[:, :key_width].reshape(seq_length, KV, HD)
    values = kv_all[:, key_width:].reshape(seq_length, KV, HD)
    key_rows = jnp.arange(seq_length, dtype=jnp.int32)
    allowed = (key_rows[None, :] <= query_rows[:, None]) & (all_segments[None, :] == own_segment[:, None])
    raw_scores = jnp.einsum("tkgd,nkd->kgtn", query, keys, preferred_element_type=f32) * score_scale
    highest = jnp.max(jnp.where(allowed, raw_scores, MASK_FILL), -1)
    exp_scores = jnp.where(allowed, jnp.exp(raw_scores - highest[..., None]), 0.0)
    running_sum = jnp.sum(exp_scores, -1)
    accumulated = jnp.einsum("kgtn,nkd->tkgd", exp_scores.astype(bf16), values, preferred_element_type=f32)
    log_total = highest + jnp.log(running_sum)
    attention = accumulated / jnp.transpose(running_sum, (2, 0, 1))[..., None]
    attention_low = attention.reshape(tok, query_width).astype(bf16)
    hidden_state = residual_in + jnp.dot(attention_low, wo_full, preferred_element_type=f32)
    inverse_second = lax.rsqrt(jnp.mean(hidden_state * hidden_state, -1, keepdims=True) + EPSILON)
    normed_second = (hidden_state * inverse_second * gain_second).astype(bf16)
    x_all = lax.all_gather(normed_second, ("ctx", "fsdp"), axis=0, tiled=True)
    x_group = comm_call(
        ag_body, sds((fsdp, tok, width), bf16), gather_sems(1), 2
    )(normed_second).reshape(fsdp * tok, width)
    cot_group = lax.dynamic_slice_in_dim(cot_all, c * fsdp * tok, fsdp * tok, 0)

    def ffn(x, cot):
        gate = jnp.dot(x, w_gate, preferred_element_type=f32)
        up = jnp.dot(x, w_up, preferred_element_type=f32)
        g_act = lax.dot_general(cot, w_down, (((1,), (1,)), ((), ())), preferred_element_type=f32)
        sg = jax.nn.sigmoid(gate)
        act = (gate * sg * up).astype(bf16)
        g_gate = (g_act * up * sg * (1.0 + gate * (1.0 - sg))).astype(bf16)
        g_up = (g_act * gate * sg).astype(bf16)
        return act, g_gate, g_up

    act, g_gate, g_up = ffn(x_group, cot_group)
    g_normed_part = (over_last(g_gate, w_gate) + over_last(g_up, w_up)).astype(bf16)
    grad_normed2 = comm_call(
        rs_body,
        sds((tok, width), f32),
        [
            pltpu.VMEM((2, tok, width), bf16),
            pltpu.VMEM((tok, width), bf16),
            pltpu.VMEM((tok, width), bf16),
            dma((3,)),
            dma((3,)),
        ],
        3,
    )(g_normed_part.reshape(fsdp, tok, width))
    down_part = jnp.dot(act, w_down, preferred_element_type=f32).astype(bf16)
    down_out = lax.psum_scatter(down_part, "fsdp", scatter_dimension=0, tiled=True).astype(f32)
    block_out = (hidden_state + down_out).astype(bf16)[None]

    hidden_back, second_gain_grad = norm_back(hidden_state, inverse_second, gain_second, grad_normed2)
    grad_hidden = grad_out.astype(f32) + hidden_back
    grad_hidden_low = grad_hidden.astype(bf16)
    grad_attention = over_last(grad_hidden_low, wo_full).astype(bf16)
    grad_attention = grad_attention.reshape(tok, KV, group, HD)
    delta_rows = jnp.einsum("tkgd,tkgd->kgt", grad_attention.astype(f32), attention)
    probs = jnp.where(allowed, jnp.exp(raw_scores - log_total[..., None]), 0.0)
    grad_values = jnp.einsum("kgtn,tkgd->nkd", probs.astype(bf16), grad_attention, preferred_element_type=f32)
    grad_probs = jnp.einsum("tkgd,nkd->kgtn", grad_attention, values, preferred_element_type=f32)
    grad_scores = (probs * (grad_probs - delta_rows[..., None])).astype(bf16)
    grad_query = jnp.einsum("kgtn,nkd->tkgd", grad_scores, keys, preferred_element_type=f32) * score_scale
    grad_keys = jnp.einsum("kgtn,tkgd->nkd", grad_scores, query, preferred_element_type=f32) * score_scale
    grad_pairs = jnp.concatenate(
        [grad_keys.reshape(seq_length, key_width), grad_values.reshape(seq_length, key_width)], 1
    ).astype(bf16)
    slices = jnp.concatenate(
        [
            normed_first.reshape(tok, fsdp, depth).transpose(1, 0, 2),
            attention_low.reshape(tok, fsdp, depth).transpose(1, 0, 2),
        ],
        1,
    )
    grad_pairs, ghl_group, slice_group = comm_call(
        functools.partial(dkv_body, ctx),
        (
            sds((tok, 2 * key_width), f32),
            sds((fsdp, tok, width), bf16),
            sds((fsdp, 2 * tok, depth), bf16),
        ),
        [pltpu.VMEM((ctx - 1, tok, 2 * key_width), bf16), dma((ctx - 1,)), dma((ctx - 1,))]
        + gather_sems(1)
        + [dma((3,)), dma((3,))],
        4,
    )(grad_pairs.reshape(ctx, tok, 2 * key_width), grad_hidden_low, slices)
    grad_q_pre = (
        rotate_back(grad_query.reshape(tok, H, HD), cosine, sine_table).reshape(tok, query_width).astype(bf16)
    )
    grad_k_pre = (
        rotate_back(grad_pairs[:, :key_width].reshape(tok, KV, HD), cosine, sine_table)
        .reshape(tok, key_width)
        .astype(bf16)
    )
    grad_v_pre = grad_pairs[:, key_width:].astype(bf16)
    grad_project = jnp.concatenate([grad_q_pre, grad_k_pre, grad_v_pre], 1)
    grad_normed1 = over_last(grad_project, w_project)
    bias_grad = jnp.sum(grad_project.astype(f32), 0)
    input_back, first_gain_grad = norm_back(residual_in, inverse_first, gain_first, grad_normed1)
    input_grad = (grad_hidden + input_back).astype(bf16)[None]
    vectors = jnp.concatenate([first_gain_grad, second_gain_grad, bias_grad])
    vectors = jnp.pad(vectors, (0, 3072 - vectors.shape[0])).reshape(8, 384)
    gp_group, vectors = comm_call(
        project_body,
        (sds((fsdp, tok, grad_project.shape[1]), bf16), sds(vectors.shape, f32)),
        gather_sems(1) + [pltpu.VMEM((3,) + vectors.shape, f32), dma((3,)), dma((3,))],
        5,
    )(grad_project, vectors)
    gp_group = gp_group.reshape(fsdp * tok, grad_project.shape[1])
    vectors = vectors.reshape(3072)
    normed_slice = slice_group[:, :tok].reshape(fsdp * tok, depth)
    attention_slice = slice_group[:, tok:].reshape(fsdp * tok, depth)
    project_grad = over_first(normed_slice, gp_group)
    output_grad = over_first(attention_slice, ghl_group.reshape(fsdp * tok, width))

    def piece(start, size):
        share = size // fsdp
        return lax.dynamic_slice_in_dim(vectors, start + f * share, share, 0)

    columns = project_grad.shape[1] + width
    starts = ((0, width), (width, width), (2 * width, query_width), (2 * width + query_width, key_width),
              (2 * width + query_width + key_width, key_width))
    own = jnp.concatenate([piece(*at) for at in starts])
    own = jnp.pad(own, (0, columns - own.shape[0]))
    weight_grads = jnp.concatenate(
        [jnp.concatenate([project_grad, output_grad], 1), jnp.broadcast_to(own[None], (16, columns))], 0
    ).astype(bf16)
    weight_grads = lax.psum(weight_grads, "ctx")
    weight_grads = weight_grads.astype(f32)
    own = weight_grads[depth]
    weight_grads = weight_grads[:depth]
    ends = [0]
    for _, size in starts:
        ends.append(ends[-1] + size // fsdp)
    own = [own[ends[i] : ends[i + 1]] for i in range(5)]

    gate_grad, up_grad, down_grad = hidden_grads(x_all, cot_all, w_gate.T, w_up.T, w_down)
    return (
        block_out,
        input_grad,
        own[0],
        weight_grads[:, :query_width],
        own[2],
        weight_grads[:, query_width : query_width + key_width],
        own[3],
        weight_grads[:, query_width + key_width : query_width + 2 * key_width],
        own[4],
        weight_grads[:, query_width + 2 * key_width :],
        own[1],
        gate_grad.T,
        up_grad.T,
        down_grad,
        log_total.reshape(H, tok)[None],
    )


def solution(mesh):
    in_specs = (
        P("fsdp", "ctx", None),
        P("fsdp", "ctx"),
        P("fsdp", "ctx"),
        P("fsdp"),
        P("fsdp", None),
        P("fsdp"),
        P("fsdp", None),
        P("fsdp"),
        P("fsdp", None),
        P("fsdp"),
        P("fsdp", None),
        P("fsdp"),
        P(None, "fsdp"),
        P(None, "fsdp"),
        P("fsdp", None),
        P("fsdp", "ctx", None),
    )
    out_specs = (
        P("fsdp", "ctx", None),
        P("fsdp", "ctx", None),
        P("fsdp"),
        P("fsdp", None),
        P("fsdp"),
        P("fsdp", None),
        P("fsdp"),
        P("fsdp", None),
        P("fsdp"),
        P("fsdp", None),
        P("fsdp"),
        P(None, "fsdp"),
        P(None, "fsdp"),
        P("fsdp", None),
        P("fsdp", None, "ctx"),
    )
    return jax.shard_map(shards, mesh=mesh, in_specs=in_specs, out_specs=out_specs, check_vma=False)
```

```python
import functools
import math

import jax
import jax.numpy as jnp
from jax import lax
from jax.experimental import pallas as pl
from jax.experimental.pallas import tpu as pltpu
from jax.sharding import PartitionSpec as P


H = 14
KV = 2
HD = 64


EPSILON = 1e-06
ROPE_BASE = 1000000.0
MASK_FILL = -1e30
MESH = pl.DeviceIdType.MESH
VMEM = pl.BlockSpec(memory_space=pltpu.VMEM)
f32 = jnp.float32
bf16 = jnp.bfloat16


def rope_tables(positions, head_dim):
    half = head_dim // 2
    freq = ROPE_BASE ** (-(jnp.arange(half, dtype=jnp.float32) * 2.0 / head_dim))
    angle = positions.astype(jnp.float32)[:, None] * freq[None, :]
    return (jnp.cos(angle)[:, None, :], jnp.sin(angle)[:, None, :])


def rotate(values, cosine, sine_table):
    half = values.shape[-1] // 2
    leading, trailing = (values[..., :half], values[..., half:])
    return jnp.concatenate(
        [leading * cosine - trailing * sine_table, trailing * cosine + leading * sine_table], -1
    )


def rotate_back(grads, cosine, sine_table):
    half = grads.shape[-1] // 2
    leading, trailing = (grads[..., :half], grads[..., half:])
    return jnp.concatenate(
        [leading * cosine + trailing * sine_table, trailing * cosine - leading * sine_table], -1
    )


def norm_back(values, inverse, gain, grads):
    scaled = values * inverse
    weighted = grads * gain
    grad_values = inverse * (weighted - scaled * jnp.mean(weighted * scaled, -1, keepdims=True))
    return (grad_values, jnp.sum(grads * scaled, 0))


def remote(src, dst, send_sem, recv_sem, device):
    return pltpu.make_async_remote_copy(
        src_ref=src, dst_ref=dst, send_sem=send_sem, recv_sem=recv_sem, device_id=device,
        device_id_type=MESH,
    )


def where_am_i():
    c, f = lax.axis_index("ctx"), lax.axis_index("fsdp")
    c2 = c + 1 - 2 * (c % 2)
    m = f + 1 - 2 * (f % 2)
    n = (f + 2) % 4
    return c, f, c2, m, n


def greet(devices):
    barrier = pltpu.get_barrier_semaphore()
    for device in devices:
        pl.semaphore_signal(barrier, inc=1, device_id=device, device_id_type=MESH)
    pl.semaphore_wait(barrier, len(devices))


def gather_start(items, ss, rs, place):
    c, f, _, m, n = place
    h = c % 2
    for i, (src, dst) in enumerate(items):
        half = src.shape[0] // 2
        rows = pl.ds(h * half, half)
        remote(src.at[rows], dst(f).at[rows], ss.at[i, 1], rs.at[i, 1], (c, n)).start()
    for i, (src, dst) in enumerate(items):
        remote(src, dst(f), ss.at[i, 0], rs.at[i, 0], (c, m)).start()
        dst(f)[...] = src[...]


def gather_finish(items, ss, rs, place):
    c, f, c2, m, n = place
    h = c % 2
    far = (m + 2) % 4
    for i, (src, dst) in enumerate(items):
        half = src.shape[0] // 2
        mine = dst(n).at[pl.ds(h * half, half)]
        remote(mine, mine, ss.at[i, 1], rs.at[i, 1], (c, n)).wait_recv()
        remote(mine, mine, ss.at[i, 2], rs.at[i, 2], (c2, f)).start()
        remote(mine, mine, ss.at[i, 3], rs.at[i, 3], (c, m)).start()
    for i, (src, dst) in enumerate(items):
        half = src.shape[0] // 2
        other = dst(n).at[pl.ds((1 - h) * half, half)]
        remote(other, other, ss.at[i, 2], rs.at[i, 2], (c2, f)).wait_recv()
        remote(other, other, ss.at[i, 4], rs.at[i, 4], (c, m)).start()
    for i, (src, dst) in enumerate(items):
        half = src.shape[0] // 2
        mine, other = pl.ds(h * half, half), pl.ds((1 - h) * half, half)
        remote(src, dst(m), ss.at[i, 0], rs.at[i, 0], (c, m)).wait()
        remote(src.at[mine], dst(f).at[mine], ss.at[i, 1], rs.at[i, 1], (c, n)).wait_send()
        remote(src.at[mine], dst(n).at[mine], ss.at[i, 2], rs.at[i, 2], (c2, f)).wait_send()
        remote(src.at[mine], dst(far).at[mine], ss.at[i, 3], rs.at[i, 3], (c, m)).wait()
        remote(src.at[other], dst(far).at[other], ss.at[i, 4], rs.at[i, 4], (c, m)).wait()


def tokens_start(items, ss, rs, place):
    c, f, _, m, n = place
    for i, (src, dst) in enumerate(items):
        half = src.shape[0] // 2
        for j in range(2):
            rows = pl.ds(j * half, half)
            remote(src.at[rows], dst(f, rows), ss.at[i, 1 + j], rs.at[i, 1 + j], (c, n)).start()
    for i, (src, dst) in enumerate(items):
        rows = pl.ds(0, src.shape[0])
        remote(src, dst(f, rows), ss.at[i, 0], rs.at[i, 0], (c, m)).start()
        dst(f, rows)[...] = src[...]


def tokens_finish(items, ss, rs, place):
    c, f, _, m, n = place
    far = (m + 2) % 4
    for i, (src, dst) in enumerate(items):
        half = src.shape[0] // 2
        for j in range(2):
            here = dst(n, pl.ds(j * half, half))
            remote(here, here, ss.at[i, 1 + j], rs.at[i, 1 + j], (c, n)).wait_recv()
            remote(here, here, ss.at[i, 3 + j], rs.at[i, 3 + j], (c, m)).start()
    for i, (src, dst) in enumerate(items):
        half = src.shape[0] // 2
        remote(src, dst(m, pl.ds(0, src.shape[0])), ss.at[i, 0], rs.at[i, 0], (c, m)).wait()
        for j in range(2):
            rows = pl.ds(j * half, half)
            remote(src.at[rows], dst(f, rows), ss.at[i, 1 + j], rs.at[i, 1 + j], (c, n)).wait_send()
            remote(src.at[rows], dst(far, rows), ss.at[i, 3 + j], rs.at[i, 3 + j], (c, m)).wait()


def gather_sems(count):
    return [pltpu.SemaphoreType.DMA((count, 5)), pltpu.SemaphoreType.DMA((count, 5))]


def comm_call(body, out_shape, scratch, ident):
    def call(*args):
        return pl.pallas_call(
            body,
            out_shape=out_shape,
            in_specs=[VMEM] * len(args),
            out_specs=jax.tree.map(lambda _: VMEM, out_shape),
            scratch_shapes=scratch,
            compiler_params=pltpu.CompilerParams(
                collective_id=ident, has_side_effects=True, vmem_limit_bytes=48 << 20
            ),
        )(*args)

    return call


def front_body(
    ctx, depth, wq, wk, wv, wo, small, seg, wp_o, wo_o, small_o, seg_o, ss, rs, small_ss, small_rs, seg_ss, seg_rs
):
    place = where_am_i()
    c, f, _, m, n = place
    far = (m + 2) % 4
    peers = [lax.rem(c + k, ctx) for k in range(1, ctx)]
    greet([(p, f) for p in peers] + [(c, m), (c, n), (c, far)])
    width = wq.shape[1]
    narrow = wk.shape[1]

    def rows(g):
        return pl.ds(pl.multiple_of(g * depth, 16), depth)

    items = [
        (wq, lambda g: wp_o.at[rows(g), pl.ds(0, width)]),
        (wk, lambda g: wp_o.at[rows(g), pl.ds(width, narrow)]),
        (wv, lambda g: wp_o.at[rows(g), pl.ds(width + narrow, narrow)]),
        (wo, lambda g: wo_o.at[rows(g)]),
    ]
    copies = [
        remote(small, small_o.at[f], small_ss.at[k], small_rs.at[k], (c, g)) for k, g in enumerate((m, n, far))
    ]
    for copy in copies:
        copy.start()
    for k, p in enumerate(peers):
        remote(seg, seg_o.at[c], seg_ss.at[k], seg_rs.at[k], (p, f)).start()
    gather_start(items, ss, rs, place)
    small_o[f] = small[...]
    seg_o[c] = seg[...]
    gather_finish(items, ss, rs, place)
    for k, g in enumerate((m, n, far)):
        remote(small, small_o.at[g], small_ss.at[k], small_rs.at[k], (c, g)).wait()
    for k, p in enumerate(peers):
        giver = lax.rem(c + ctx - 1 - k, ctx)
        remote(seg, seg_o.at[giver], seg_ss.at[k], seg_rs.at[k], (p, f)).wait()


def spread_start(src, dst, ss, rs, place, lines):
    c, f, c2, _, _ = place
    for k in range(1, lines):
        p = lax.rem(c // 2 + k, lines) * 2 + c % 2
        remote(src, dst.at[c], ss.at[0, k], rs.at[0, k], (p, f)).start()
    remote(src, dst.at[c], ss.at[1, 0], rs.at[1, 0], (c2, f)).start()


def spread_finish(src, dst, ss, rs, place, lines):
    c, f, c2, _, _ = place
    for k in range(1, lines):
        giver = lax.rem(c // 2 + lines - k, lines) * 2 + c % 2
        block = dst.at[giver]
        remote(block, block, ss.at[0, k], rs.at[0, k], (c2, f)).wait_recv()
        remote(block, block, ss.at[1, k], rs.at[1, k], (c2, f)).start()
    for k in range(lines):
        giver = lax.rem(c2 // 2 + lines - k, lines) * 2 + c2 % 2
        remote(src, dst.at[giver], ss.at[1, k], rs.at[1, k], (c2, f)).wait()
        if k:
            remote(src, dst.at[c], ss.at[0, k], rs.at[0, k], (c2, f)).wait_send()


def line_devices(place, lines):
    c, f, c2, _, _ = place
    return [(lax.rem(c // 2 + k, lines) * 2 + c % 2, f) for k in range(1, lines)] + [(c2, f)]


def kv_body(lines, kv, cot, kv_o, cot_o, ss, rs, ts, tr):
    place = where_am_i()
    c, _, _, m, n = place
    greet(line_devices(place, lines) + [(c, m), (c, n)])
    spread_start(kv, kv_o, ss, rs, place, lines)
    items = [(cot, lambda g, rows: cot_o.at[g, rows])]
    tokens_start(items, ts, tr, place)
    kv_o[c] = kv[...]
    spread_finish(kv, kv_o, ss, rs, place, lines)
    tokens_finish(items, ts, tr, place)


def gates(gate, up, g_act):
    sg = jax.nn.sigmoid(gate)
    silu = gate * sg
    act = (silu * up).astype(bf16)
    g_gate = (g_act * up * (sg * (1.0 + gate * (1.0 - sg)))).astype(bf16)
    g_up = (g_act * silu).astype(bf16)
    return act, g_gate, g_up


def mid_body(x, cot, wg_h, wu_h, wd_h, gn_o, down_o, xg, wg, wu, wd, act, back, near, sums, far_in, ws, ss, rs, ns, nr):
    place = where_am_i()
    c, f, _, m, n = place
    far = (m + 2) % 4
    tok, width = x.shape
    loads = [
        pltpu.make_async_copy(src, dst, ws.at[j])
        for j, (src, dst) in enumerate(((wg_h, wg), (wu_h, wu), (wd_h, wd)))
    ]
    for copy in loads:
        copy.start()
    greet([(c, m), (c, n)])
    half = tok // 2
    own = remote(x, xg.at[f], ss.at[0], rs.at[0], (c, m))
    own.start()
    for j in range(2):
        rows = pl.ds(j * half, half)
        remote(x.at[rows], xg.at[f, rows], ss.at[1 + j], rs.at[1 + j], (c, n)).start()
    xg[f] = x[...]
    for copy in loads:
        copy.wait()
    own.wait()

    def forward(pair):
        at = pl.ds(pair * 2, 2)
        xs = xg[at].reshape(2 * tok, width)
        cs = cot[at].reshape(2 * tok, width)
        parts = gates(over_last(xs, wg[...]), over_last(xs, wu[...]), over_last(cs, wd[...]))
        for j, part in enumerate(parts):
            act[j] = part

    def backward():
        return plain_dot(act[1], wg[...]) + plain_dot(act[2], wu[...])

    def down(pair):
        down_o[pl.ds(pair * 2, 2)] = plain_dot(act[0], wd[...]).astype(bf16).reshape(2, tok, width)

    y = f // 2
    core = f % 2
    forward(y)
    for j in range(2):
        here = xg.at[n, pl.ds(j * half, half)]
        remote(here, here, ss.at[1 + j], rs.at[1 + j], (c, n)).wait_recv()
        remote(here, here, ss.at[3 + j], rs.at[3 + j], (c, m)).start()
    back[...] = backward().reshape(2, tok, width)
    near[0] = back[1 - core].astype(bf16)
    to_mate = remote(near.at[0], near.at[1], ns.at[0], nr.at[0], (c, m))
    to_mate.start()
    mine = back[core]
    down(y)
    gn_o[...] = mine
    for j in range(2):
        rows = pl.ds(j * half, half)
        remote(x.at[rows], xg.at[far, rows], ss.at[3 + j], rs.at[3 + j], (c, m)).wait_recv()
    forward(1 - y)
    back[...] = backward().reshape(2, tok, width)
    near[2] = back[1 - core].astype(bf16)
    first = remote(near.at[2], near.at[3], ns.at[1], nr.at[1], (c, m))
    first.start()
    first.wait()
    sums[...] = (back[core] + near[3].astype(f32)).astype(bf16)
    across = remote(sums, far_in, ns.at[2], nr.at[2], (c, n))
    across.start()
    down(1 - y)
    to_mate.wait()
    for j in range(2):
        rows = pl.ds(j * half, half)
        remote(x.at[rows], xg.at[f, rows], ss.at[1 + j], rs.at[1 + j], (c, n)).wait_send()
        remote(x.at[rows], xg.at[far, rows], ss.at[3 + j], rs.at[3 + j], (c, m)).wait_send()
    across.wait()
    gn_o[...] += near[1].astype(f32) + far_in[...].astype(f32)


def project_body(x, vec, x_o, vec_o, ss, rs, held, vs, vr):
    place = where_am_i()
    c, _, _, m, n = place
    far = (m + 2) % 4
    greet([(c, m), (c, n), (c, far)])
    items = [(x, lambda g, rows: x_o.at[g, rows])]
    tokens_start(items, ss, rs, place)
    copies = [remote(vec, held.at[k], vs.at[k], vr.at[k], (c, g)) for k, g in enumerate((m, n, far))]
    for copy in copies:
        copy.start()
    tokens_finish(items, ss, rs, place)
    total = vec[...]
    for k, copy in enumerate(copies):
        copy.wait()
        total = total + held[k]
    vec_o[...] = total


def dkv_body(ctx, part, ghl, sl, out, ghl_o, sl_o, held, ss, rs, gs, gr, as_, ar):
    place = where_am_i()
    c, f, _, m, n = place
    far = (m + 2) % 4
    peers = [lax.rem(c + k, ctx) for k in range(1, ctx)]
    greet([(p, f) for p in peers] + [(c, m), (c, n), (c, far)])
    for k, p in enumerate(peers):
        remote(part.at[p], held.at[k], ss.at[k], rs.at[k], (p, f)).start()
    for k, g in enumerate((n, far, m)):
        remote(sl.at[g], sl_o.at[f], as_.at[k], ar.at[k], (c, g)).start()
    items = [(ghl, lambda g, rows: ghl_o.at[g, rows])]
    tokens_start(items, gs, gr, place)
    sl_o[f] = sl[f]
    total = part[c].astype(f32)
    tokens_finish(items, gs, gr, place)
    for k, p in enumerate(peers):
        remote(part.at[p], held.at[k], ss.at[k], rs.at[k], (p, f)).wait()
        total = total + held[k].astype(f32)
    for k, g in enumerate((n, far, m)):
        remote(sl.at[g], sl_o.at[g], as_.at[k], ar.at[k], (c, g)).wait()
    out[...] = total


def over_last(a, b):
    return lax.dot_general(a, b, (((1,), (1,)), ((), ())), preferred_element_type=f32)


def over_first(a, b):
    return lax.dot_general(a, b, (((0,), (0,)), ((), ())), preferred_element_type=f32)


def plain_dot(a, b):
    return jnp.dot(a, b, preferred_element_type=f32)


def hidden_units(x, cot, wg, wu, wd):
    return gates(over_last(wg, x), over_last(wu, x), over_last(wd, cot))


def hidden_body(
    chunk, block, x_h, c_h, wg_h, wu_h, wd_h, og_h, ou_h, od_h, xs, cs, wg, wu, wd, acc, in_sem, w_sem, out_sem
):
    rows = x_h.shape[0]
    steps, blocks, held = rows // chunk, wg.shape[0] // block, xs.shape[0] // chunk
    loads = [
        pltpu.make_async_copy(src, dst, w_sem.at[j])
        for j, (src, dst) in enumerate(((wg_h, wg), (wu_h, wu), (wd_h, wd)))
    ]

    def tokens(i):
        src = pl.ds(pl.multiple_of(i * chunk, chunk), chunk)
        dst = pl.ds(pl.multiple_of(i % held * chunk, chunk), chunk)
        return [
            pltpu.make_async_copy(x_h.at[src], xs.at[dst], in_sem.at[i % held, 0]),
            pltpu.make_async_copy(c_h.at[src], cs.at[dst], in_sem.at[i % held, 1]),
        ]

    def results(b, slot):
        at = pl.ds(pl.multiple_of(b * block, 16), block)
        return [
            pltpu.make_async_copy(acc.at[slot, j], out.at[at], out_sem.at[slot, j])
            for j, out in enumerate((og_h, ou_h, od_h))
        ]

    resident = held == steps
    for copy in tokens(0) + loads:
        copy.start()
    for i in range(1, held if resident else 1):
        for copy in tokens(i):
            copy.start()
    for copy in loads:
        copy.wait()
    slots = acc.shape[0]

    @pl.loop(0, blocks)
    def _(b):
        slot = b % slots
        at = pl.ds(pl.multiple_of(b * block, 16), block)

        @pl.when(b >= slots)
        def _():
            for copy in results(b - slots, slot):
                copy.wait()

        @pl.loop(0, steps)
        def _(i):
            if resident:

                @pl.when(b == 0)
                def _():
                    for copy in tokens(i):
                        copy.wait()

            else:
                for copy in tokens(i):
                    copy.wait()

                @pl.when((i + 1 < steps) | (b + 1 < blocks))
                def _():
                    for copy in tokens(lax.rem(i + 1, steps)):
                        copy.start()

            t = pl.ds(pl.multiple_of(i % held * chunk, chunk), chunk)
            x, cot = xs[t], cs[t]
            act, g_gate, g_up = hidden_units(x, cot, wg[at], wu[at], wd[at])

            @pl.when(i == 0)
            def _():
                acc[slot, 0] = plain_dot(g_gate, x)
                acc[slot, 1] = plain_dot(g_up, x)
                acc[slot, 2] = plain_dot(act, cot)

            @pl.when(i > 0)
            def _():
                acc[slot, 0] += plain_dot(g_gate, x)
                acc[slot, 1] += plain_dot(g_up, x)
                acc[slot, 2] += plain_dot(act, cot)

        for copy in results(b, slot):
            copy.start()

    for b in range(max(0, blocks - slots), blocks):
        for copy in results(b, b % slots):
            copy.wait()


def hidden_grads(x, cot, wg, wu, wd):
    rows, width = x.shape
    units = wg.shape[0]
    chunk = math.gcd(rows, 1024)
    block = units // 2
    held = min(rows // chunk, 4)
    any_spec = pl.BlockSpec(memory_space=pl.ANY)
    dma = pltpu.SemaphoreType.DMA
    return pl.pallas_call(
        functools.partial(hidden_body, chunk, block),
        out_shape=(jax.ShapeDtypeStruct((units, width), f32),) * 3,
        in_specs=[any_spec] * 5,
        out_specs=(any_spec,) * 3,
        scratch_shapes=[pltpu.VMEM((held * chunk, width), bf16)] * 2
        + [pltpu.VMEM((units, width), bf16)] * 3
        + [pltpu.VMEM((2, 3, block, width), f32), dma((held, 2)), dma((3,)), dma((2, 3))],
        compiler_params=pltpu.CompilerParams(vmem_limit_bytes=60 << 20),
        cost_estimate=pl.CostEstimate(
            flops=12 * rows * width * units, bytes_accessed=4 * rows * width + 18 * units * width, transcendentals=0
        ),
        name="hidden_grads",
    )(x, cot, wg, wu, wd)


def shards(
    layer_input,
    seq_ids,
    positions,
    norm_gain,
    w_query,
    b_query,
    w_key,
    b_key,
    w_value,
    b_value,
    w_output,
    mlp_gain,
    w_gate,
    w_up,
    w_down,
    cotangent,
):
    tok = layer_input.shape[1]
    width = layer_input.shape[2]
    group = H // KV
    query_width = H * HD
    key_width = KV * HD
    score_scale = HD ** (-0.5)
    ctx = lax.axis_size("ctx")
    fsdp = lax.axis_size("fsdp")
    depth = width // fsdp
    lines = ctx // 2
    c, f = lax.axis_index("ctx"), lax.axis_index("fsdp")
    seq_length = ctx * tok
    dma = pltpu.SemaphoreType.DMA
    sds = jax.ShapeDtypeStruct
    input_rows = layer_input[0]
    grad_out = cotangent[0]
    own_segment = seq_ids[0]
    own_positions = positions[0]
    query_rows = c * tok + jnp.arange(tok, dtype=jnp.int32)

    cot_all = lax.all_gather(grad_out, ("ctx", "fsdp"), axis=0, tiled=True)

    def padded(v):
        return jnp.pad(v, (0, 256 - v.shape[0]))

    small = jnp.stack([padded(v) for v in (norm_gain, mlp_gain, b_query, b_key, b_value)])
    small = jnp.pad(small, ((0, 11), (0, 0)))
    seg_tile = jnp.broadcast_to(own_segment[None], (8, tok))
    w_project, wo_full, small_all, seg_all = comm_call(
        functools.partial(front_body, ctx, depth),
        (
            sds((width, query_width + 2 * key_width), bf16),
            sds((query_width, width), bf16),
            sds((fsdp, 16, 256), bf16),
            sds((ctx, 8, tok), jnp.int32),
        ),
        gather_sems(4) + [dma((3,)), dma((3,)), dma((ctx - 1,)), dma((ctx - 1,))],
        0,
    )(w_query, w_key, w_value, w_output, small, seg_tile)
    all_segments = seg_all[:, 0].reshape(seq_length)
    small_all = small_all.astype(f32)
    gain_first = small_all[:, 0, :depth].reshape(width)
    gain_second = small_all[:, 1, :depth].reshape(width)
    kd = key_width // fsdp
    b_project = jnp.concatenate(
        [
            small_all[:, 2, :depth].reshape(query_width),
            small_all[:, 3, :kd].reshape(key_width),
            small_all[:, 4, :kd].reshape(key_width),
        ]
    )
    residual_in = input_rows.astype(f32)
    inverse_first = lax.rsqrt(jnp.mean(residual_in * residual_in, -1, keepdims=True) + EPSILON)
    normed_first = (residual_in * inverse_first * gain_first).astype(bf16)
    projected = jnp.dot(normed_first, w_project, preferred_element_type=f32) + b_project
    cosine, sine_table = rope_tables(own_positions, HD)
    query = rotate(projected[:, :query_width].reshape(tok, H, HD), cosine, sine_table)
    query = query.astype(bf16).reshape(tok, KV, group, HD)
    key_rot = rotate(
        projected[:, query_width : query_width + key_width].reshape(tok, KV, HD), cosine, sine_table
    )
    value_low = projected[:, query_width + key_width :].astype(bf16)
    key_value = jnp.concatenate([key_rot.astype(bf16).reshape(tok, key_width), value_low], 1)
    kv_all, cot_group = comm_call(
        functools.partial(kv_body, lines),
        (sds((ctx, tok, 2 * key_width), bf16), sds((fsdp, tok, width), bf16)),
        [dma((2, lines)), dma((2, lines))] + gather_sems(1),
        1,
    )(key_value, grad_out)
    kv_all = kv_all.reshape(seq_length, 2 * key_width)
    keys = kv_all[:, :key_width].reshape(seq_length, KV, HD)
    values = kv_all[:, key_width:].reshape(seq_length, KV, HD)
    key_rows = jnp.arange(seq_length, dtype=jnp.int32)
    allowed = (key_rows[None, :] <= query_rows[:, None]) & (all_segments[None, :] == own_segment[:, None])
    raw_scores = jnp.einsum("tkgd,nkd->kgtn", query, keys, preferred_element_type=f32) * score_scale
    highest = jnp.max(jnp.where(allowed, raw_scores, MASK_FILL), -1)
    exp_scores = jnp.where(allowed, jnp.exp(raw_scores - highest[..., None]), 0.0)
    running_sum = jnp.sum(exp_scores, -1)
    accumulated = jnp.einsum("kgtn,nkd->tkgd", exp_scores.astype(bf16), values, preferred_element_type=f32)
    log_total = highest + jnp.log(running_sum)
    attention = accumulated / jnp.transpose(running_sum, (2, 0, 1))[..., None]
    attention_low = attention.reshape(tok, query_width).astype(bf16)
    hidden_state = residual_in + jnp.dot(attention_low, wo_full, preferred_element_type=f32)
    inverse_second = lax.rsqrt(jnp.mean(hidden_state * hidden_state, -1, keepdims=True) + EPSILON)
    normed_second = (hidden_state * inverse_second * gain_second).astype(bf16)
    x_all = lax.all_gather(normed_second, ("ctx", "fsdp"), axis=0, tiled=True)
    units = w_down.shape[0]
    any_spec = pl.BlockSpec(memory_space=pltpu.HBM)
    wg_t, wu_t = w_gate.T, w_up.T
    grad_normed2, down_part = pl.pallas_call(
        mid_body,
        out_shape=(sds((tok, width), f32), sds((fsdp, tok, width), bf16)),
        in_specs=[VMEM, VMEM, any_spec, any_spec, any_spec],
        out_specs=(VMEM, VMEM),
        scratch_shapes=[pltpu.VMEM((fsdp, tok, width), bf16)]
        + [pltpu.VMEM((units, width), bf16)] * 3
        + [
            pltpu.VMEM((3, 2 * tok, units), bf16),
            pltpu.VMEM((2, tok, width), f32),
            pltpu.VMEM((4, tok, width), bf16),
            pltpu.VMEM((tok, width), bf16),
            pltpu.VMEM((tok, width), bf16),
            dma((3,)),
            dma((5,)),
            dma((5,)),
            dma((3,)),
            dma((3,)),
        ],
        compiler_params=pltpu.CompilerParams(
            collective_id=2, has_side_effects=True, vmem_limit_bytes=40 << 20
        ),
        cost_estimate=pl.CostEstimate(
            flops=12 * fsdp * tok * width * units, bytes_accessed=6 * units * width, transcendentals=0
        ),
        name="mid",
    )(normed_second, cot_group, wg_t, wu_t, w_down)
    down_part = down_part.reshape(fsdp * tok, width)
    down_out = lax.psum_scatter(down_part, "fsdp", scatter_dimension=0, tiled=True)
    down_out = down_out.astype(f32)
    block_out = (hidden_state + down_out).astype(bf16)[None]

    hidden_back, second_gain_grad = norm_back(hidden_state, inverse_second, gain_second, grad_normed2)
    grad_hidden = grad_out.astype(f32) + hidden_back
    grad_hidden_low = grad_hidden.astype(bf16)
    grad_attention = over_last(grad_hidden_low, wo_full).astype(bf16)
    grad_attention = grad_attention.reshape(tok, KV, group, HD)
    delta_rows = jnp.einsum("tkgd,tkgd->kgt", grad_attention.astype(f32), attention)
    probs = jnp.where(allowed, jnp.exp(raw_scores - log_total[..., None]), 0.0)
    grad_values = jnp.einsum("kgtn,tkgd->nkd", probs.astype(bf16), grad_attention, preferred_element_type=f32)
    grad_probs = jnp.einsum("tkgd,nkd->kgtn", grad_attention, values, preferred_element_type=f32)
    grad_scores = (probs * (grad_probs - delta_rows[..., None])).astype(bf16)
    grad_query = jnp.einsum("kgtn,nkd->tkgd", grad_scores, keys, preferred_element_type=f32) * score_scale
    grad_keys = jnp.einsum("kgtn,tkgd->nkd", grad_scores, query, preferred_element_type=f32) * score_scale
    grad_pairs = jnp.concatenate(
        [grad_keys.reshape(seq_length, key_width), grad_values.reshape(seq_length, key_width)], 1
    ).astype(bf16)
    slices = jnp.concatenate(
        [
            normed_first.reshape(tok, fsdp, depth).transpose(1, 0, 2),
            attention_low.reshape(tok, fsdp, depth).transpose(1, 0, 2),
        ],
        1,
    )
    grad_pairs, ghl_group, slice_group = comm_call(
        functools.partial(dkv_body, ctx),
        (
            sds((tok, 2 * key_width), f32),
            sds((fsdp, tok, width), bf16),
            sds((fsdp, 2 * tok, depth), bf16),
        ),
        [pltpu.VMEM((ctx - 1, tok, 2 * key_width), bf16), dma((ctx - 1,)), dma((ctx - 1,))]
        + gather_sems(1)
        + [dma((3,)), dma((3,))],
        4,
    )(grad_pairs.reshape(ctx, tok, 2 * key_width), grad_hidden_low, slices)
    grad_q_pre = (
        rotate_back(grad_query.reshape(tok, H, HD), cosine, sine_table).reshape(tok, query_width).astype(bf16)
    )
    grad_k_pre = (
        rotate_back(grad_pairs[:, :key_width].reshape(tok, KV, HD), cosine, sine_table)
        .reshape(tok, key_width)
        .astype(bf16)
    )
    grad_v_pre = grad_pairs[:, key_width:].astype(bf16)
    grad_project = jnp.concatenate([grad_q_pre, grad_k_pre, grad_v_pre], 1)
    grad_normed1 = over_last(grad_project, w_project)
    bias_grad = jnp.sum(grad_project.astype(f32), 0)
    input_back, first_gain_grad = norm_back(residual_in, inverse_first, gain_first, grad_normed1)
    input_grad = (grad_hidden + input_back).astype(bf16)[None]
    vectors = jnp.concatenate([first_gain_grad, second_gain_grad, bias_grad])
    vectors = jnp.pad(vectors, (0, 3072 - vectors.shape[0])).reshape(8, 384)
    gp_group, vectors = comm_call(
        project_body,
        (sds((fsdp, tok, grad_project.shape[1]), bf16), sds(vectors.shape, f32)),
        gather_sems(1) + [pltpu.VMEM((3,) + vectors.shape, f32), dma((3,)), dma((3,))],
        5,
    )(grad_project, vectors)
    gp_group = gp_group.reshape(fsdp * tok, grad_project.shape[1])
    vectors = vectors.reshape(3072)
    normed_slice = slice_group[:, :tok].reshape(fsdp * tok, depth)
    attention_slice = slice_group[:, tok:].reshape(fsdp * tok, depth)
    project_grad = over_first(normed_slice, gp_group)
    output_grad = over_first(attention_slice, ghl_group.reshape(fsdp * tok, width))

    def piece(start, size):
        share = size // fsdp
        return lax.dynamic_slice_in_dim(vectors, start + f * share, share, 0)

    columns = project_grad.shape[1] + width
    starts = ((0, width), (width, width), (2 * width, query_width), (2 * width + query_width, key_width),
              (2 * width + query_width + key_width, key_width))
    own = jnp.concatenate([piece(*at) for at in starts])
    own = jnp.pad(own, (0, columns - own.shape[0]))
    weight_grads = jnp.concatenate(
        [jnp.concatenate([project_grad, output_grad], 1), jnp.broadcast_to(own[None], (16, columns))], 0
    ).astype(bf16)
    weight_grads = lax.psum(weight_grads, "ctx")
    weight_grads = weight_grads.astype(f32)
    own = weight_grads[depth]
    weight_grads = weight_grads[:depth]
    ends = [0]
    for _, size in starts:
        ends.append(ends[-1] + size // fsdp)
    own = [own[ends[i] : ends[i + 1]] for i in range(5)]

    gate_grad, up_grad, down_grad = hidden_grads(x_all, cot_all, wg_t, wu_t, w_down)
    return (
        block_out,
        input_grad,
        own[0],
        weight_grads[:, :query_width],
        own[2],
        weight_grads[:, query_width : query_width + key_width],
        own[3],
        weight_grads[:, query_width + key_width : query_width + 2 * key_width],
        own[4],
        weight_grads[:, query_width + 2 * key_width :],
        own[1],
        gate_grad.T,
        up_grad.T,
        down_grad,
        log_total.reshape(H, tok)[None],
    )


def solution(mesh):
    in_specs = (
        P("fsdp", "ctx", None),
        P("fsdp", "ctx"),
        P("fsdp", "ctx"),
        P("fsdp"),
        P("fsdp", None),
        P("fsdp"),
        P("fsdp", None),
        P("fsdp"),
        P("fsdp", None),
        P("fsdp"),
        P("fsdp", None),
        P("fsdp"),
        P(None, "fsdp"),
        P(None, "fsdp"),
        P("fsdp", None),
        P("fsdp", "ctx", None),
    )
    out_specs = (
        P("fsdp", "ctx", None),
        P("fsdp", "ctx", None),
        P("fsdp"),
        P("fsdp", None),
        P("fsdp"),
        P("fsdp", None),
        P("fsdp"),
        P("fsdp", None),
        P("fsdp"),
        P("fsdp", None),
        P("fsdp"),
        P(None, "fsdp"),
        P(None, "fsdp"),
        P("fsdp", None),
        P("fsdp", None, "ctx"),
    )

    return jax.shard_map(shards, mesh=mesh, in_specs=in_specs, out_specs=out_specs, check_vma=False)
```

```python
import functools
import math

import jax
import jax.numpy as jnp
from jax import lax
from jax.experimental import pallas as pl
from jax.experimental.pallas import tpu as pltpu
from jax.sharding import PartitionSpec as P


H = 14
KV = 2
HD = 64


EPSILON = 1e-06
ROPE_BASE = 1000000.0
MASK_FILL = -1e30
MESH = pl.DeviceIdType.MESH
VMEM = pl.BlockSpec(memory_space=pltpu.VMEM)
f32 = jnp.float32
bf16 = jnp.bfloat16


def rope_tables(positions, head_dim):
    half = head_dim // 2
    freq = ROPE_BASE ** (-(jnp.arange(half, dtype=jnp.float32) * 2.0 / head_dim))
    angle = positions.astype(jnp.float32)[None, :] * freq[:, None]
    return jnp.cos(angle), jnp.sin(angle)


def remote(src, dst, send_sem, recv_sem, device):
    return pltpu.make_async_remote_copy(
        src_ref=src, dst_ref=dst, send_sem=send_sem, recv_sem=recv_sem, device_id=device,
        device_id_type=MESH,
    )


def where_am_i():
    c, f = lax.axis_index("ctx"), lax.axis_index("fsdp")
    c2 = c + 1 - 2 * (c % 2)
    m = f + 1 - 2 * (f % 2)
    n = (f + 2) % 4
    return c, f, c2, m, n


def greet(devices):
    barrier = pltpu.get_barrier_semaphore()
    for device in devices:
        pl.semaphore_signal(barrier, inc=1, device_id=device, device_id_type=MESH)
    pl.semaphore_wait(barrier, len(devices))


def gather_start(items, ss, rs, place):
    c, f, _, m, n = place
    h = c % 2
    for i, (src, dst) in enumerate(items):
        half = src.shape[0] // 2
        rows = pl.ds(h * half, half)
        remote(src.at[rows], dst(f).at[rows], ss.at[i, 1], rs.at[i, 1], (c, n)).start()
    for i, (src, dst) in enumerate(items):
        remote(src, dst(f), ss.at[i, 0], rs.at[i, 0], (c, m)).start()
        pltpu.make_async_copy(src, dst(f), ss.at[i, 5]).start()


def gather_finish(items, ss, rs, place):
    c, f, c2, m, n = place
    h = c % 2
    far = (m + 2) % 4
    for i, (src, dst) in enumerate(items):
        half = src.shape[0] // 2
        mine = dst(n).at[pl.ds(h * half, half)]
        remote(mine, mine, ss.at[i, 1], rs.at[i, 1], (c, n)).wait_recv()
        remote(mine, mine, ss.at[i, 2], rs.at[i, 2], (c2, f)).start()
        remote(mine, mine, ss.at[i, 3], rs.at[i, 3], (c, m)).start()
    for i, (src, dst) in enumerate(items):
        half = src.shape[0] // 2
        other = dst(n).at[pl.ds((1 - h) * half, half)]
        remote(other, other, ss.at[i, 2], rs.at[i, 2], (c2, f)).wait_recv()
        remote(other, other, ss.at[i, 4], rs.at[i, 4], (c, m)).start()
    for i, (src, dst) in enumerate(items):
        half = src.shape[0] // 2
        mine, other = pl.ds(h * half, half), pl.ds((1 - h) * half, half)
        remote(src, dst(m), ss.at[i, 0], rs.at[i, 0], (c, m)).wait()
        remote(src.at[mine], dst(f).at[mine], ss.at[i, 1], rs.at[i, 1], (c, n)).wait_send()
        remote(src.at[mine], dst(n).at[mine], ss.at[i, 2], rs.at[i, 2], (c2, f)).wait_send()
        remote(src.at[mine], dst(far).at[mine], ss.at[i, 3], rs.at[i, 3], (c, m)).wait()
        remote(src.at[other], dst(far).at[other], ss.at[i, 4], rs.at[i, 4], (c, m)).wait()
        pltpu.make_async_copy(src, dst(f), ss.at[i, 5]).wait()


def tokens_start(items, ss, rs, place):
    c, f, _, m, n = place
    for i, (src, dst) in enumerate(items):
        half = src.shape[0] // 2
        for j in range(2):
            rows = pl.ds(j * half, half)
            remote(src.at[rows], dst(f, rows), ss.at[i, 1 + j], rs.at[i, 1 + j], (c, n)).start()
    for i, (src, dst) in enumerate(items):
        rows = pl.ds(0, src.shape[0])
        remote(src, dst(f, rows), ss.at[i, 0], rs.at[i, 0], (c, m)).start()
        dst(f, rows)[...] = src[...]


def tokens_finish(items, ss, rs, place):
    c, f, _, m, n = place
    far = (m + 2) % 4
    for i, (src, dst) in enumerate(items):
        half = src.shape[0] // 2
        for j in range(2):
            here = dst(n, pl.ds(j * half, half))
            remote(here, here, ss.at[i, 1 + j], rs.at[i, 1 + j], (c, n)).wait_recv()
            remote(here, here, ss.at[i, 3 + j], rs.at[i, 3 + j], (c, m)).start()
    for i, (src, dst) in enumerate(items):
        half = src.shape[0] // 2
        remote(src, dst(m, pl.ds(0, src.shape[0])), ss.at[i, 0], rs.at[i, 0], (c, m)).wait()
        for j in range(2):
            rows = pl.ds(j * half, half)
            remote(src.at[rows], dst(f, rows), ss.at[i, 1 + j], rs.at[i, 1 + j], (c, n)).wait_send()
            remote(src.at[rows], dst(far, rows), ss.at[i, 3 + j], rs.at[i, 3 + j], (c, m)).wait()


def gather_sems(count):
    return [pltpu.SemaphoreType.DMA((count, 6)), pltpu.SemaphoreType.DMA((count, 6))]


def spread_start(src, dst, ss, rs, place, lines):
    c, f, c2, _, _ = place
    for k in range(1, lines):
        p = lax.rem(c // 2 + k, lines) * 2 + c % 2
        remote(src, dst.at[c], ss.at[0, k], rs.at[0, k], (p, f)).start()
    remote(src, dst.at[c], ss.at[1, 0], rs.at[1, 0], (c2, f)).start()


def spread_finish(src, dst, ss, rs, place, lines):
    c, f, c2, _, _ = place
    for k in range(1, lines):
        giver = lax.rem(c // 2 + lines - k, lines) * 2 + c % 2
        block = dst.at[giver]
        remote(block, block, ss.at[0, k], rs.at[0, k], (c2, f)).wait_recv()
        remote(block, block, ss.at[1, k], rs.at[1, k], (c2, f)).start()
    for k in range(lines):
        giver = lax.rem(c2 // 2 + lines - k, lines) * 2 + c2 % 2
        remote(src, dst.at[giver], ss.at[1, k], rs.at[1, k], (c2, f)).wait()
        if k:
            remote(src, dst.at[c], ss.at[0, k], rs.at[0, k], (c2, f)).wait_send()


def line_devices(place, lines):
    c, f, c2, _, _ = place
    return [(lax.rem(c // 2 + k, lines) * 2 + c % 2, f) for k in range(1, lines)] + [(c2, f)]


def gates(gate, up, g_act):
    sg = jax.nn.sigmoid(gate)
    silu = gate * sg
    act = (silu * up).astype(bf16)
    g_gate = (g_act * up * (sg * (1.0 + gate * (1.0 - sg)))).astype(bf16)
    g_up = (g_act * silu).astype(bf16)
    return act, g_gate, g_up


class Spread:
    def __init__(self, place, lines, x, group, full, sems):
        self.place, self.lines, self.x, self.group, self.full = place, lines, x, group, full
        self.half = x.shape[0] // 2
        self.line_s, self.line_r, self.pair_s, self.pair_r, self.y_s, self.y_r, self.mate_s, self.mate_r = sems

    def column(self, k):
        c = self.place[0]
        return lax.rem(c // 2 + self.lines - k, self.lines) * 2 + c % 2

    def ahead(self, k):
        c = self.place[0]
        return lax.rem(c // 2 + k, self.lines) * 2 + c % 2

    def each(self, first, act):
        if self.lines <= 4:
            for k in range(first, self.lines):
                act(k)
        else:
            pl.loop(first, self.lines)(act)

    def view(self, b, g, j):
        return self.full.at[b, g, pl.ds(j * self.half, self.half)]

    def source(self, way):
        _, _, _, _, n = self.place
        rows = pl.ds((0 if way == 0 else 1) * self.half, self.half)
        return self.x.at[rows] if way < 2 else self.group.at[n, rows]

    def slot(self, b, way):
        _, f, _, _, n = self.place
        return self.view(b, n if way == 2 else f, 0 if way == 0 else 1)

    def line(self, way, k):
        c, f, _, _, _ = self.place
        return remote(
            self.source(way), self.slot(c, way), self.line_s.at[way, k], self.line_r.at[way, k], (self.ahead(k), f)
        )

    def arrived(self, way, k):
        here = self.slot(self.column(k), way)
        f = self.place[1]
        return remote(here, here, self.line_s.at[way, k], self.line_r.at[way, k], (self.ahead(k), f))

    def pair(self, way, k):
        c, f, c2, _, _ = self.place
        here = self.slot(self.column(k), way) if not isinstance(k, int) or k else None
        src = self.source(way) if here is None else here
        dst = self.slot(c, way) if here is None else here
        return remote(src, dst, self.pair_s.at[way, k], self.pair_r.at[way, k], (c2, f))

    def other(self, k):
        b = self.column(k)
        return b + 1 - 2 * (b % 2)

    def paired(self, way, k):
        _, f, c2, _, _ = self.place
        here = self.slot(self.other(k), way)
        return remote(here, here, self.pair_s.at[way, k], self.pair_r.at[way, k], (c2, f))

    def block(self, side, k):
        return self.other(k) if side else self.column(k)

    def across(self, side, k):
        c, _, _, _, n = self.place
        here = self.slot(self.block(side, k), 0)
        return remote(here, here, self.y_s.at[side, k], self.y_r.at[side, k], (c, n))

    def crossed(self, side, k):
        c, _, _, _, n = self.place
        here = self.view(self.block(side, k), n, 0)
        return remote(here, here, self.y_s.at[side, k], self.y_r.at[side, k], (c, n))

    def hand(self, way, side, k):
        c, _, _, m, n = self.place
        b = self.block(side, k)
        here = self.view(b, n, 0) if way == 3 else self.slot(b, way)
        return remote(here, here, self.mate_s.at[way, side, k], self.mate_r.at[way, side, k], (c, m))

    def handed(self, way, side, k):
        c, _, _, m, _ = self.place
        far = (m + 2) % 4
        b = self.block(side, k)
        here = self.view(b, far if way > 1 else m, 1 if way in (1, 2) else 0)
        return remote(here, here, self.mate_s.at[way, side, k], self.mate_r.at[way, side, k], (c, m))

    def start(self, way):
        self.each(1, lambda k: self.line(way, k).start())
        self.pair(way, 0).start()

    def on_line(self, way):
        def act(k):
            self.arrived(way, k).wait_recv()
            self.pair(way, k).start()
            self.hand(way, 0, k).start()
            if way == 0:
                self.across(0, k).start()

        self.each(1, act)

    def on_pair(self, way):
        def act(k):
            self.paired(way, k).wait_recv()
            self.hand(way, 1, k).start()
            if way == 0:
                self.across(1, k).start()

        self.each(0, act)

    def on_y(self, side):
        def act(k):
            self.crossed(side, k).wait_recv()
            self.hand(3, side, k).start()

        self.each(1 - side, act)

    def finish(self):
        for way in range(3):
            self.each(1, lambda k: self.line(way, k).wait_send())
            self.each(0, lambda k: self.pair(way, k).wait_send())
        for side in range(2):
            self.each(1 - side, lambda k: self.across(side, k).wait_send())
            for way in range(4):
                self.each(1 - side, lambda k: self.hand(way, side, k).wait_send())
                self.each(1 - side, lambda k: self.handed(way, side, k).wait_recv())


def spread_sems(lines):
    dma = pltpu.SemaphoreType.DMA
    return [dma(shape) for shape in ((3, lines), (3, lines), (2, lines), (4, 2, lines)) for _ in range(2)]


def mid_body(
    lines, x, cot, hid, wg_h, wu_h, wd_h, gn_o, block_o, x_o,
    xg, wg, wu, wd, act, back, near, sums, far_in, ws, os, ss, rs, ns, nr, *spread
):
    place = where_am_i()
    c, f, _, m, n = place
    far = (m + 2) % 4
    tok, width = x.shape
    loads = [
        pltpu.make_async_copy(src, dst, ws.at[j])
        for j, (src, dst) in enumerate(((wg_h, wg), (wu_h, wu), (wd_h, wd)))
    ]
    for copy in loads:
        copy.start()
    greet(line_devices(place, lines) + [(c, m), (c, n)])
    half = tok // 2
    own = remote(x, xg.at[f], ss.at[0], rs.at[0], (c, m))
    own.start()
    for j in range(2):
        rows = pl.ds(j * half, half)
        remote(x.at[rows], xg.at[f, rows], ss.at[1 + j], rs.at[1 + j], (c, n)).start()
    everyone = Spread(place, lines, x, xg, x_o, spread)
    everyone.start(0)
    everyone.start(1)
    xg[f] = x[...]
    for copy in loads:
        copy.wait()
    own.wait()

    def forward(pair):
        at = pl.ds(pair * 2, 2)
        xs = xg[at].reshape(2 * tok, width)
        cs = cot[at].reshape(2 * tok, width)
        parts = gates(over_last(xs, wg[...]), over_last(xs, wu[...]), over_last(cs, wd[...]))
        for j, part in enumerate(parts):
            act[j] = part

    def backward():
        return plain_dot(act[1], wg[...]) + plain_dot(act[2], wu[...])

    def down():
        return plain_dot(act[0], wd[...])

    y = f // 2
    core = f % 2

    def swap(j):
        return remote(near.at[2 * j], near.at[2 * j + 1], ns.at[j], nr.at[j], (c, m))

    def give(j, value):
        back[...] = value.reshape(2, tok, width)
        near[2 * j] = back[1 - core].astype(bf16)
        swap(j).start()

    def cross(j):
        return remote(sums.at[j], far_in.at[j], ns.at[4 + j], nr.at[4 + j], (c, n))

    def send_over(j, j_swap):
        swap(j_swap).wait()
        sums[j] = (back[core] + near[2 * j_swap + 1].astype(f32)).astype(bf16)
        cross(j).start()

    forward(y)
    for j in range(2):
        here = xg.at[n, pl.ds(j * half, half)]
        remote(here, here, ss.at[1 + j], rs.at[1 + j], (c, n)).wait_recv()
        remote(here, here, ss.at[3 + j], rs.at[3 + j], (c, m)).start()
    everyone.start(2)
    give(0, backward())
    gn_o[...] = back[core]
    give(1, down())
    down_own = hid[...] + back[core]
    everyone.on_line(0)
    for j in range(2):
        rows = pl.ds(j * half, half)
        remote(x.at[rows], xg.at[far, rows], ss.at[3 + j], rs.at[3 + j], (c, m)).wait_recv()
    keep = pltpu.make_async_copy(xg, x_o.at[c], os)
    keep.start()
    forward(1 - y)
    give(2, backward())
    send_over(0, 2)
    everyone.on_line(1)
    give(3, down())
    send_over(1, 3)
    everyone.on_pair(0)
    everyone.on_pair(1)
    everyone.on_y(0)
    cross(0).wait()
    swap(0).wait()
    gn_o[...] += near[1].astype(f32) + far_in[0].astype(f32)
    everyone.on_line(2)
    cross(1).wait()
    swap(1).wait()
    block_o[...] = (down_own + near[3].astype(f32) + far_in[1].astype(f32)).astype(bf16)
    everyone.on_y(1)
    everyone.on_pair(2)
    for j in range(2):
        rows = pl.ds(j * half, half)
        remote(x.at[rows], xg.at[f, rows], ss.at[1 + j], rs.at[1 + j], (c, n)).wait_send()
        remote(x.at[rows], xg.at[far, rows], ss.at[3 + j], rs.at[3 + j], (c, m)).wait_send()
    keep.wait()
    everyone.finish()


def turn(values, cos, sin, size):
    half = size // 2
    pieces = []
    for at in range(0, values.shape[0], size):
        lead, trail = values[at : at + half], values[at + half : at + size]
        pieces += [lead * cos - trail * sin, trail * cos + lead * sin]
    return jnp.concatenate(pieces, 0)


def key_bias(first, count, c, pos):
    tok = pos.shape[1]
    keys = lax.broadcasted_iota(jnp.int32, (count, tok), 0) + first
    queries = lax.broadcasted_iota(jnp.int32, (count, tok), 1) + c * tok
    allowed = (keys <= queries) & (keys >= queries - pos[...])
    return jnp.where(allowed, 0.0, MASK_FILL)


def front_body(
    lines, step,
    inp, cot, v0, v1, v2, v3, v4, pos, cos_r, sin_r, wq, wk, wv, wo,
    wp_o, wo_o, gains_o, n1_o, q_o, kv_o, cot_o, att_o, lse_o, hid_o, n2_o,
    kv, small, small_g, ms, mr, gs, gr, ks, kr, ts, tr,
):
    place = where_am_i()
    c, f, _, m, n = place
    far = (m + 2) % 4
    greet(line_devices(place, lines) + [(c, m), (c, n), (c, far)])
    tok, _ = inp.shape
    depth, query_width = wq.shape
    key_width = wk.shape[1]
    group = H // KV
    scale = HD ** (-0.5)

    def rows(g):
        return pl.ds(pl.multiple_of(g * depth, 16), depth)

    small[...] = jnp.zeros_like(small)
    for k, v in enumerate((v0, v1, v2, v3, v4)):
        small[k : k + 1, : v.shape[0]] = v[...].astype(f32).reshape(1, v.shape[0])
    smalls = [remote(small, small_g.at[f], ms.at[k], mr.at[k], (c, g)) for k, g in enumerate((m, n, far))]
    for copy in smalls:
        copy.start()
    project = [
        (wq, lambda g: wp_o.at[rows(g), pl.ds(0, query_width)]),
        (wk, lambda g: wp_o.at[rows(g), pl.ds(query_width, key_width)]),
        (wv, lambda g: wp_o.at[rows(g), pl.ds(query_width + key_width, key_width)]),
    ]
    output = [(wo, lambda g: wo_o.at[rows(g)])]
    gather_start(project, gs.at[pl.ds(0, 3)], gr.at[pl.ds(0, 3)], place)
    values = inp[...].astype(f32)
    unit = values * lax.rsqrt(jnp.mean(values * values, -1, keepdims=True) + EPSILON)
    small_g[f] = small[...]
    for k, g in enumerate((m, n, far)):
        remote(small, small_g.at[g], ms.at[k], mr.at[k], (c, g)).wait()

    def vector(row, size):
        return jnp.concatenate([small_g[g, row : row + 1, :size] for g in range(4)], 1)

    gains_o[0:1] = vector(0, depth)
    gains_o[1:2] = vector(1, depth)
    bias = jnp.concatenate([vector(2, depth), vector(3, key_width // 4), vector(4, key_width // 4)], 1)
    normed = unit * gains_o[0:1]
    n1_o[...] = normed.T.astype(bf16)
    gather_start(output, gs.at[pl.ds(3, 1)], gr.at[pl.ds(3, 1)], place)
    gather_finish(project, gs.at[pl.ds(0, 3)], gr.at[pl.ds(0, 3)], place)
    projected = plain_dot(normed.astype(bf16), wp_o[...]) + bias
    cos, sin = cos_r[...], sin_r[...]
    keys = turn(projected[:, query_width : query_width + key_width].T, cos, sin, HD)
    kv[:, :key_width] = keys.T.astype(bf16)
    kv[:, key_width:] = projected[:, query_width + key_width :].astype(bf16)
    spread_start(kv, kv_o, ks, kr, place, lines)
    kv_o[c] = kv[...]
    q_o[...] = turn(projected[:, :query_width].T, cos, sin, HD).astype(bf16)
    items = [(cot, lambda g, at: cot_o.at[g, at])]
    tokens_start(items, ts, tr, place)
    gather_finish(output, gs.at[pl.ds(3, 1)], gr.at[pl.ds(3, 1)], place)
    spread_finish(kv, kv_o, ks, kr, place, lines)
    for g in range(KV):
        queries = heads(q_o, g, group, HD)

        def visit(i, state):
            highest, total, acc = state
            at = pl.ds(i * step, step)
            both = kv_o[at].reshape(step * tok, 2 * key_width)
            seen = both[:, g * HD : (g + 1) * HD]
            carried = both[:, key_width + g * HD : key_width + (g + 1) * HD]
            mask = key_bias(i * step * tok, step * tok, c, pos)
            scores = plain_dot(seen, queries) * scale + jnp.concatenate([mask] * group, 1)
            top = jnp.maximum(highest, jnp.max(scores, 0, keepdims=True))
            exps = jnp.exp(scores - top)
            shrink = jnp.exp(highest - top)
            total = total * shrink + jnp.sum(exps, 0, keepdims=True)
            acc = acc * shrink + over_first(carried, exps.astype(bf16))
            return top, total, acc

        state = (
            jnp.full((1, group * tok), MASK_FILL, f32),
            jnp.zeros((1, group * tok), f32),
            jnp.zeros((HD, group * tok), f32),
        )
        blocks = kv_o.shape[0] // step
        if blocks <= 2:
            for i in range(blocks):
                state = visit(i, state)
        else:
            state = lax.fori_loop(0, blocks, visit, state)
        highest, total, acc = state
        attention = acc / total
        logs = highest + jnp.log(total)
        for j in range(group):
            at = slice(j * tok, (j + 1) * tok)
            h = g * group + j
            att_o[h * HD : (h + 1) * HD] = attention[:, at]
            lse_o[h : h + 1] = logs[:, at]
    hidden = values + plain_dot(att_o[...].T.astype(bf16), wo_o[...])
    hid_o[...] = hidden
    inverse = lax.rsqrt(jnp.mean(hidden * hidden, -1, keepdims=True) + EPSILON)
    n2_o[...] = (hidden * inverse * gains_o[1:2]).astype(bf16)
    tokens_finish(items, ts, tr, place)


def heads(ref, g, group, size):
    return jnp.concatenate([ref[pl.ds((g * group + j) * size, size)] for j in range(group)], 1)


def turn_back(grads, cos, sin, size):
    half = size // 2
    pieces = []
    for at in range(0, grads.shape[0], size):
        lead, trail = grads[at : at + half], grads[at + half : at + size]
        pieces += [lead * cos + trail * sin, trail * cos - lead * sin]
    return jnp.concatenate(pieces, 0)


def norm_grad(values, gain, grads):
    inverse = lax.rsqrt(jnp.mean(values * values, -1, keepdims=True) + EPSILON)
    scaled = values * inverse
    weighted = grads * gain
    back = inverse * (weighted - scaled * jnp.mean(weighted * scaled, -1, keepdims=True))
    return back, jnp.sum(grads * scaled, 0, keepdims=True)


def back_body(
    ctx, step,
    gn, hid, gains, cot, wo, att_t, q_t, kv, pos, lse, cos_r, sin_r, n1_t, inp, wp,
    inp_o, sums_o,
    gh, do_t, part, dq, held, ghl, ghl_g, low_t, n1_g, low_g, gp, gp_g, vec, vec_g,
    ks, kr, ts, tr, as_, ar, vs, vr,
):
    place = where_am_i()
    c, f, _, m, n = place
    far = (m + 2) % 4
    peers = [lax.rem(c + k, ctx) for k in range(1, ctx)]
    greet([(p, f) for p in peers] + [(c, m), (c, n), (c, far)])
    tok, width = cot.shape
    group = H // KV
    depth = n1_g.shape[1]
    scale = HD ** (-0.5)

    def rows(g):
        return pl.ds(pl.multiple_of(g * depth, 16), depth)

    def swaps():
        return [
            remote(src.at[rows(g)], dst.at[f], as_.at[j, k], ar.at[j, k], (c, g))
            for j, (src, dst) in enumerate(((n1_t, n1_g), (low_t, low_g)))
            for k, g in enumerate((n, far, m))
        ]

    low_t[...] = att_t[...].astype(bf16)
    back, gain_two = norm_grad(hid[...], gains[1:2], gn[...])
    gh[...] = cot[...].astype(f32) + back
    ghl[...] = gh[...].astype(bf16)
    items = [(ghl, lambda g, at: ghl_g.at[g, at])]
    tokens_start(items, ts.at[0], tr.at[0], place)
    for copy in swaps():
        copy.start()
    n1_g[f] = n1_t[rows(f)]
    low_g[f] = low_t[rows(f)]
    do_t[...] = over_last(wo[...], ghl[...]).astype(bf16)
    key_width = KV * HD
    for g in range(KV):
        queries, grads = heads(q_t, g, group, HD), heads(do_t, g, group, HD)
        delta = jnp.sum(grads.astype(f32) * heads(att_t, g, group, HD), 0, keepdims=True)
        total = jnp.concatenate([lse[pl.ds(g * group + j, 1)] for j in range(group)], 1)

        @pl.loop(0, kv.shape[0] // step)
        def _(i):
            at = pl.ds(i * step, step)
            both = kv[at].reshape(step * tok, 2 * key_width)
            keys = both[:, g * HD : (g + 1) * HD]
            values = both[:, key_width + g * HD : key_width + (g + 1) * HD]
            bias = key_bias(i * step * tok, step * tok, c, pos)
            scores = plain_dot(keys, queries) * scale + jnp.concatenate([bias] * group, 1)
            probs = jnp.exp(scores - total)
            g_probs = plain_dot(values, grads)
            g_scores = (probs * (g_probs - delta)).astype(bf16)
            g_keys = over_last(g_scores, queries) * scale
            g_values = over_last(probs.astype(bf16), grads)
            part[at, :, g * HD : (g + 1) * HD] = g_keys.astype(bf16).reshape(step, tok, HD)
            part[at, :, key_width + g * HD : key_width + (g + 1) * HD] = g_values.astype(bf16).reshape(
                step, tok, HD
            )
            g_queries = over_first(keys, g_scores) * scale

            @pl.when(i == 0)
            def _():
                dq[g] = g_queries

            @pl.when(i > 0)
            def _():
                dq[g] += g_queries

    owners = [remote(part.at[p], held.at[k], ks.at[k], kr.at[k], (p, f)) for k, p in enumerate(peers)]
    for copy in owners:
        copy.start()
    tokens_finish(items, ts.at[0], tr.at[0], place)
    for copy in swaps():
        copy.wait()
    cos, sin = cos_r[...], sin_r[...]
    g_q = [
        turn_back(dq[g, :, j * tok : (j + 1) * tok], cos, sin, HD) for g in range(KV) for j in range(group)
    ]
    g_q = jnp.concatenate(g_q, 0)
    query_width = g_q.shape[0]
    gp[:, :query_width] = g_q.T.astype(bf16)
    columns = gp.shape[1]
    low_all = jnp.concatenate([low_g[g] for g in range(4)], 1)
    sums_o[pl.ds(0, depth), pl.ds(columns, width)] = plain_dot(low_all, ghl_g[...].reshape(4 * tok, width)).astype(
        bf16
    )
    pairs = part[c].astype(f32)
    for k, copy in enumerate(owners):
        copy.wait()
        pairs = pairs + held[k].astype(f32)
    g_k = turn_back(pairs[:, :key_width].T, cos, sin, HD)
    gp[:, query_width : query_width + key_width] = g_k.T.astype(bf16)
    gp[:, query_width + key_width :] = pairs[:, key_width:].astype(bf16)
    items = [(gp, lambda g, at: gp_g.at[g, at])]
    tokens_start(items, ts.at[1], tr.at[1], place)
    g_normed = over_last(gp[...], wp[...])
    values = inp[...].astype(f32)
    back, gain_one = norm_grad(values, gains[0:1], g_normed)
    inp_o[...] = (gh[...] + back).astype(bf16)
    vec[...] = jnp.zeros_like(vec)
    vec[0:1, :width] = gain_one
    vec[1:2, :width] = gain_two
    vec[2:3, :columns] = jnp.sum(gp[...].astype(f32), 0, keepdims=True)
    vectors = [remote(vec, vec_g.at[k], vs.at[k], vr.at[k], (c, g)) for k, g in enumerate((m, n, far))]
    for copy in vectors:
        copy.start()
    tokens_finish(items, ts.at[1], tr.at[1], place)
    n1_all = jnp.concatenate([n1_g[g] for g in range(4)], 1)
    sums_o[pl.ds(0, depth), pl.ds(0, columns)] = plain_dot(n1_all, gp_g[...].reshape(4 * tok, columns)).astype(bf16)
    total = vec[...]
    for k, copy in enumerate(vectors):
        copy.wait()
        total = total + vec_g[k]
    sums_o[pl.ds(depth, 16)] = jnp.concatenate([total, total], 0).astype(bf16)


def over_last(a, b):
    return lax.dot_general(a, b, (((1,), (1,)), ((), ())), preferred_element_type=f32)


def over_first(a, b):
    return lax.dot_general(a, b, (((0,), (0,)), ((), ())), preferred_element_type=f32)


def plain_dot(a, b):
    return jnp.dot(a, b, preferred_element_type=f32)


def hidden_units(x, cot, wg, wu, wd):
    return gates(over_last(wg, x), over_last(wu, x), over_last(wd, cot))


def hidden_body(
    chunk, block, x_h, c_h, wg_h, wu_h, wd_h, og_h, ou_h, od_h, xs, cs, wg, wu, wd, acc, in_sem, w_sem, out_sem
):
    rows = x_h.shape[0]
    steps, blocks, held = rows // chunk, wg.shape[0] // block, xs.shape[0] // chunk
    loads = [
        pltpu.make_async_copy(src, dst, w_sem.at[j])
        for j, (src, dst) in enumerate(((wg_h, wg), (wu_h, wu), (wd_h, wd)))
    ]

    def tokens(i):
        src = pl.ds(pl.multiple_of(i * chunk, chunk), chunk)
        dst = pl.ds(pl.multiple_of(i % held * chunk, chunk), chunk)
        return [
            pltpu.make_async_copy(x_h.at[src], xs.at[dst], in_sem.at[i % held, 0]),
            pltpu.make_async_copy(c_h.at[src], cs.at[dst], in_sem.at[i % held, 1]),
        ]

    def results(b, slot):
        at = pl.ds(pl.multiple_of(b * block, 16), block)
        return [
            pltpu.make_async_copy(acc.at[slot, j], out.at[at], out_sem.at[slot, j])
            for j, out in enumerate((og_h, ou_h, od_h))
        ]

    resident = held == steps
    for copy in tokens(0) + loads:
        copy.start()
    for i in range(1, held if resident else 1):
        for copy in tokens(i):
            copy.start()
    for copy in loads:
        copy.wait()
    slots = acc.shape[0]

    @pl.loop(0, blocks)
    def _(b):
        slot = b % slots
        at = pl.ds(pl.multiple_of(b * block, 16), block)

        @pl.when(b >= slots)
        def _():
            for copy in results(b - slots, slot):
                copy.wait()

        @pl.loop(0, steps)
        def _(i):
            if resident:

                @pl.when(b == 0)
                def _():
                    for copy in tokens(i):
                        copy.wait()

            else:
                for copy in tokens(i):
                    copy.wait()

                @pl.when((i + 1 < steps) | (b + 1 < blocks))
                def _():
                    for copy in tokens(lax.rem(i + 1, steps)):
                        copy.start()

            t = pl.ds(pl.multiple_of(i % held * chunk, chunk), chunk)
            x, cot = xs[t], cs[t]
            act, g_gate, g_up = hidden_units(x, cot, wg[at], wu[at], wd[at])

            @pl.when(i == 0)
            def _():
                acc[slot, 0] = plain_dot(g_gate, x)
                acc[slot, 1] = plain_dot(g_up, x)
                acc[slot, 2] = plain_dot(act, cot)

            @pl.when(i > 0)
            def _():
                acc[slot, 0] += plain_dot(g_gate, x)
                acc[slot, 1] += plain_dot(g_up, x)
                acc[slot, 2] += plain_dot(act, cot)

        for copy in results(b, slot):
            copy.start()

    for b in range(max(0, blocks - slots), blocks):
        for copy in results(b, b % slots):
            copy.wait()


def hidden_grads(x, cot, wg, wu, wd):
    rows, width = x.shape
    units = wg.shape[0]
    chunk = math.gcd(rows, 1024)
    block = units // 2
    held = min(rows // chunk, 4)
    any_spec = pl.BlockSpec(memory_space=pl.ANY)
    dma = pltpu.SemaphoreType.DMA
    return pl.pallas_call(
        functools.partial(hidden_body, chunk, block),
        out_shape=(jax.ShapeDtypeStruct((units, width), f32),) * 3,
        in_specs=[any_spec] * 5,
        out_specs=(any_spec,) * 3,
        scratch_shapes=[pltpu.VMEM((held * chunk, width), bf16)] * 2
        + [pltpu.VMEM((units, width), bf16)] * 3
        + [pltpu.VMEM((2, 3, block, width), f32), dma((held, 2)), dma((3,)), dma((2, 3))],
        compiler_params=pltpu.CompilerParams(vmem_limit_bytes=62 << 20),
        cost_estimate=pl.CostEstimate(
            flops=12 * rows * width * units, bytes_accessed=4 * rows * width + 18 * units * width, transcendentals=0
        ),
        name="hidden_grads",
    )(x, cot, wg, wu, wd)


def shards(
    layer_input,
    seq_ids,
    positions,
    norm_gain,
    w_query,
    b_query,
    w_key,
    b_key,
    w_value,
    b_value,
    w_output,
    mlp_gain,
    w_gate,
    w_up,
    w_down,
    cotangent,
):
    tok = layer_input.shape[1]
    width = layer_input.shape[2]
    group = H // KV
    query_width = H * HD
    key_width = KV * HD
    ctx = lax.axis_size("ctx")
    fsdp = lax.axis_size("fsdp")
    depth = width // fsdp
    lines = ctx // 2
    c, f = lax.axis_index("ctx"), lax.axis_index("fsdp")
    dma = pltpu.SemaphoreType.DMA
    sds = jax.ShapeDtypeStruct
    input_rows = layer_input[0]
    grad_out = cotangent[0]
    own_positions = positions[0]
    query_rows = c * tok + jnp.arange(tok, dtype=jnp.int32)

    cot_all = lax.all_gather(grad_out, ("ctx", "fsdp"), axis=0, tiled=True)

    cosine, sine_table = rope_tables(own_positions, HD)
    own_positions = own_positions[None]
    step = math.gcd(ctx, 4)
    columns = query_width + 2 * key_width
    hbm = pl.BlockSpec(memory_space=pltpu.HBM)
    (w_project, wo_full, gains, n1_t, q_t, kv_all, cot_group, att_t, log_total, hidden_state, normed_second) = (
        pl.pallas_call(
            functools.partial(front_body, lines, step),
            out_shape=(
                sds((width, columns), bf16),
                sds((query_width, width), bf16),
                sds((8, width), f32),
                sds((width, tok), bf16),
                sds((query_width, tok), bf16),
                sds((ctx, tok, 2 * key_width), bf16),
                sds((fsdp, tok, width), bf16),
                sds((query_width, tok), f32),
                sds((H, tok), f32),
                sds((tok, width), f32),
                sds((tok, width), bf16),
            ),
            in_specs=[VMEM] * 10 + [hbm] * 4,
            out_specs=(VMEM,) * 11,
            scratch_shapes=[
                pltpu.VMEM((tok, 2 * key_width), bf16),
                pltpu.VMEM((8, 256), f32),
                pltpu.VMEM((fsdp, 8, 256), f32),
                dma((3,)),
                dma((3,)),
            ]
            + gather_sems(4)
            + [dma((2, lines)), dma((2, lines))]
            + gather_sems(1),
            compiler_params=pltpu.CompilerParams(
                collective_id=0, has_side_effects=True, vmem_limit_bytes=62 << 20
            ),
            cost_estimate=pl.CostEstimate(flops=4 * 10**9, bytes_accessed=10**7, transcendentals=0),
            name="front",
        )(
            input_rows, grad_out, norm_gain, mlp_gain, b_query, b_key, b_value, own_positions, cosine, sine_table,
            w_query, w_key, w_value, w_output,
        )
    )
    units = w_down.shape[0]
    any_spec = pl.BlockSpec(memory_space=pltpu.HBM)
    wg_t, wu_t = w_gate.T, w_up.T
    grad_normed2, block_out, x_all = pl.pallas_call(
        functools.partial(mid_body, lines),
        out_shape=(
            sds((tok, width), f32),
            sds((tok, width), bf16),
            sds((ctx, fsdp, tok, width), bf16),
        ),
        in_specs=[VMEM, VMEM, VMEM, any_spec, any_spec, any_spec],
        out_specs=(VMEM, VMEM, any_spec),
        scratch_shapes=[pltpu.VMEM((fsdp, tok, width), bf16)]
        + [pltpu.VMEM((units, width), bf16)] * 3
        + [
            pltpu.VMEM((3, 2 * tok, units), bf16),
            pltpu.VMEM((2, tok, width), f32),
            pltpu.VMEM((8, tok, width), bf16),
            pltpu.VMEM((2, tok, width), bf16),
            pltpu.VMEM((2, tok, width), bf16),
            dma((3,)),
            dma,
            dma((5,)),
            dma((5,)),
            dma((6,)),
            dma((6,)),
        ]
        + spread_sems(lines),
        compiler_params=pltpu.CompilerParams(
            collective_id=2, has_side_effects=True, vmem_limit_bytes=62 << 20
        ),
        cost_estimate=pl.CostEstimate(
            flops=12 * fsdp * tok * width * units, bytes_accessed=6 * units * width, transcendentals=0
        ),
        name="mid",
    )(normed_second, cot_group, hidden_state, wg_t, wu_t, w_down)
    block_out = block_out[None]
    x_all = x_all.reshape(ctx * fsdp * tok, width)
    params = pltpu.CompilerParams(collective_id=3, has_side_effects=True, vmem_limit_bytes=62 << 20)
    input_grad, weight_grads = pl.pallas_call(
        functools.partial(back_body, ctx, step),
        out_shape=(sds((tok, width), bf16), sds((depth + 16, columns + width), bf16)),
        in_specs=[VMEM] * 15,
        out_specs=(VMEM, VMEM),
        scratch_shapes=[
            pltpu.VMEM((tok, width), f32),
            pltpu.VMEM((query_width, tok), bf16),
            pltpu.VMEM((ctx, tok, 2 * key_width), bf16),
            pltpu.VMEM((KV, HD, group * tok), f32),
            pltpu.VMEM((ctx - 1, tok, 2 * key_width), bf16),
            pltpu.VMEM((tok, width), bf16),
            pltpu.VMEM((fsdp, tok, width), bf16),
            pltpu.VMEM((query_width, tok), bf16),
            pltpu.VMEM((fsdp, depth, tok), bf16),
            pltpu.VMEM((fsdp, depth, tok), bf16),
            pltpu.VMEM((tok, columns), bf16),
            pltpu.VMEM((fsdp, tok, columns), bf16),
            pltpu.VMEM((8, columns + width), f32),
            pltpu.VMEM((3, 8, columns + width), f32),
            dma((ctx - 1,)),
            dma((ctx - 1,)),
            dma((2, 1, 6)),
            dma((2, 1, 6)),
            dma((2, 3)),
            dma((2, 3)),
            dma((3,)),
            dma((3,)),
        ],
        compiler_params=params,
        cost_estimate=pl.CostEstimate(flops=10**10, bytes_accessed=10**7, transcendentals=0),
        name="back",
    )(
        grad_normed2,
        hidden_state,
        gains,
        grad_out,
        wo_full,
        att_t,
        q_t,
        kv_all,
        own_positions,
        log_total,
        cosine,
        sine_table,
        n1_t,
        input_rows,
        w_project,
    )
    input_grad = input_grad[None]
    weight_grads = lax.psum(weight_grads, "ctx")
    weight_grads = weight_grads.astype(f32)
    starts = ((0, 0, width), (1, 0, width), (2, 0, query_width), (2, query_width, key_width),
              (2, query_width + key_width, key_width))

    def piece(row, start, size):
        share = size // fsdp
        return lax.dynamic_slice_in_dim(weight_grads[depth + row], start + f * share, share, 0)

    own = [piece(*at) for at in starts]
    weight_grads = weight_grads[:depth]

    gate_grad, up_grad, down_grad = hidden_grads(x_all, cot_all, wg_t, wu_t, w_down)
    return (
        block_out,
        input_grad,
        own[0],
        weight_grads[:, :query_width],
        own[2],
        weight_grads[:, query_width : query_width + key_width],
        own[3],
        weight_grads[:, query_width + key_width : query_width + 2 * key_width],
        own[4],
        weight_grads[:, query_width + 2 * key_width :],
        own[1],
        gate_grad.T,
        up_grad.T,
        down_grad,
        log_total[None],
    )


def solution(mesh):
    in_specs = (
        P("fsdp", "ctx", None),
        P("fsdp", "ctx"),
        P("fsdp", "ctx"),
        P("fsdp"),
        P("fsdp", None),
        P("fsdp"),
        P("fsdp", None),
        P("fsdp"),
        P("fsdp", None),
        P("fsdp"),
        P("fsdp", None),
        P("fsdp"),
        P(None, "fsdp"),
        P(None, "fsdp"),
        P("fsdp", None),
        P("fsdp", "ctx", None),
    )
    out_specs = (
        P("fsdp", "ctx", None),
        P("fsdp", "ctx", None),
        P("fsdp"),
        P("fsdp", None),
        P("fsdp"),
        P("fsdp", None),
        P("fsdp"),
        P("fsdp", None),
        P("fsdp"),
        P("fsdp", None),
        P("fsdp"),
        P(None, "fsdp"),
        P(None, "fsdp"),
        P("fsdp", None),
        P("fsdp", None, "ctx"),
    )

    return jax.shard_map(shards, mesh=mesh, in_specs=in_specs, out_specs=out_specs, check_vma=False)
```

```python
import functools
import math

import jax
import jax.numpy as jnp
from jax import lax
from jax.experimental import pallas as pl
from jax.experimental.pallas import tpu as pltpu
from jax.sharding import PartitionSpec as P

H = 14
KV = 2
HD = 64


EPSILON = 1e-06
ROPE_BASE = 1000000.0
MASK_FILL = -1e30
MESH = pl.DeviceIdType.MESH
VMEM = pl.BlockSpec(memory_space=pltpu.VMEM)
f32 = jnp.float32
bf16 = jnp.bfloat16


def rope_tables(positions, head_dim):
    half = head_dim // 2
    freq = ROPE_BASE ** (-(jnp.arange(half, dtype=jnp.float32) * 2.0 / head_dim))
    angle = positions.astype(jnp.float32)[None, :] * freq[:, None]
    return jnp.cos(angle), jnp.sin(angle)


def remote(src, dst, send_sem, recv_sem, device):
    return pltpu.make_async_remote_copy(
        src_ref=src, dst_ref=dst, send_sem=send_sem, recv_sem=recv_sem, device_id=device,
        device_id_type=MESH,
    )


def where_am_i():
    c, f = lax.axis_index("ctx"), lax.axis_index("fsdp")
    c2 = c + 1 - 2 * (c % 2)
    m = f + 1 - 2 * (f % 2)
    n = (f + 2) % 4
    return c, f, c2, m, n


def greet(devices):
    barrier = pltpu.get_barrier_semaphore()
    for device in devices:
        pl.semaphore_signal(barrier, inc=1, device_id=device, device_id_type=MESH)
    pl.semaphore_wait(barrier, len(devices))


def gather_start(items, ss, rs, place):
    c, f, c2, m, n = place
    h = c % 2
    for i, (src, dst) in enumerate(items):
        half = src.shape[0] // 2
        rows = pl.ds(h * half, half)
        remote(src.at[rows], dst(f).at[rows], ss.at[i, 1], rs.at[i, 1], (c, n)).start()
    for i, (src, dst) in enumerate(items):
        remote(src, dst(f), ss.at[i, 0], rs.at[i, 0], (c, m)).start()
        pltpu.make_async_copy(src, dst(f), ss.at[i, 5]).start()


def gather_finish(items, ss, rs, place):
    c, f, c2, m, n = place
    h = c % 2
    far = (m + 2) % 4
    for i, (src, dst) in enumerate(items):
        half = src.shape[0] // 2
        mine = dst(n).at[pl.ds(h * half, half)]
        remote(mine, mine, ss.at[i, 1], rs.at[i, 1], (c, n)).wait_recv()
        remote(mine, mine, ss.at[i, 2], rs.at[i, 2], (c2, f)).start()
        remote(mine, mine, ss.at[i, 3], rs.at[i, 3], (c, m)).start()
    for i, (src, dst) in enumerate(items):
        half = src.shape[0] // 2
        other = dst(n).at[pl.ds((1 - h) * half, half)]
        remote(other, other, ss.at[i, 2], rs.at[i, 2], (c2, f)).wait_recv()
        remote(other, other, ss.at[i, 4], rs.at[i, 4], (c, m)).start()
    for i, (src, dst) in enumerate(items):
        half = src.shape[0] // 2
        mine, other = pl.ds(h * half, half), pl.ds((1 - h) * half, half)
        remote(src, dst(m), ss.at[i, 0], rs.at[i, 0], (c, m)).wait()
        remote(src.at[mine], dst(f).at[mine], ss.at[i, 1], rs.at[i, 1], (c, n)).wait_send()
        remote(src.at[mine], dst(n).at[mine], ss.at[i, 2], rs.at[i, 2], (c2, f)).wait_send()
        remote(src.at[mine], dst(far).at[mine], ss.at[i, 3], rs.at[i, 3], (c, m)).wait()
        remote(src.at[other], dst(far).at[other], ss.at[i, 4], rs.at[i, 4], (c, m)).wait()
        pltpu.make_async_copy(src, dst(f), ss.at[i, 5]).wait()


def tokens_start(items, ss, rs, place):
    c, f, c2, m, n = place
    for i, (src, dst) in enumerate(items):
        half = src.shape[0] // 2
        for j in range(2):
            rows = pl.ds(j * half, half)
            remote(src.at[rows], dst(f, rows), ss.at[i, 1 + j], rs.at[i, 1 + j], (c, n)).start()
    for i, (src, dst) in enumerate(items):
        rows = pl.ds(0, src.shape[0])
        remote(src, dst(f, rows), ss.at[i, 0], rs.at[i, 0], (c, m)).start()
        dst(f, rows)[...] = src[...]


def tokens_finish(items, ss, rs, place):
    c, f, c2, m, n = place
    far = (m + 2) % 4
    for i, (src, dst) in enumerate(items):
        half = src.shape[0] // 2
        for j in range(2):
            here = dst(n, pl.ds(j * half, half))
            remote(here, here, ss.at[i, 1 + j], rs.at[i, 1 + j], (c, n)).wait_recv()
            remote(here, here, ss.at[i, 3 + j], rs.at[i, 3 + j], (c, m)).start()
    for i, (src, dst) in enumerate(items):
        half = src.shape[0] // 2
        remote(src, dst(m, pl.ds(0, src.shape[0])), ss.at[i, 0], rs.at[i, 0], (c, m)).wait()
        for j in range(2):
            rows = pl.ds(j * half, half)
            remote(src.at[rows], dst(f, rows), ss.at[i, 1 + j], rs.at[i, 1 + j], (c, n)).wait_send()
            remote(src.at[rows], dst(far, rows), ss.at[i, 3 + j], rs.at[i, 3 + j], (c, m)).wait()


def gather_sems(count):
    return [pltpu.SemaphoreType.DMA((count, 6)), pltpu.SemaphoreType.DMA((count, 6))]


def staged_call(body, args, in_hbm, out_shape, out_hbm, scratch, ident, name, cost):
    hbm = pl.BlockSpec(memory_space=pltpu.HBM)
    staged_in = [i for i in range(len(args)) if i not in in_hbm]
    staged_out = [i for i in range(len(out_shape)) if i not in out_hbm]

    def kernel(*refs):
        ins, outs = list(refs[: len(args)]), list(refs[len(args) : len(args) + len(out_shape)])
        rest = list(refs[len(args) + len(out_shape) :])
        own, rest = rest[: len(scratch)], rest[len(scratch) :]
        in_sem, out_sem = rest[-2:]
        copies_in, copies_out = [], []
        for j, i in enumerate(staged_in):
            buffer = rest.pop(0)
            copies_in.append(pltpu.make_async_copy(ins[i], buffer, in_sem.at[j]))
            ins[i] = buffer
        for j, i in enumerate(staged_out):
            buffer = rest.pop(0)
            copies_out.append(pltpu.make_async_copy(buffer, outs[i], out_sem.at[j]))
            outs[i] = buffer
        for copy in copies_in:
            copy.start()

        def ready():
            for copy in copies_in:
                copy.wait()

        body(ready, *ins, *outs, *own)
        for copy in copies_out:
            copy.start()
        for copy in copies_out:
            copy.wait()

    buffers = [pltpu.VMEM(args[i].shape, args[i].dtype) for i in staged_in]
    buffers += [pltpu.VMEM(out_shape[i].shape, out_shape[i].dtype) for i in staged_out]
    sems = [pltpu.SemaphoreType.DMA((len(staged_in),)), pltpu.SemaphoreType.DMA((len(staged_out),))]
    return pl.pallas_call(
        kernel,
        out_shape=out_shape,
        in_specs=[hbm] * len(args),
        out_specs=(hbm,) * len(out_shape),
        scratch_shapes=scratch + buffers + sems,
        compiler_params=pltpu.CompilerParams(
            collective_id=ident, has_side_effects=True, vmem_limit_bytes=62 << 20
        ),
        cost_estimate=cost,
        name=name,
    )(*args)


def spread_start(src, dst, ss, rs, place, lines):
    c, f, c2, m, n = place
    for k in range(1, lines):
        p = lax.rem(c // 2 + k, lines) * 2 + c % 2
        remote(src, dst.at[c], ss.at[0, k], rs.at[0, k], (p, f)).start()
    remote(src, dst.at[c], ss.at[1, 0], rs.at[1, 0], (c2, f)).start()


def spread_finish(src, dst, ss, rs, place, lines):
    c, f, c2, m, n = place
    for k in range(1, lines):
        giver = lax.rem(c // 2 + lines - k, lines) * 2 + c % 2
        block = dst.at[giver]
        remote(block, block, ss.at[0, k], rs.at[0, k], (c2, f)).wait_recv()
        remote(block, block, ss.at[1, k], rs.at[1, k], (c2, f)).start()
    for k in range(lines):
        giver = lax.rem(c2 // 2 + lines - k, lines) * 2 + c2 % 2
        remote(src, dst.at[giver], ss.at[1, k], rs.at[1, k], (c2, f)).wait()
        if k:
            remote(src, dst.at[c], ss.at[0, k], rs.at[0, k], (c2, f)).wait_send()


def line_devices(place, lines):
    c, f, c2, m, n = place
    return [(lax.rem(c // 2 + k, lines) * 2 + c % 2, f) for k in range(1, lines)] + [(c2, f)]


def gates(gate, up, g_act):
    sg = jax.nn.sigmoid(gate)
    silu = gate * sg
    act = (silu * up).astype(bf16)
    g_gate = (g_act * up * (sg * (1.0 + gate * (1.0 - sg)))).astype(bf16)
    g_up = (g_act * silu).astype(bf16)
    return act, g_gate, g_up


class Spread:
    def __init__(self, place, lines, x, group, into, sems):
        self.place, self.lines, self.x, self.group, self.into = place, lines, x, group, into
        self.half = x.shape[0] // 2
        self.core = place[1] % 2
        self.line_s, self.line_r, self.pair_s, self.pair_r, self.y_s, self.y_r, self.mate_s, self.mate_r, self.own = sems

    def at(self, k):
        return lax.rem(self.place[0] // 2 + self.lines - k, self.lines)

    def each(self, first, act):
        if self.lines <= 4:
            for k in range(first, self.lines):
                act(k)
        else:
            pl.loop(first, self.lines)(act)

    def source(self, way):
        n = self.place[4]
        rows = pl.ds((0 if way == 0 else 1) * self.half, self.half)
        return self.x.at[rows] if way < 2 else self.group.at[n, rows]

    def slot(self, way, side, k, core=None):
        return self.into[(0, 1, 3, 2)[way]][side].at[self.at(k), self.core if core is None else core]

    def line(self, way, k):
        c, f = self.place[:2]
        sems = self.line_s.at[way, k], self.line_r.at[way, k]
        device = (lax.rem(c // 2 + k, self.lines) * 2 + c % 2, f)
        return remote(self.source(way), self.slot(way, 0, 0), *sems, device)

    def arrived(self, way, k):
        here = self.slot(way, 0, k)
        c, f, c2 = self.place[:3]
        return remote(here, here, self.line_s.at[way, k], self.line_r.at[way, k], (c2, f))

    def pair(self, way, k):
        c, f, c2 = self.place[:3]
        src = self.source(way) if isinstance(k, int) and k == 0 else self.slot(way, 0, k)
        return remote(src, self.slot(way, 1, k), self.pair_s.at[way, k], self.pair_r.at[way, k], (c2, f))

    def across(self, side, k):
        c, n = self.place[0], self.place[4]
        sems = self.y_s.at[side, k], self.y_r.at[side, k]
        return remote(self.slot(0, side, k), self.slot(3, side, k), *sems, (c, n))

    def hand(self, way, side, k, core=None):
        c, m = self.place[0], self.place[3]
        here = self.slot(way, side, k, core)
        return remote(here, here, self.mate_s.at[way, side, k], self.mate_r.at[way, side, k], (c, m))

    def lines_out(self, way):
        self.each(1, lambda k: self.line(way, k).start())

    def on_line(self, way, forward):
        def act(k):
            self.arrived(way, k).wait_recv()
            if forward:
                self.pair(way, k).start()
            self.hand(way, 0, k).start()

        if forward:
            self.pair(way, 0).start()
        self.each(1, act)

    def pairs_out(self, way):
        self.pair(way, 0).start()
        self.each(1, lambda k: self.pair(way, k).start())

    def on_pair(self, way):
        def act(k):
            self.pair(way, k).wait_recv()
            self.hand(way, 1, k).start()

        self.each(0, act)

    def cross(self, side):
        self.each(1 - side, lambda k: self.across(side, k).start())

    def on_y(self, side):
        def act(k):
            self.across(side, k).wait_recv()
            self.hand(3, side, k).start()

        self.each(1 - side, act)

    def keep(self, group, *parts):
        c, f = self.place[:2]
        copies = []
        for part in parts:
            pair = pl.ds((f // 2 if part < 2 else 1 - f // 2) * 2, 2)
            rows = pl.ds(part % 2 * self.half, self.half)
            into = self.into[part][0].at[c // 2]
            copies.append(pltpu.make_async_copy(group.at[pair, rows], into, self.own.at[part]))
        return copies

    def handed(self, way, side):
        self.each(1 - side, lambda k: self.hand(way, side, k).wait_send())
        self.each(1 - side, lambda k: self.hand(way, side, k, 1 - self.core).wait_recv())

    def finish_line(self, way):
        self.each(1, lambda k: self.line(way, k).wait_send())
        self.handed(way, 0)

    def finish_pair(self, way):
        self.each(0, lambda k: self.pair(way, k).wait_send())
        self.handed(way, 1)

    def finish_cross(self):
        for side in range(2):
            self.each(1 - side, lambda k: self.across(side, k).wait_send())
            self.handed(3, side)


def spread_sems(lines):
    dma = pltpu.SemaphoreType.DMA
    return [dma(shape) for shape in ((3, lines), (3, lines), (2, lines), (4, 2, lines)) for _ in range(2)] + [dma((4,))]


def mid_body(
    lines, ready, x, cot, own_cot, a0, a1, b0, hid, wg_h, wu_h, wd_h,
    gn_o, block_o, xg, b1_o, fa0_o, fa1_o, fb0_o, fb1_o, xa0_o,
    wg, wu, wd, act, back, near, sums, far_in, ws, ss, rs, ns, nr, *sems
):
    place = where_am_i()
    c, f, c2, m, n = place
    far = (m + 2) % 4
    tok, width = x.shape
    loads = [
        pltpu.make_async_copy(src, dst, ws.at[j])
        for j, (src, dst) in enumerate(((wg_h, wg), (wu_h, wu), (wd_h, wd)))
    ]
    for copy in loads:
        copy.start()
    greet(line_devices(place, lines) + [(c, m), (c, n)])
    ready()
    half = tok // 2
    own = remote(x, xg.at[f], ss.at[0], rs.at[0], (c, m))
    own.start()
    for j in range(2):
        rows = pl.ds(j * half, half)
        remote(x.at[rows], xg.at[f, rows], ss.at[1 + j], rs.at[1 + j], (c, n)).start()
    rest = Spread(place, lines, own_cot, cot, ((a0, a1), (b0, b1_o), (fa0_o, fa1_o), (fb0_o, fb1_o)), sems[:9])
    spread = Spread(place, lines, x, xg, ((xa0_o,),), sems[9:])
    rest.pairs_out(1)
    rest.lines_out(2)
    spread.lines_out(0)
    kept = rest.keep(cot, 2, 3)
    for copy in kept:
        copy.start()
    xg[f] = x[...]
    for copy in loads:
        copy.wait()
    own.wait()

    def forward(pair):
        at = pl.ds(pair * 2, 2)
        xs = xg[at].reshape(2 * tok, width)
        cs = cot[at].reshape(2 * tok, width)
        parts = gates(over_last(xs, wg[...]), over_last(xs, wu[...]), over_last(cs, wd[...]))
        for j, part in enumerate(parts):
            act[j] = part

    def backward():
        return plain_dot(act[1], wg[...]) + plain_dot(act[2], wu[...])

    def down():
        return plain_dot(act[0], wd[...])

    y = f // 2
    core = f % 2

    def swap(j):
        return remote(near.at[2 * j], near.at[2 * j + 1], ns.at[j], nr.at[j], (c, m))

    def give(j, value):
        back[...] = value.reshape(2, tok, width)
        near[2 * j] = back[1 - core].astype(bf16)
        swap(j).start()

    def cross(j):
        return remote(sums.at[j], far_in.at[j], ns.at[4 + j], nr.at[4 + j], (c, n))

    def send_over(j, j_swap):
        swap(j_swap).wait()
        sums[j] = (back[core] + near[2 * j_swap + 1].astype(f32)).astype(bf16)
        cross(j).start()

    forward(y)
    for j in range(2):
        here = xg.at[n, pl.ds(j * half, half)]
        remote(here, here, ss.at[1 + j], rs.at[1 + j], (c, n)).wait_recv()
        remote(here, here, ss.at[3 + j], rs.at[3 + j], (c, m)).start()
    rest.cross(0)
    give(0, backward())
    gn_o[...] = back[core]
    give(1, down())
    down_own = hid[...] + back[core]
    for j in range(2):
        rows = pl.ds(j * half, half)
        remote(x.at[rows], xg.at[far, rows], ss.at[3 + j], rs.at[3 + j], (c, m)).wait_recv()
    kept += spread.keep(xg, 0)
    kept[-1].start()
    forward(1 - y)
    give(2, backward())
    send_over(0, 2)
    rest.on_line(2, True)
    give(3, down())
    send_over(1, 3)
    rest.cross(1)
    rest.on_y(0)
    rest.on_pair(1)
    cross(0).wait()
    swap(0).wait()
    gn_o[...] += near[1].astype(f32) + far_in[0].astype(f32)
    cross(1).wait()
    swap(1).wait()
    block_o[...] = (down_own + near[3].astype(f32) + far_in[1].astype(f32)).astype(bf16)
    spread.on_line(0, False)
    rest.on_pair(2)
    rest.on_y(1)
    for j in range(2):
        rows = pl.ds(j * half, half)
        remote(x.at[rows], xg.at[f, rows], ss.at[1 + j], rs.at[1 + j], (c, n)).wait_send()
        remote(x.at[rows], xg.at[far, rows], ss.at[3 + j], rs.at[3 + j], (c, m)).wait_send()
    for copy in kept:
        copy.wait()
    rest.finish_pair(1)
    rest.finish_line(2)
    rest.finish_pair(2)
    rest.finish_cross()
    spread.finish_line(0)


def turn(values, cos, sin, size):
    half = size // 2
    pieces = []
    for at in range(0, values.shape[0], size):
        lead, trail = values[at : at + half], values[at + half : at + size]
        pieces += [lead * cos - trail * sin, trail * cos + lead * sin]
    return jnp.concatenate(pieces, 0)


def key_bias(first, count, c, pos):
    tok = pos.shape[1]
    keys = lax.broadcasted_iota(jnp.int32, (count, tok), 0) + first
    queries = lax.broadcasted_iota(jnp.int32, (count, tok), 1) + c * tok
    allowed = (keys <= queries) & (keys >= queries - pos[...])
    return jnp.where(allowed, 0.0, MASK_FILL)


def front_body(
    lines, step, ready,
    inp, cot, v0, v1, v2, v3, v4, pos, cos_r, sin_r, wq, wk, wv, wo,
    wp_o, wo_o, gains_o, n1_o, q_o, kv_o, cot_o, att_o, lse_o, hid_o, n2_o, a0_o, a1_o, b0_o,
    kv, small, small_g, ms, mr, gs, gr, ks, kr, ts, tr, *sems
):
    place = where_am_i()
    c, f, c2, m, n = place
    far = (m + 2) % 4
    greet(line_devices(place, lines) + [(c, m), (c, n), (c, far)])
    tok, width = inp.shape
    depth, query_width = wq.shape
    key_width = wk.shape[1]
    group = H // KV
    scale = HD ** (-0.5)

    def rows(g):
        return pl.ds(pl.multiple_of(g * depth, 16), depth)

    project = [
        (wq, lambda g: wp_o.at[rows(g), pl.ds(0, query_width)]),
        (wk, lambda g: wp_o.at[rows(g), pl.ds(query_width, key_width)]),
        (wv, lambda g: wp_o.at[rows(g), pl.ds(query_width + key_width, key_width)]),
    ]
    output = [(wo, lambda g: wo_o.at[rows(g)])]
    gather_start(project, gs.at[pl.ds(0, 3)], gr.at[pl.ds(0, 3)], place)
    ready()
    small[...] = jnp.zeros_like(small)
    for k, v in enumerate((v0, v1, v2, v3, v4)):
        small[k : k + 1, : v.shape[0]] = v[...].astype(f32).reshape(1, v.shape[0])
    smalls = [remote(small, small_g.at[f], ms.at[k], mr.at[k], (c, g)) for k, g in enumerate((m, n, far))]
    for copy in smalls:
        copy.start()
    spread = Spread(place, lines, cot, cot_o, ((a0_o, a1_o), (b0_o,)), sems)
    spread.lines_out(0)
    values = inp[...].astype(f32)
    unit = values * lax.rsqrt(jnp.mean(values * values, -1, keepdims=True) + EPSILON)
    small_g[f] = small[...]
    for k, g in enumerate((m, n, far)):
        remote(small, small_g.at[g], ms.at[k], mr.at[k], (c, g)).wait()

    def vector(row, size):
        return jnp.concatenate([small_g[g, row : row + 1, :size] for g in range(4)], 1)

    gains_o[0:1] = vector(0, depth)
    gains_o[1:2] = vector(1, depth)
    bias = jnp.concatenate([vector(2, depth), vector(3, key_width // 4), vector(4, key_width // 4)], 1)
    normed = unit * gains_o[0:1]
    n1_o[...] = normed.T.astype(bf16)
    gather_start(output, gs.at[pl.ds(3, 1)], gr.at[pl.ds(3, 1)], place)
    gather_finish(project, gs.at[pl.ds(0, 3)], gr.at[pl.ds(0, 3)], place)
    projected = plain_dot(normed.astype(bf16), wp_o[...]) + bias
    cos, sin = cos_r[...], sin_r[...]
    keys = turn(projected[:, query_width : query_width + key_width].T, cos, sin, HD)
    kv[:, :key_width] = keys.T.astype(bf16)
    kv[:, key_width:] = projected[:, query_width + key_width :].astype(bf16)
    spread_start(kv, kv_o, ks, kr, place, lines)
    kv_o[c] = kv[...]
    q_o[...] = turn(projected[:, :query_width].T, cos, sin, HD).astype(bf16)
    items = [(cot, lambda g, at: cot_o.at[g, at])]
    tokens_start(items, ts, tr, place)
    gather_finish(output, gs.at[pl.ds(3, 1)], gr.at[pl.ds(3, 1)], place)
    spread_finish(kv, kv_o, ks, kr, place, lines)
    spread.lines_out(1)
    spread.on_line(0, True)
    for g in range(KV):
        if g == 1:
            spread.on_pair(0)
        queries = heads(q_o, g, group, HD)

        def visit(i, state):
            highest, total, acc = state
            at = pl.ds(i * step, step)
            both = kv_o[at].reshape(step * tok, 2 * key_width)
            seen = both[:, g * HD : (g + 1) * HD]
            carried = both[:, key_width + g * HD : key_width + (g + 1) * HD]
            mask = key_bias(i * step * tok, step * tok, c, pos)
            scores = plain_dot(seen, queries) * scale + jnp.concatenate([mask] * group, 1)
            top = jnp.maximum(highest, jnp.max(scores, 0, keepdims=True))
            exps = jnp.exp(scores - top)
            shrink = jnp.exp(highest - top)
            total = total * shrink + jnp.sum(exps, 0, keepdims=True)
            acc = acc * shrink + over_first(carried, exps.astype(bf16))
            return top, total, acc

        state = (
            jnp.full((1, group * tok), MASK_FILL, f32),
            jnp.zeros((1, group * tok), f32),
            jnp.zeros((HD, group * tok), f32),
        )
        blocks = kv_o.shape[0] // step
        if blocks <= 2:
            for i in range(blocks):
                state = visit(i, state)
        else:
            state = lax.fori_loop(0, blocks, visit, state)
        highest, total, acc = state
        attention = acc / total
        logs = highest + jnp.log(total)
        for j in range(group):
            at = slice(j * tok, (j + 1) * tok)
            h = g * group + j
            att_o[h * HD : (h + 1) * HD] = attention[:, at]
            lse_o[h : h + 1] = logs[:, at]
    hidden = values + plain_dot(att_o[...].T.astype(bf16), wo_o[...])
    hid_o[...] = hidden
    inverse = lax.rsqrt(jnp.mean(hidden * hidden, -1, keepdims=True) + EPSILON)
    n2_o[...] = (hidden * inverse * gains_o[1:2]).astype(bf16)
    tokens_finish(items, ts, tr, place)
    kept = spread.keep(cot_o, 0, 1)
    for copy in kept:
        copy.start()
    spread.on_line(1, False)
    spread.finish_line(0)
    spread.finish_pair(0)
    spread.finish_line(1)
    for copy in kept:
        copy.wait()


def heads(ref, g, group, size):
    return jnp.concatenate([ref[pl.ds((g * group + j) * size, size)] for j in range(group)], 1)


def turn_back(grads, cos, sin, size):
    half = size // 2
    pieces = []
    for at in range(0, grads.shape[0], size):
        lead, trail = grads[at : at + half], grads[at + half : at + size]
        pieces += [lead * cos + trail * sin, trail * cos - lead * sin]
    return jnp.concatenate(pieces, 0)


def norm_grad(values, gain, grads):
    inverse = lax.rsqrt(jnp.mean(values * values, -1, keepdims=True) + EPSILON)
    scaled = values * inverse
    weighted = grads * gain
    back = inverse * (weighted - scaled * jnp.mean(weighted * scaled, -1, keepdims=True))
    return back, jnp.sum(grads * scaled, 0, keepdims=True)


class Total:
    def __init__(self, place, lines, pay, total, a_in, a_sum, a_line, b_line, b_sum, b_in, ss, rs):
        self.place, self.lines, self.pay, self.total = place, lines, pay, total
        self.a_in, self.a_sum, self.a_line, self.b_line, self.b_sum, self.b_in = a_in, a_sum, a_line, b_line, b_sum, b_in
        self.ss, self.rs = ss, rs
        self.p, self.x = place[0] // 2, place[0] % 2
        self.height, self.half = pay.shape[0] // lines, pay.shape[1] // 2
        self.wide = pl.ds(self.half, self.half)

    def rows(self, p):
        return pl.ds(pl.multiple_of(p * self.height, 16), self.height)

    def columns(self, h, x):
        return pl.ds(pl.multiple_of(h * self.half + x * (self.half // 2), 128), self.half // 2)

    def ahead(self, k):
        return lax.rem(self.p + k, self.lines)

    def behind(self, k):
        return lax.rem(self.p + self.lines - k, self.lines)

    def to_pair(self, way, stage, src, dst):
        c, f, c2 = self.place[:3]
        return remote(src, dst, self.ss.at[way, stage, 0], self.rs.at[way, stage, 0], (c2, f))

    def to_line(self, way, stage, k, src, dst):
        f = self.place[1]
        device = (self.ahead(k) * 2 + self.x, f)
        return remote(src, dst, self.ss.at[way, stage, k], self.rs.at[way, stage, k], device)

    def copies(self, way, stage):
        pay, total, p, x = self.pay, self.total, self.p, self.x
        every = range(1, self.lines)
        if way == 0:
            own = total.at[self.rows(p), self.columns(0, x)]
            group = total.at[:, self.columns(0, x)]
            if stage == 0:
                return [self.to_pair(0, 0, pay.at[:, self.columns(0, 1 - x)], self.a_in)]
            if stage == 1:
                return [
                    self.to_line(0, 1, k, self.a_sum.at[self.rows(self.ahead(k))], self.a_line.at[k - 1]) for k in every
                ]
            if stage == 2:
                return [self.to_line(0, 2, k, own, own) for k in every]
            return [self.to_pair(0, 3, group, group)]
        own = total.at[self.rows(p), self.columns(1, x)]
        both = total.at[self.rows(p), self.wide]
        if stage == 0:
            return [
                self.to_line(1, 0, k, pay.at[self.rows(self.ahead(k)), self.wide], self.b_line.at[k - 1]) for k in every
            ]
        if stage == 1:
            return [self.to_pair(1, 1, self.b_sum.at[:, self.columns(0, 1 - x)], self.b_in)]
        if stage == 2:
            return [self.to_pair(1, 2, own, own)]
        return [self.to_line(1, 3, k, both, both) for k in every]

    def start(self, stage):
        for way in range(2):
            for copy in self.copies(way, stage):
                copy.start()

    def wait(self, stage):
        pay, total, p, x = self.pay, self.total, self.p, self.x
        for way in range(2):
            for copy in self.copies(way, stage):
                copy.wait()
        if stage == 0:
            self.a_sum[...] = (pay[:, self.columns(0, x)].astype(f32) + self.a_in[...].astype(f32)).astype(bf16)
            value = pay[self.rows(p), self.wide].astype(f32)
            for k in range(1, self.lines):
                value = value + self.b_line[k - 1].astype(f32)
            self.b_sum[...] = value.astype(bf16)
        if stage == 1:
            value = self.a_sum[self.rows(p)].astype(f32)
            for k in range(1, self.lines):
                value = value + self.a_line[k - 1].astype(f32)
            total[self.rows(p), self.columns(0, x)] = value.astype(bf16)
            value = self.b_sum[:, self.columns(0, x)].astype(f32) + self.b_in[...].astype(f32)
            total[self.rows(p), self.columns(1, x)] = value.astype(bf16)


def back_body(
    ctx, step, block, chunk, ready,
    gn, hid, gains, cot, wo, att_t, q_t, kv, pos, lse, cos_r, sin_r, n1_t, inp, wp, n2, n2_g,
    cot_a0, cot_a1, cot_b0, cot_b1, x_a0, wg_h, wu_h, wd_h,
    inp_o, grads_o, acc_g, acc_u, acc_d, x_a1, x_b0, x_b1, x_fa0, x_fa1, x_fb0, x_fb1,
    gh, do_t, part, dq, held, ghl, ghl_g, low_t, n1_g, low_g, gp, gp_g, vec, vec_g,
    pay, total_r, a_in, a_sum, a_line, b_line, b_sum, b_in,
    xs, cs, wg, wu, wd, acc,
    ks, kr, ts, tr, as_, ar, vs, vr, sum_s, sum_r, ws, ins, outs, *sems
):
    place = where_am_i()
    c, f, c2, m, n = place
    far = (m + 2) % 4
    peers = [lax.rem(c + k, ctx) for k in range(1, ctx)]
    greet([(p, f) for p in peers] + [(c, m), (c, n), (c, far)])
    tok, width = cot.shape
    group = H // KV
    depth = n1_g.shape[1]
    scale = HD ** (-0.5)

    def rows(g):
        return pl.ds(pl.multiple_of(g * depth, 16), depth)

    def swaps():
        return [
            remote(src.at[rows(g)], dst.at[f], as_.at[j, k], ar.at[j, k], (c, g))
            for j, (src, dst) in enumerate(((n1_t, n1_g), (low_t, low_g)))
            for k, g in enumerate((n, far, m))
        ]

    ready()
    spread = Spread(place, ctx // 2, n2, n2_g, ((x_a0, x_a1), (x_b0, x_b1), (x_fa0, x_fa1), (x_fb0, x_fb1)), sems)
    spread.pairs_out(0)
    spread.lines_out(1)
    kept = spread.keep(n2_g, 1, 2, 3)
    loads = [
        pltpu.make_async_copy(src, dst, ws.at[j])
        for j, (src, dst) in enumerate(((wg_h, wg), (wu_h, wu), (wd_h, wd)))
    ]
    for copy in kept + loads:
        copy.start()
    low_t[...] = att_t[...].astype(bf16)
    back, gain_two = norm_grad(hid[...], gains[1:2], gn[...])
    gh[...] = cot[...].astype(f32) + back
    ghl[...] = gh[...].astype(bf16)
    items = [(ghl, lambda g, at: ghl_g.at[g, at])]
    tokens_start(items, ts.at[0], tr.at[0], place)
    for copy in swaps():
        copy.start()
    n1_g[f] = n1_t[rows(f)]
    low_g[f] = low_t[rows(f)]
    do_t[...] = over_last(wo[...], ghl[...]).astype(bf16)
    key_width = KV * HD
    for g in range(KV):
        queries, grads = heads(q_t, g, group, HD), heads(do_t, g, group, HD)
        delta = jnp.sum(grads.astype(f32) * heads(att_t, g, group, HD), 0, keepdims=True)
        total = jnp.concatenate([lse[pl.ds(g * group + j, 1)] for j in range(group)], 1)

        @pl.loop(0, kv.shape[0] // step)
        def _(i):
            at = pl.ds(i * step, step)
            both = kv[at].reshape(step * tok, 2 * key_width)
            keys = both[:, g * HD : (g + 1) * HD]
            values = both[:, key_width + g * HD : key_width + (g + 1) * HD]
            bias = key_bias(i * step * tok, step * tok, c, pos)
            scores = plain_dot(keys, queries) * scale + jnp.concatenate([bias] * group, 1)
            probs = jnp.exp(scores - total)
            g_probs = plain_dot(values, grads)
            g_scores = (probs * (g_probs - delta)).astype(bf16)
            g_keys = over_last(g_scores, queries) * scale
            g_values = over_last(probs.astype(bf16), grads)
            part[at, :, g * HD : (g + 1) * HD] = g_keys.astype(bf16).reshape(step, tok, HD)
            part[at, :, key_width + g * HD : key_width + (g + 1) * HD] = g_values.astype(bf16).reshape(
                step, tok, HD
            )
            g_queries = over_first(keys, g_scores) * scale

            @pl.when(i == 0)
            def _():
                dq[g] = g_queries

            @pl.when(i > 0)
            def _():
                dq[g] += g_queries

    owners = [remote(part.at[p], held.at[k], ks.at[k], kr.at[k], (p, f)) for k, p in enumerate(peers)]
    for copy in owners:
        copy.start()
    tokens_finish(items, ts.at[0], tr.at[0], place)
    for copy in swaps():
        copy.wait()
    cos, sin = cos_r[...], sin_r[...]
    g_q = [
        turn_back(dq[g, :, j * tok : (j + 1) * tok], cos, sin, HD) for g in range(KV) for j in range(group)
    ]
    g_q = jnp.concatenate(g_q, 0)
    query_width = g_q.shape[0]
    gp[:, :query_width] = g_q.T.astype(bf16)
    columns = gp.shape[1]
    low_all = jnp.concatenate([low_g[g] for g in range(4)], 1)
    pay[pl.ds(0, depth), pl.ds(columns, width)] = plain_dot(low_all, ghl_g[...].reshape(4 * tok, width)).astype(
        bf16
    )
    pairs = part[c].astype(f32)
    for k, copy in enumerate(owners):
        copy.wait()
        pairs = pairs + held[k].astype(f32)
    g_k = turn_back(pairs[:, :key_width].T, cos, sin, HD)
    gp[:, query_width : query_width + key_width] = g_k.T.astype(bf16)
    gp[:, query_width + key_width :] = pairs[:, key_width:].astype(bf16)
    items = [(gp, lambda g, at: gp_g.at[g, at])]
    tokens_start(items, ts.at[1], tr.at[1], place)
    g_normed = over_last(gp[...], wp[...])
    values = inp[...].astype(f32)
    back, gain_one = norm_grad(values, gains[0:1], g_normed)
    inp_o[...] = (gh[...] + back).astype(bf16)
    vec[...] = jnp.zeros_like(vec)
    vec[0:1, :width] = gain_one
    vec[1:2, :width] = gain_two
    vec[2:3, :columns] = jnp.sum(gp[...].astype(f32), 0, keepdims=True)
    vectors = [remote(vec, vec_g.at[k], vs.at[k], vr.at[k], (c, g)) for k, g in enumerate((m, n, far))]
    for copy in vectors:
        copy.start()
    spread.on_pair(0)
    spread.on_line(1, True)
    spread.lines_out(2)
    tokens_finish(items, ts.at[1], tr.at[1], place)
    n1_all = jnp.concatenate([n1_g[g] for g in range(4)], 1)
    pay[pl.ds(0, depth), pl.ds(0, columns)] = plain_dot(n1_all, gp_g[...].reshape(4 * tok, columns)).astype(bf16)
    total = vec[...]
    for k, copy in enumerate(vectors):
        copy.wait()
        total = total + vec_g[k]
    pay[pl.ds(depth, 8)] = total.astype(bf16)
    pay[pl.ds(depth + 8, pay.shape[0] - depth - 8)] = jnp.zeros_like(pay[pl.ds(depth + 8, pay.shape[0] - depth - 8)])
    summed = Total(place, ctx // 2, pay, total_r, a_in, a_sum, a_line, b_line, b_sum, b_in, sum_s, sum_r)
    summed.start(0)
    spread.cross(0)
    spread.cross(1)
    for copy in loads:
        copy.wait()
    parts = (((x_a0, x_a1), (cot_a0, cot_a1)), ((x_b0, x_b1), (cot_b0, cot_b1)))
    blocks = wg.shape[0] // block
    per_part = ctx * tok // chunk
    for way, sides in enumerate(parts):
        if way == 1:
            spread.finish_line(1)
            kept[0].wait()
        spread.finish_pair(way)
        for i in range(per_part):
            count = chunk // tok // 2
            at = pl.ds(i * count, count)
            fetch = [
                pltpu.make_async_copy(sides[j][side].at[at], into.at[side], ins.at[j, side])
                for j, into in enumerate((xs, cs))
                for side in range(2)
            ]
            for copy in fetch:
                copy.start()
            for copy in fetch:
                copy.wait()
            tokens = xs[...].reshape(chunk, width), cs[...].reshape(chunk, width)
            first = way == 0 and i == 0
            last = way == 1 and i == per_part - 1

            @pl.loop(0, blocks)
            def _(b):
                at = pl.ds(pl.multiple_of(b * block, 16), block)
                act, g_gate, g_up = hidden_units(*tokens, wg[at], wu[at], wd[at])
                for j, (left, right) in enumerate(((g_gate, 0), (g_up, 0), (act, 1))):
                    value = plain_dot(left, tokens[right])
                    if first:
                        acc[j, at] = value
                    else:
                        acc[j, at] += value
                for stage in range(3 if first else 0):

                    @pl.when(b == stage)
                    def _():
                        summed.wait(stage)
                        summed.start(stage + 1)

                if way == 0 and i == 0:

                    @pl.when(b == 1)
                    def _():
                        spread.on_pair(1)

                    @pl.when(b == 3)
                    def _():
                        spread.on_line(2, True)

                if way == 1 and i == 0:

                    @pl.when(b == 0)
                    def _():
                        spread.on_y(0)

                    @pl.when(b == 1)
                    def _():
                        spread.on_y(1)

                    @pl.when(b == 2)
                    def _():
                        spread.on_pair(2)

                if last:
                    for j, out in enumerate((acc_g, acc_u, acc_d)):
                        pltpu.make_async_copy(acc.at[j, at], out.at[at], outs.at[b, j]).start()

    summed.wait(3)
    grads_o[...] = total_r[...].astype(f32)
    spread.finish_line(2)
    spread.finish_pair(2)
    spread.finish_cross()
    for b in range(blocks):
        at = pl.ds(b * block, block)
        for j, out in enumerate((acc_g, acc_u, acc_d)):
            pltpu.make_async_copy(acc.at[j, at], out.at[at], outs.at[b, j]).wait()
    for copy in kept[1:]:
        copy.wait()


def over_last(a, b):
    return lax.dot_general(a, b, (((1,), (1,)), ((), ())), preferred_element_type=f32)


def over_first(a, b):
    return lax.dot_general(a, b, (((0,), (0,)), ((), ())), preferred_element_type=f32)


def plain_dot(a, b):
    return jnp.dot(a, b, preferred_element_type=f32)


def hidden_units(x, cot, wg, wu, wd):
    return gates(over_last(wg, x), over_last(wu, x), over_last(wd, cot))


def hidden_body(
    chunk, block, x0_h, x1_h, x2_h, x3_h, c0_h, c1_h, c2_h, c3_h, wg_h, wu_h, wd_h, ig_h, iu_h, id_h, og_h, ou_h, od_h, xs, cs, wg, wu, wd, acc, in_sem, w_sem, out_sem, init_sem
):
    parts = (((x0_h, x1_h), (c0_h, c1_h)), ((x2_h, x3_h), (c2_h, c3_h)))
    rows = 4 * x0_h.shape[0]
    steps, blocks, held = rows // chunk, wg.shape[0] // block, xs.shape[0] // chunk
    def weights(b):
        at = pl.ds(b * block, block)
        return [
            pltpu.make_async_copy(src.at[at], dst.at[at], w_sem.at[b, j])
            for j, (src, dst) in enumerate(((wg_h, wg), (wu_h, wu), (wd_h, wd)))
        ]

    def fetch(i, begin, part):
        half = chunk // 2
        src = pl.ds(pl.multiple_of(begin * half, half), half)
        slot = i % held
        return [
            pltpu.make_async_copy(
                part[j][side].at[src],
                into.at[pl.ds(pl.multiple_of(slot * chunk + side * half, half), half)],
                in_sem.at[slot, j, side],
            )
            for j, into in enumerate((xs, cs))
            for side in range(2)
        ]

    def start_tokens(i):
        begin = 0
        for part in parts:
            count = 2 * x0_h.shape[0] // chunk

            def go(begin=begin, part=part):
                for copy in fetch(i, i - begin, part):
                    copy.start()

            if isinstance(i, int):
                if begin <= i < begin + count:
                    go()
            else:
                pl.when((i >= begin) & (i < begin + count))(go)
            begin += count

    def wait_tokens(i):
        for copy in fetch(i, 0, parts[0]):
            copy.wait()

    def results(b, slot):
        at = pl.ds(pl.multiple_of(b * block, 16), block)
        return [
            pltpu.make_async_copy(acc.at[slot, j], out.at[at], out_sem.at[slot, j])
            for j, out in enumerate((og_h, ou_h, od_h))
        ]

    def initial(b, slot):
        at = pl.ds(pl.multiple_of(b * block, 16), block)
        return [
            pltpu.make_async_copy(src.at[at], acc.at[slot, j], init_sem.at[slot, j])
            for j, src in enumerate((ig_h, iu_h, id_h))
        ]

    resident = held == steps
    slots = acc.shape[0]
    start_tokens(0)
    for copy in weights(0):
        copy.start()
    for copy in weights(0):
        copy.wait()
    for copy in initial(0, 0):
        copy.start()
    for i in range(1, held if resident else 1):
        start_tokens(i)
    for b in range(1, slots):
        for copy in weights(b) + initial(b, b):
            copy.start()

    @pl.loop(0, blocks)
    def _(b):
        slot = b % slots
        at = pl.ds(pl.multiple_of(b * block, 16), block)

        @pl.when(b == 1)
        def _():
            for copy in weights(1):
                copy.wait()

        @pl.loop(0, steps)
        def _(i):
            if resident:

                @pl.when(b == 0)
                def _():
                    wait_tokens(i)

            else:
                wait_tokens(i)

                @pl.when((i + 1 < steps) | (b + 1 < blocks))
                def _():
                    start_tokens(lax.rem(i + 1, steps))

            t = pl.ds(pl.multiple_of(i % held * chunk, chunk), chunk)
            x, cot = xs[t], cs[t]
            act, g_gate, g_up = hidden_units(x, cot, wg[at], wu[at], wd[at])

            @pl.when(i == 0)
            def _():
                for copy in initial(b, slot):
                    copy.wait()

            acc[slot, 0] += plain_dot(g_gate, x)
            acc[slot, 1] += plain_dot(g_up, x)
            acc[slot, 2] += plain_dot(act, cot)

        for copy in results(b, slot):
            copy.start()

    for b in range(max(0, blocks - slots), blocks):
        for copy in results(b, b % slots):
            copy.wait()


def hidden_grads(xs, cots, wg, wu, wd, initial):
    width = wg.shape[1]
    xs, cots = [[part.reshape(-1, width) for part in parts] for parts in (xs, cots)]
    rows = sum(part.shape[0] for part in xs)
    units = wg.shape[0]
    chunk = math.gcd(rows // 2, 1024)
    block = units // 2
    held = min(rows // chunk, 4)
    any_spec = pl.BlockSpec(memory_space=pl.ANY)
    dma = pltpu.SemaphoreType.DMA
    return pl.pallas_call(
        functools.partial(hidden_body, chunk, block),
        out_shape=(jax.ShapeDtypeStruct((units, width), f32),) * 3,
        in_specs=[any_spec] * 14,
        out_specs=(any_spec,) * 3,
        scratch_shapes=[pltpu.VMEM((held * chunk, width), bf16)] * 2
        + [pltpu.VMEM((units, width), bf16)] * 3
        + [pltpu.VMEM((2, 3, block, width), f32), dma((held, 2, 2)), dma((2, 3)), dma((2, 3)), dma((2, 3))],
        compiler_params=pltpu.CompilerParams(vmem_limit_bytes=62 << 20),
        cost_estimate=pl.CostEstimate(
            flops=12 * rows * width * units, bytes_accessed=4 * rows * width + 18 * units * width, transcendentals=0
        ),
        name="hidden_grads",
    )(*xs, *cots, wg, wu, wd, *initial)


def shards(
    layer_input,
    seq_ids,
    positions,
    norm_gain,
    w_query,
    b_query,
    w_key,
    b_key,
    w_value,
    b_value,
    w_output,
    mlp_gain,
    w_gate,
    w_up,
    w_down,
    cotangent,
):
    tok = layer_input.shape[1]
    width = layer_input.shape[2]
    group = H // KV
    query_width = H * HD
    key_width = KV * HD
    score_scale = HD ** (-0.5)
    ctx = lax.axis_size("ctx")
    fsdp = lax.axis_size("fsdp")
    depth = width // fsdp
    lines = ctx // 2
    c, f = lax.axis_index("ctx"), lax.axis_index("fsdp")
    seq_length = ctx * tok
    dma = pltpu.SemaphoreType.DMA
    sds = jax.ShapeDtypeStruct
    input_rows = layer_input[0]
    grad_out = cotangent[0]
    own_segment = seq_ids[0]
    own_positions = positions[0]
    query_rows = c * tok + jnp.arange(tok, dtype=jnp.int32)

    cosine, sine_table = rope_tables(own_positions, HD)
    own_positions = own_positions[None]
    step = math.gcd(ctx, 4)
    columns = query_width + 2 * key_width
    hbm = pl.BlockSpec(memory_space=pltpu.HBM)
    half_blocks = sds((lines, 2, tok // 2, width), bf16)
    (w_project, wo_full, gains, n1_t, q_t, kv_all, cot_group, att_t, log_total, hidden_state, normed_second,
     cot_a0, cot_a1, cot_b0) = (
        staged_call(
            functools.partial(front_body, lines, step),
            (
                input_rows, grad_out, norm_gain, mlp_gain, b_query, b_key, b_value, own_positions, cosine, sine_table,
                w_query, w_key, w_value, w_output,
            ),
            (10, 11, 12, 13),
            (
                sds((width, columns), bf16),
                sds((query_width, width), bf16),
                sds((8, width), f32),
                sds((width, tok), bf16),
                sds((query_width, tok), bf16),
                sds((ctx, tok, 2 * key_width), bf16),
                sds((fsdp, tok, width), bf16),
                sds((query_width, tok), f32),
                sds((H, tok), f32),
                sds((tok, width), f32),
                sds((tok, width), bf16),
                half_blocks,
                half_blocks,
                half_blocks,
            ),
            (11, 12, 13),
            [
                pltpu.VMEM((tok, 2 * key_width), bf16),
                pltpu.VMEM((8, 256), f32),
                pltpu.VMEM((fsdp, 8, 256), f32),
                dma((3,)),
                dma((3,)),
            ]
            + gather_sems(4)
            + [dma((2, lines)), dma((2, lines))]
            + gather_sems(1)
            + spread_sems(lines),
            0,
            "front",
            pl.CostEstimate(flops=4 * 10**9, bytes_accessed=10**7, transcendentals=0),
        )
    )
    units = w_down.shape[0]
    wg_t, wu_t = w_gate.T, w_up.T
    (grad_normed2, block_out, x_group, cot_b1, cot_fa0, cot_fa1, cot_fb0, cot_fb1, x_a0) = staged_call(
        functools.partial(mid_body, lines),
        (normed_second, cot_group, grad_out, cot_a0, cot_a1, cot_b0, hidden_state, wg_t, wu_t, w_down),
        (3, 4, 5, 7, 8, 9),
        (
            sds((tok, width), f32),
            sds((tok, width), bf16),
            sds((fsdp, tok, width), bf16),
        )
        + (half_blocks,) * 6,
        (3, 4, 5, 6, 7, 8),
        [pltpu.VMEM((units, width), bf16)] * 3
        + [
            pltpu.VMEM((3, 2 * tok, units), bf16),
            pltpu.VMEM((2, tok, width), f32),
            pltpu.VMEM((8, tok, width), bf16),
            pltpu.VMEM((2, tok, width), bf16),
            pltpu.VMEM((2, tok, width), bf16),
            dma((3,)),
            dma((5,)),
            dma((5,)),
            dma((6,)),
            dma((6,)),
        ]
        + spread_sems(lines)
        + spread_sems(lines),
        2,
        "mid",
        pl.CostEstimate(
            flops=12 * fsdp * tok * width * units, bytes_accessed=6 * units * width, transcendentals=0
        ),
    )
    block_out = block_out[None]
    tall, everything = 256, columns + width
    height = tall // lines
    block = units // 4
    chunk = math.gcd(ctx * tok, 1024)
    big = sds((units, width), f32)
    (input_grad, weight_grads, acc_g, acc_u, acc_d, x_a1, x_b0, x_b1, x_fa0, x_fa1, x_fb0, x_fb1) = staged_call(
        functools.partial(back_body, ctx, step, block, chunk),
        (
            grad_normed2, hidden_state, gains, grad_out, wo_full, att_t, q_t, kv_all, own_positions, log_total,
            cosine, sine_table, n1_t, input_rows, w_project, normed_second, x_group, cot_a0, cot_a1,
            cot_b0, cot_b1, x_a0, wg_t, wu_t, w_down,
        ),
        (17, 18, 19, 20, 21, 22, 23, 24),
        (sds((tok, width), bf16), sds((tall, everything), f32), big, big, big) + (half_blocks,) * 7,
        (2, 3, 4, 5, 6, 7, 8, 9, 10, 11),
        [
            pltpu.VMEM((tok, width), f32),
            pltpu.VMEM((query_width, tok), bf16),
            pltpu.VMEM((ctx, tok, 2 * key_width), bf16),
            pltpu.VMEM((KV, HD, group * tok), f32),
            pltpu.VMEM((ctx - 1, tok, 2 * key_width), bf16),
            pltpu.VMEM((tok, width), bf16),
            pltpu.VMEM((fsdp, tok, width), bf16),
            pltpu.VMEM((query_width, tok), bf16),
            pltpu.VMEM((fsdp, depth, tok), bf16),
            pltpu.VMEM((fsdp, depth, tok), bf16),
            pltpu.VMEM((tok, columns), bf16),
            pltpu.VMEM((fsdp, tok, columns), bf16),
            pltpu.VMEM((8, everything), f32),
            pltpu.VMEM((3, 8, everything), f32),
            pltpu.VMEM((tall, everything), bf16),
            pltpu.VMEM((tall, everything), bf16),
            pltpu.VMEM((tall, everything // 4), bf16),
            pltpu.VMEM((tall, everything // 4), bf16),
            pltpu.VMEM((lines - 1, height, everything // 4), bf16),
            pltpu.VMEM((lines - 1, height, everything // 2), bf16),
            pltpu.VMEM((height, everything // 2), bf16),
            pltpu.VMEM((height, everything // 4), bf16),
            pltpu.VMEM((2, chunk // tok // 2, 2, tok // 2, width), bf16),
            pltpu.VMEM((2, chunk // tok // 2, 2, tok // 2, width), bf16),
            pltpu.VMEM((units, width), bf16),
            pltpu.VMEM((units, width), bf16),
            pltpu.VMEM((units, width), bf16),
            pltpu.VMEM((3, units, width), f32),
            dma((ctx - 1,)),
            dma((ctx - 1,)),
            dma((2, 1, 6)),
            dma((2, 1, 6)),
            dma((2, 3)),
            dma((2, 3)),
            dma((3,)),
            dma((3,)),
            dma((2, 4, lines)),
            dma((2, 4, lines)),
            dma((3,)),
            dma((2, 2)),
            dma((4, 3)),
        ]
        + spread_sems(lines),
        3,
        "back",
        pl.CostEstimate(flops=4 * 10**10, bytes_accessed=6 * 10**7, transcendentals=0),
    )
    input_grad = input_grad[None]
    starts = ((0, 0, width), (1, 0, width), (2, 0, query_width), (2, query_width, key_width),
              (2, query_width + key_width, key_width))

    def piece(row, start, size):
        share = size // fsdp
        return lax.dynamic_slice_in_dim(weight_grads[depth + row], start + f * share, share, 0)

    own = [piece(*at) for at in starts]
    weight_grads = weight_grads[:depth]

    gate_grad, up_grad, down_grad = hidden_grads(
        (x_fa0, x_fa1, x_fb0, x_fb1), (cot_fa0, cot_fa1, cot_fb0, cot_fb1), wg_t, wu_t, w_down, (acc_g, acc_u, acc_d)
    )
    return (
        block_out,
        input_grad,
        own[0],
        weight_grads[:, :query_width],
        own[2],
        weight_grads[:, query_width : query_width + key_width],
        own[3],
        weight_grads[:, query_width + key_width : query_width + 2 * key_width],
        own[4],
        weight_grads[:, query_width + 2 * key_width :],
        own[1],
        gate_grad.T,
        up_grad.T,
        down_grad,
        log_total[None],
    )


def solution(mesh):
    in_specs = (
        P("fsdp", "ctx", None),
        P("fsdp", "ctx"),
        P("fsdp", "ctx"),
        P("fsdp"),
        P("fsdp", None),
        P("fsdp"),
        P("fsdp", None),
        P("fsdp"),
        P("fsdp", None),
        P("fsdp"),
        P("fsdp", None),
        P("fsdp"),
        P(None, "fsdp"),
        P(None, "fsdp"),
        P("fsdp", None),
        P("fsdp", "ctx", None),
    )
    out_specs = (
        P("fsdp", "ctx", None),
        P("fsdp", "ctx", None),
        P("fsdp"),
        P("fsdp", None),
        P("fsdp"),
        P("fsdp", None),
        P("fsdp"),
        P("fsdp", None),
        P("fsdp"),
        P("fsdp", None),
        P("fsdp"),
        P(None, "fsdp"),
        P(None, "fsdp"),
        P("fsdp", None),
        P("fsdp", None, "ctx"),
    )

    return jax.shard_map(shards, mesh=mesh, in_specs=in_specs, out_specs=out_specs, check_vma=False)
```

```python
import functools
import math

import jax
import jax.numpy as jnp
from jax import lax
from jax.experimental import pallas as pl
from jax.experimental.pallas import tpu as pltpu
from jax.sharding import PartitionSpec as P

H = 14
KV = 2
HD = 64


EPSILON = 1e-06
ROPE_BASE = 1000000.0
MASK_FILL = -1e30
MESH = pl.DeviceIdType.MESH
VMEM = pl.BlockSpec(memory_space=pltpu.VMEM)
f32 = jnp.float32
bf16 = jnp.bfloat16


def rope_tables(positions, head_dim):
    half = head_dim // 2
    freq = ROPE_BASE ** (-(jnp.arange(half, dtype=jnp.float32) * 2.0 / head_dim))
    angle = positions.astype(jnp.float32)[None, :] * freq[:, None]
    return jnp.cos(angle), jnp.sin(angle)


def remote(src, dst, send_sem, recv_sem, device):
    return pltpu.make_async_remote_copy(
        src_ref=src, dst_ref=dst, send_sem=send_sem, recv_sem=recv_sem, device_id=device,
        device_id_type=MESH,
    )


def where_am_i():
    c, f = lax.axis_index("ctx"), lax.axis_index("fsdp")
    c2 = c + 1 - 2 * (c % 2)
    m = f + 1 - 2 * (f % 2)
    n = (f + 2) % 4
    return c, f, c2, m, n


def greet(devices):
    barrier = pltpu.get_barrier_semaphore()
    for device in devices:
        pl.semaphore_signal(barrier, inc=1, device_id=device, device_id_type=MESH)
    pl.semaphore_wait(barrier, len(devices))


def gather_start(items, ss, rs, place):
    c, f, c2, m, n = place
    h = c % 2
    for i, (src, dst) in enumerate(items):
        half = src.shape[0] // 2
        rows = pl.ds(h * half, half)
        remote(src.at[rows], dst(f).at[rows], ss.at[i, 1], rs.at[i, 1], (c, n)).start()
    for i, (src, dst) in enumerate(items):
        remote(src, dst(f), ss.at[i, 0], rs.at[i, 0], (c, m)).start()
        pltpu.make_async_copy(src, dst(f), ss.at[i, 5]).start()


def gather_finish(items, ss, rs, place):
    c, f, c2, m, n = place
    h = c % 2
    far = (m + 2) % 4
    for i, (src, dst) in enumerate(items):
        half = src.shape[0] // 2
        mine = dst(n).at[pl.ds(h * half, half)]
        remote(mine, mine, ss.at[i, 1], rs.at[i, 1], (c, n)).wait_recv()
        remote(mine, mine, ss.at[i, 2], rs.at[i, 2], (c2, f)).start()
        remote(mine, mine, ss.at[i, 3], rs.at[i, 3], (c, m)).start()
    for i, (src, dst) in enumerate(items):
        half = src.shape[0] // 2
        other = dst(n).at[pl.ds((1 - h) * half, half)]
        remote(other, other, ss.at[i, 2], rs.at[i, 2], (c2, f)).wait_recv()
        remote(other, other, ss.at[i, 4], rs.at[i, 4], (c, m)).start()
    for i, (src, dst) in enumerate(items):
        half = src.shape[0] // 2
        mine, other = pl.ds(h * half, half), pl.ds((1 - h) * half, half)
        remote(src, dst(m), ss.at[i, 0], rs.at[i, 0], (c, m)).wait()
        remote(src.at[mine], dst(f).at[mine], ss.at[i, 1], rs.at[i, 1], (c, n)).wait_send()
        remote(src.at[mine], dst(n).at[mine], ss.at[i, 2], rs.at[i, 2], (c2, f)).wait_send()
        remote(src.at[mine], dst(far).at[mine], ss.at[i, 3], rs.at[i, 3], (c, m)).wait()
        remote(src.at[other], dst(far).at[other], ss.at[i, 4], rs.at[i, 4], (c, m)).wait()
        pltpu.make_async_copy(src, dst(f), ss.at[i, 5]).wait()


def tokens_start(items, ss, rs, place):
    c, f, c2, m, n = place
    for i, (src, dst) in enumerate(items):
        half = src.shape[0] // 2
        for j in range(2):
            rows = pl.ds(j * half, half)
            remote(src.at[rows], dst(f, rows), ss.at[i, 1 + j], rs.at[i, 1 + j], (c, n)).start()
    for i, (src, dst) in enumerate(items):
        rows = pl.ds(0, src.shape[0])
        remote(src, dst(f, rows), ss.at[i, 0], rs.at[i, 0], (c, m)).start()
        dst(f, rows)[...] = src[...]


def tokens_finish(items, ss, rs, place):
    c, f, c2, m, n = place
    far = (m + 2) % 4
    for i, (src, dst) in enumerate(items):
        half = src.shape[0] // 2
        for j in range(2):
            here = dst(n, pl.ds(j * half, half))
            remote(here, here, ss.at[i, 1 + j], rs.at[i, 1 + j], (c, n)).wait_recv()
            remote(here, here, ss.at[i, 3 + j], rs.at[i, 3 + j], (c, m)).start()
    for i, (src, dst) in enumerate(items):
        half = src.shape[0] // 2
        remote(src, dst(m, pl.ds(0, src.shape[0])), ss.at[i, 0], rs.at[i, 0], (c, m)).wait()
        for j in range(2):
            rows = pl.ds(j * half, half)
            remote(src.at[rows], dst(f, rows), ss.at[i, 1 + j], rs.at[i, 1 + j], (c, n)).wait_send()
            remote(src.at[rows], dst(far, rows), ss.at[i, 3 + j], rs.at[i, 3 + j], (c, m)).wait()


def gather_sems(count):
    return [pltpu.SemaphoreType.DMA((count, 6)), pltpu.SemaphoreType.DMA((count, 6))]


def staged_call(body, args, in_hbm, out_shape, out_hbm, scratch, ident, name, cost):
    hbm = pl.BlockSpec(memory_space=pltpu.HBM)
    staged_in = [i for i in range(len(args)) if i not in in_hbm]
    staged_out = [i for i in range(len(out_shape)) if i not in out_hbm]

    def kernel(*refs):
        ins, outs = list(refs[: len(args)]), list(refs[len(args) : len(args) + len(out_shape)])
        rest = list(refs[len(args) + len(out_shape) :])
        own, rest = rest[: len(scratch)], rest[len(scratch) :]
        in_sem, out_sem = rest[-2:]
        copies_in, copies_out = [], []
        for j, i in enumerate(staged_in):
            buffer = rest.pop(0)
            copies_in.append(pltpu.make_async_copy(ins[i], buffer, in_sem.at[j]))
            ins[i] = buffer
        for j, i in enumerate(staged_out):
            buffer = rest.pop(0)
            copies_out.append(pltpu.make_async_copy(buffer, outs[i], out_sem.at[j]))
            outs[i] = buffer
        for copy in copies_in:
            copy.start()

        def ready():
            for copy in copies_in:
                copy.wait()

        body(ready, *ins, *outs, *own)
        for copy in copies_out:
            copy.start()
        for copy in copies_out:
            copy.wait()

    buffers = [pltpu.VMEM(args[i].shape, args[i].dtype) for i in staged_in]
    buffers += [pltpu.VMEM(out_shape[i].shape, out_shape[i].dtype) for i in staged_out]
    sems = [pltpu.SemaphoreType.DMA((len(staged_in),)), pltpu.SemaphoreType.DMA((len(staged_out),))]
    return pl.pallas_call(
        kernel,
        out_shape=out_shape,
        in_specs=[hbm] * len(args),
        out_specs=(hbm,) * len(out_shape),
        scratch_shapes=scratch + buffers + sems,
        compiler_params=pltpu.CompilerParams(
            collective_id=ident, has_side_effects=True, vmem_limit_bytes=67_043_328
        ),
        cost_estimate=cost,
        name=name,
    )(*args)


def spread_start(src, dst, ss, rs, place, lines):
    c, f, c2, m, n = place
    for k in range(1, lines):
        p = lax.rem(c // 2 + k, lines) * 2 + c % 2
        remote(src, dst.at[c], ss.at[0, k], rs.at[0, k], (p, f)).start()
    remote(src, dst.at[c], ss.at[1, 0], rs.at[1, 0], (c2, f)).start()


def spread_finish(src, dst, ss, rs, place, lines):
    c, f, c2, m, n = place
    for k in range(1, lines):
        giver = lax.rem(c // 2 + lines - k, lines) * 2 + c % 2
        block = dst.at[giver]
        remote(block, block, ss.at[0, k], rs.at[0, k], (c2, f)).wait_recv()
        remote(block, block, ss.at[1, k], rs.at[1, k], (c2, f)).start()
    for k in range(lines):
        giver = lax.rem(c2 // 2 + lines - k, lines) * 2 + c2 % 2
        remote(src, dst.at[giver], ss.at[1, k], rs.at[1, k], (c2, f)).wait()
        if k:
            remote(src, dst.at[c], ss.at[0, k], rs.at[0, k], (c2, f)).wait_send()


def line_devices(place, lines):
    c, f, c2, m, n = place
    return [(lax.rem(c // 2 + k, lines) * 2 + c % 2, f) for k in range(1, lines)] + [(c2, f)]


def gates(gate, up, g_act):
    sg = jax.nn.sigmoid(gate)
    silu = gate * sg
    act = (silu * up).astype(bf16)
    g_gate = (g_act * up * (sg * (1.0 + gate * (1.0 - sg)))).astype(bf16)
    g_up = (g_act * silu).astype(bf16)
    return act, g_gate, g_up


class Spread:
    def __init__(self, place, lines, x, group, into, sems):
        self.place, self.lines, self.x, self.group, self.into = place, lines, x, group, into
        self.half = x.shape[0] // 2
        self.core = place[1] % 2
        self.line_s, self.line_r, self.pair_s, self.pair_r, self.y_s, self.y_r, self.mate_s, self.mate_r, self.own = sems

    def at(self, k):
        return lax.rem(self.place[0] // 2 + self.lines - k, self.lines)

    def each(self, first, act):
        pl.loop(first, self.lines)(act)

    def source(self, way):
        n = self.place[4]
        rows = pl.ds((0 if way == 0 else 1) * self.half, self.half)
        return self.x.at[rows] if way < 2 else self.group.at[n, rows]

    def slot(self, way, side, k, core=None):
        return self.into[(0, 1, 3, 2)[way]][side].at[self.at(k), self.core if core is None else core]

    def line(self, way, k):
        c, f = self.place[:2]
        sems = self.line_s.at[way, k], self.line_r.at[way, k]
        device = (lax.rem(c // 2 + k, self.lines) * 2 + c % 2, f)
        return remote(self.source(way), self.slot(way, 0, 0), *sems, device)

    def arrived(self, way, k):
        here = self.slot(way, 0, k)
        c, f, c2 = self.place[:3]
        return remote(here, here, self.line_s.at[way, k], self.line_r.at[way, k], (c2, f))

    def pair(self, way, k):
        c, f, c2 = self.place[:3]
        src = self.source(way) if isinstance(k, int) and k == 0 else self.slot(way, 0, k)
        return remote(src, self.slot(way, 1, k), self.pair_s.at[way, k], self.pair_r.at[way, k], (c2, f))

    def across(self, side, k):
        c, n = self.place[0], self.place[4]
        sems = self.y_s.at[side, k], self.y_r.at[side, k]
        return remote(self.slot(0, side, k), self.slot(3, side, k), *sems, (c, n))

    def hand(self, way, side, k, core=None):
        c, m = self.place[0], self.place[3]
        here = self.slot(way, side, k, core)
        return remote(here, here, self.mate_s.at[way, side, k], self.mate_r.at[way, side, k], (c, m))

    def lines_out(self, way):
        self.each(1, lambda k: self.line(way, k).start())

    def on_line(self, way, forward):
        def act(k):
            self.arrived(way, k).wait_recv()
            if forward:
                self.pair(way, k).start()
            self.hand(way, 0, k).start()

        if forward:
            self.pair(way, 0).start()
        self.each(1, act)

    def pairs_out(self, way):
        self.pair(way, 0).start()
        self.each(1, lambda k: self.pair(way, k).start())

    def on_pair(self, way):
        def act(k):
            self.pair(way, k).wait_recv()
            self.hand(way, 1, k).start()

        self.each(0, act)

    def cross(self, side):
        self.each(1 - side, lambda k: self.across(side, k).start())

    def on_y(self, side):
        def act(k):
            self.across(side, k).wait_recv()
            self.hand(3, side, k).start()

        self.each(1 - side, act)

    def keep(self, group, *parts):
        c, f = self.place[:2]
        copies = []
        for part in parts:
            pair = pl.ds((f // 2 if part < 2 else 1 - f // 2) * 2, 2)
            rows = pl.ds(part % 2 * self.half, self.half)
            into = self.into[part][0].at[c // 2]
            copies.append(pltpu.make_async_copy(group.at[pair, rows], into, self.own.at[part]))
        return copies

    def handed(self, way, side):
        def act(k):
            self.hand(way, side, k).wait_send()
            self.hand(way, side, k, 1 - self.core).wait_recv()

        self.each(1 - side, act)

    def finish_line(self, way):
        self.each(1, lambda k: self.line(way, k).wait_send())
        self.handed(way, 0)

    def finish_pair(self, way):
        self.each(0, lambda k: self.pair(way, k).wait_send())
        self.handed(way, 1)

    def finish_cross(self):
        for side in range(2):
            self.each(1 - side, lambda k: self.across(side, k).wait_send())
            self.handed(3, side)


def spread_sems(lines):
    dma = pltpu.SemaphoreType.DMA
    return [dma(shape) for shape in ((3, lines), (3, lines), (2, lines), (4, 2, lines)) for _ in range(2)] + [dma((4,))]


def mid_body(
    lines, ready, x, cot, own_cot, a0, a1, b0, hid, wg_h, wu_h, wd_h,
    gn_o, block_o, xg, b1_o, fb0_o, xa0_o, xa1_o,
    wg, wu, wd, act, back, near, sums, far_in, ws, ss, rs, ns, nr, *sems
):
    place = where_am_i()
    c, f, c2, m, n = place
    far = (m + 2) % 4
    tok, width = x.shape
    loads = [
        pltpu.make_async_copy(src, dst, ws.at[j])
        for j, (src, dst) in enumerate(((wg_h, wg), (wu_h, wu), (wd_h, wd)))
    ]
    for copy in loads:
        copy.start()
    greet(line_devices(place, lines) + [(c, m), (c, n)])
    ready()
    half = tok // 2
    own = remote(x, xg.at[f], ss.at[0], rs.at[0], (c, m))
    own.start()
    for j in range(2):
        rows = pl.ds(j * half, half)
        remote(x.at[rows], xg.at[f, rows], ss.at[1 + j], rs.at[1 + j], (c, n)).start()
    rest = Spread(place, lines, own_cot, cot, ((a0, a1), (b0, b1_o), None, (fb0_o,)), sems[:9])
    spread = Spread(place, lines, x, xg, ((xa0_o, xa1_o),), sems[9:])
    rest.pairs_out(1)
    spread.lines_out(0)
    kept = rest.keep(cot, 3)
    for copy in kept:
        copy.start()
    xg[f] = x[...]
    for copy in loads:
        copy.wait()
    own.wait()

    def forward(pair):
        at = pl.ds(pair * 2, 2)
        xs = xg[at].reshape(2 * tok, width)
        cs = cot[at].reshape(2 * tok, width)
        parts = gates(over_last(xs, wg[...]), over_last(xs, wu[...]), over_last(cs, wd[...]))
        for j, part in enumerate(parts):
            act[j] = part

    def backward():
        return plain_dot(act[1], wg[...]) + plain_dot(act[2], wu[...])

    def down():
        return plain_dot(act[0], wd[...])

    y = f // 2
    core = f % 2

    def swap(j):
        return remote(near.at[2 * j], near.at[2 * j + 1], ns.at[j], nr.at[j], (c, m))

    def give(j, value):
        back[...] = value.reshape(2, tok, width)
        near[2 * j] = back[1 - core].astype(bf16)
        swap(j).start()

    def cross(j):
        return remote(sums.at[j], far_in.at[j], ns.at[4 + j], nr.at[4 + j], (c, n))

    def send_over(j, j_swap):
        swap(j_swap).wait()
        sums[j] = (back[core] + near[2 * j_swap + 1].astype(f32)).astype(bf16)
        cross(j).start()

    forward(y)
    for j in range(2):
        here = xg.at[n, pl.ds(j * half, half)]
        remote(here, here, ss.at[1 + j], rs.at[1 + j], (c, n)).wait_recv()
        remote(here, here, ss.at[3 + j], rs.at[3 + j], (c, m)).start()
    rest.lines_out(2)
    give(0, backward())
    gn_o[...] = back[core]
    give(1, down())
    down_own = hid[...] + back[core]
    for j in range(2):
        rows = pl.ds(j * half, half)
        remote(x.at[rows], xg.at[far, rows], ss.at[3 + j], rs.at[3 + j], (c, m)).wait_recv()
    kept += spread.keep(xg, 0)
    kept[-1].start()
    forward(1 - y)
    give(2, backward())
    send_over(0, 2)
    spread.on_line(0, True)
    give(3, down())
    send_over(1, 3)
    rest.on_pair(1)
    cross(0).wait()
    swap(0).wait()
    gn_o[...] += near[1].astype(f32) + far_in[0].astype(f32)
    cross(1).wait()
    swap(1).wait()
    block_o[...] = (down_own + near[3].astype(f32) + far_in[1].astype(f32)).astype(bf16)
    rest.on_line(2, False)
    spread.on_pair(0)
    for j in range(2):
        rows = pl.ds(j * half, half)
        remote(x.at[rows], xg.at[f, rows], ss.at[1 + j], rs.at[1 + j], (c, n)).wait_send()
        remote(x.at[rows], xg.at[far, rows], ss.at[3 + j], rs.at[3 + j], (c, m)).wait_send()
    for copy in kept:
        copy.wait()
    rest.finish_pair(1)
    rest.finish_line(2)
    spread.finish_line(0)
    spread.finish_pair(0)


def turn(values, cos, sin, size):
    half = size // 2
    pieces = []
    for at in range(0, values.shape[0], size):
        lead, trail = values[at : at + half], values[at + half : at + size]
        pieces += [lead * cos - trail * sin, trail * cos + lead * sin]
    return jnp.concatenate(pieces, 0)


def key_bias(first, count, c, pos):
    tok = pos.shape[1]
    keys = lax.broadcasted_iota(jnp.int32, (count, tok), 0) + first
    queries = lax.broadcasted_iota(jnp.int32, (count, tok), 1) + c * tok
    allowed = (keys <= queries) & (keys >= queries - pos[...])
    return jnp.where(allowed, 0.0, MASK_FILL)


def front_body(
    lines, step, ready,
    inp, cot, v0, v1, v2, v3, v4, pos, cos_r, sin_r, wq, wk, wv, wo,
    wp_o, wo_o, gains_o, n1_o, q_o, kv_o, cot_o, att_o, lse_o, hid_o, n2_o, a0_o, a1_o, b0_o,
    kv, small, small_g, ms, mr, gs, gr, ks, kr, ts, tr, *sems
):
    place = where_am_i()
    c, f, c2, m, n = place
    far = (m + 2) % 4
    greet(line_devices(place, lines) + [(c, m), (c, n), (c, far)])
    tok, width = inp.shape
    depth, query_width = wq.shape
    key_width = wk.shape[1]
    group = H // KV
    scale = HD ** (-0.5)

    def rows(g):
        return pl.ds(pl.multiple_of(g * depth, 16), depth)

    project = [
        (wq, lambda g: wp_o.at[rows(g), pl.ds(0, query_width)]),
        (wk, lambda g: wp_o.at[rows(g), pl.ds(query_width, key_width)]),
        (wv, lambda g: wp_o.at[rows(g), pl.ds(query_width + key_width, key_width)]),
    ]
    output = [(wo, lambda g: wo_o.at[rows(g)])]
    gather_start(project, gs.at[pl.ds(0, 3)], gr.at[pl.ds(0, 3)], place)
    ready()
    small[...] = jnp.zeros_like(small)
    for k, v in enumerate((v0, v1, v2, v3, v4)):
        small[k : k + 1, : v.shape[0]] = v[...].astype(f32).reshape(1, v.shape[0])
    smalls = [remote(small, small_g.at[f], ms.at[k], mr.at[k], (c, g)) for k, g in enumerate((m, n, far))]
    for copy in smalls:
        copy.start()
    spread = Spread(place, lines, cot, cot_o, ((a0_o, a1_o), (b0_o,)), sems)
    spread.lines_out(0)
    values = inp[...].astype(f32)
    unit = values * lax.rsqrt(jnp.mean(values * values, -1, keepdims=True) + EPSILON)
    small_g[f] = small[...]
    for k, g in enumerate((m, n, far)):
        remote(small, small_g.at[g], ms.at[k], mr.at[k], (c, g)).wait()

    def vector(row, size):
        return jnp.concatenate([small_g[g, row : row + 1, :size] for g in range(4)], 1)

    gains_o[0:1] = vector(0, depth)
    gains_o[1:2] = vector(1, depth)
    bias = jnp.concatenate([vector(2, depth), vector(3, key_width // 4), vector(4, key_width // 4)], 1)
    normed = unit * gains_o[0:1]
    n1_o[...] = normed.T.astype(bf16)
    gather_start(output, gs.at[pl.ds(3, 1)], gr.at[pl.ds(3, 1)], place)
    gather_finish(project, gs.at[pl.ds(0, 3)], gr.at[pl.ds(0, 3)], place)
    projected = plain_dot(normed.astype(bf16), wp_o[...]) + bias
    cos, sin = cos_r[...], sin_r[...]
    keys = turn(projected[:, query_width : query_width + key_width].T, cos, sin, HD)
    kv[:, :key_width] = keys.T.astype(bf16)
    kv[:, key_width:] = projected[:, query_width + key_width :].astype(bf16)
    spread_start(kv, kv_o, ks, kr, place, lines)
    kv_o[c] = kv[...]
    q_o[...] = turn(projected[:, :query_width].T, cos, sin, HD).astype(bf16)
    items = [(cot, lambda g, at: cot_o.at[g, at])]
    tokens_start(items, ts, tr, place)
    gather_finish(output, gs.at[pl.ds(3, 1)], gr.at[pl.ds(3, 1)], place)
    spread_finish(kv, kv_o, ks, kr, place, lines)
    spread.lines_out(1)
    spread.on_line(0, True)
    for g in range(KV):
        queries = heads(q_o, g, group, HD)

        def visit(i, state):
            highest, total, acc = state
            at = pl.ds(i * step, step)
            both = kv_o[at].reshape(step * tok, 2 * key_width)
            seen = both[:, g * HD : (g + 1) * HD]
            carried = both[:, key_width + g * HD : key_width + (g + 1) * HD]
            mask = key_bias(i * step * tok, step * tok, c, pos)
            scores = plain_dot(seen, queries) * scale + jnp.concatenate([mask] * group, 1)
            top = jnp.maximum(highest, jnp.max(scores, 0, keepdims=True))
            exps = jnp.exp(scores - top)
            shrink = jnp.exp(highest - top)
            total = total * shrink + jnp.sum(exps, 0, keepdims=True)
            acc = acc * shrink + over_first(carried, exps.astype(bf16))
            return top, total, acc

        state = (
            jnp.full((1, group * tok), MASK_FILL, f32),
            jnp.zeros((1, group * tok), f32),
            jnp.zeros((HD, group * tok), f32),
        )
        blocks = kv_o.shape[0] // step
        if blocks <= 2:
            for i in range(blocks):
                state = visit(i, state)
        else:
            state = lax.fori_loop(0, blocks, visit, state)
        highest, total, acc = state
        attention = acc / total
        logs = highest + jnp.log(total)
        for j in range(group):
            at = slice(j * tok, (j + 1) * tok)
            h = g * group + j
            att_o[h * HD : (h + 1) * HD] = attention[:, at]
            lse_o[h : h + 1] = logs[:, at]
    hidden = values + plain_dot(att_o[...].T.astype(bf16), wo_o[...])
    hid_o[...] = hidden
    inverse = lax.rsqrt(jnp.mean(hidden * hidden, -1, keepdims=True) + EPSILON)
    n2_o[...] = (hidden * inverse * gains_o[1:2]).astype(bf16)
    tokens_finish(items, ts, tr, place)
    kept = spread.keep(cot_o, 0, 1)
    for copy in kept:
        copy.start()
    spread.on_pair(0)
    spread.on_line(1, False)
    spread.finish_line(0)
    spread.finish_pair(0)
    spread.finish_line(1)
    for copy in kept:
        copy.wait()


def heads(ref, g, group, size):
    return jnp.concatenate([ref[pl.ds((g * group + j) * size, size)] for j in range(group)], 1)


def turn_back(grads, cos, sin, size):
    half = size // 2
    pieces = []
    for at in range(0, grads.shape[0], size):
        lead, trail = grads[at : at + half], grads[at + half : at + size]
        pieces += [lead * cos + trail * sin, trail * cos - lead * sin]
    return jnp.concatenate(pieces, 0)


def norm_grad(values, gain, grads):
    inverse = lax.rsqrt(jnp.mean(values * values, -1, keepdims=True) + EPSILON)
    scaled = values * inverse
    weighted = grads * gain
    back = inverse * (weighted - scaled * jnp.mean(weighted * scaled, -1, keepdims=True))
    return back, jnp.sum(grads * scaled, 0, keepdims=True)


class Total:
    def __init__(self, place, lines, low, wide, rest, pay, total, bufs, ss, rs):
        self.place, self.lines, self.pay, self.total = place, lines, pay, total
        self.a_in, self.a_sum, self.a_line, self.b_line, self.b_sum, self.b_in = bufs
        self.ss, self.rs = ss, rs
        self.p, self.x = place[0] // 2, place[0] % 2
        self.height = pay.shape[0] // (2 * lines)
        self.a, self.b = pl.ds(low, wide), pl.ds(low + wide, rest)

    def rows(self, first, count=1):
        return pl.ds(pl.multiple_of(first * self.height, 16), count * self.height)

    def ahead(self, k):
        return lax.rem(self.p + k, self.lines)

    def to_pair(self, way, stage, src, dst):
        c, f, c2 = self.place[:3]
        return remote(src, dst, self.ss.at[way, stage, 0], self.rs.at[way, stage, 0], (c2, f))

    def to_line(self, way, stage, k, src, dst):
        f = self.place[1]
        device = (self.ahead(k) * 2 + self.x, f)
        return remote(src, dst, self.ss.at[way, stage, k], self.rs.at[way, stage, k], device)

    def copies(self, way, stage):
        pay, total, p, x, n = self.pay, self.total, self.p, self.x, self.lines
        every = range(1, n)
        if way == 0:
            own = total.at[self.rows(x * n + p), self.a]
            group = total.at[self.rows(x * n, n), self.a]
            if stage == 0:
                return [self.to_pair(0, 0, pay.at[self.rows((1 - x) * n, n), self.a], self.a_in)]
            if stage == 1:
                return [
                    self.to_line(0, 1, k, self.a_sum.at[self.rows(self.ahead(k))], self.a_line.at[k - 1]) for k in every
                ]
            if stage == 2:
                return [self.to_line(0, 2, k, own, own) for k in every]
            return [self.to_pair(0, 3, group, group)]
        own = total.at[self.rows(p * 2 + x), self.b]
        both = total.at[self.rows(p * 2, 2), self.b]
        if stage == 0:
            return [
                self.to_line(1, 0, k, pay.at[self.rows(self.ahead(k) * 2, 2), self.b], self.b_line.at[k - 1])
                for k in every
            ]
        if stage == 1:
            return [self.to_pair(1, 1, self.b_sum.at[self.rows(1 - x)], self.b_in)]
        if stage == 2:
            return [self.to_pair(1, 2, own, own)]
        return [self.to_line(1, 3, k, both, both) for k in every]

    def start(self, stage):
        for way in range(2):
            for copy in self.copies(way, stage):
                copy.start()

    def wait(self, stage):
        pay, total, p, x, n = self.pay, self.total, self.p, self.x, self.lines
        for way in range(2):
            for copy in self.copies(way, stage):
                copy.wait()
        if stage == 0:
            value = pay[self.rows(x * n, n), self.a].astype(f32) + self.a_in[...].astype(f32)
            self.a_sum[...] = value.astype(bf16)
            value = pay[self.rows(p * 2, 2), self.b].astype(f32)
            for k in range(1, n):
                value = value + self.b_line[k - 1].astype(f32)
            self.b_sum[...] = value.astype(bf16)
        if stage == 1:
            value = self.a_sum[self.rows(p)].astype(f32)
            for k in range(1, n):
                value = value + self.a_line[k - 1].astype(f32)
            total[self.rows(x * n + p), self.a] = value.astype(bf16)
            value = self.b_sum[self.rows(x)].astype(f32) + self.b_in[...].astype(f32)
            total[self.rows(p * 2 + x), self.b] = value.astype(bf16)


def sum_buffers(lines, tall, wide, rest):
    height = tall // (2 * lines)
    shapes = (
        (lines * height, wide), (lines * height, wide), (lines - 1, height, wide),
        (lines - 1, 2 * height, rest), (2 * height, rest), (height, rest),
    )
    return [pltpu.VMEM(shape, bf16) for shape in shapes]


def back_body(
    ctx, step, block, chunk, ready,
    gn, hid, gains, cot, wo, att_t, q_t, kv, pos, lse, cos_r, sin_r, n1_t, inp, wp, n2, n2_g,
    cot_g, cot_a0, cot_a1, cot_b0, cot_b1, cot_fb0, x_a0, x_a1, wg_h, wu_h, wd_h,
    inp_o, grads_o, acc_g, acc_u, acc_d, x_b0, x_b1, x_fa0, x_fa1, x_fb0, x_fb1, cot_fa0, cot_fa1, cot_fb1,
    gh, do_t, part, dq, held, ghl, ghl_g, low_t, n1_g, low_g, gp, gp_g, vec, vec_g,
    pay, total_r, p0, p1, p2, p3, p4, p5, q0, q1, q2, q3, q4, q5,
    xs, cs, wg, wu, wd, acc,
    ks, kr, ts, tr, as_, ar, vs, vr, sum_s, sum_r, ws, ins, outs, *sems
):
    place = where_am_i()
    c, f, c2, m, n = place
    far = (m + 2) % 4
    peers = [lax.rem(c + k, ctx) for k in range(1, ctx)]
    greet([(p, f) for p in peers] + [(c, m), (c, n), (c, far)])
    tok, width = cot.shape
    group = H // KV
    depth = n1_g.shape[1]
    scale = HD ** (-0.5)

    def rows(g):
        return pl.ds(pl.multiple_of(g * depth, 16), depth)

    def swaps():
        return [
            remote(src.at[rows(g)], dst.at[f], as_.at[j, k], ar.at[j, k], (c, g))
            for j, (src, dst) in enumerate(((n1_t, n1_g), (low_t, low_g)))
            for k, g in enumerate((n, far, m))
        ]

    ready()
    spread = Spread(place, ctx // 2, n2, n2_g, ((x_a0, x_a1), (x_b0, x_b1), (x_fa0, x_fa1), (x_fb0, x_fb1)), sems[:9])
    rest = Spread(
        place, ctx // 2, cot, cot_g, ((cot_a0, cot_a1), None, (cot_fa0, cot_fa1), (cot_fb0, cot_fb1)), sems[9:]
    )
    rest.pairs_out(2)
    spread.lines_out(1)
    rest.cross(0)
    rest.cross(1)
    kept = spread.keep(n2_g, 1, 2, 3) + rest.keep(cot_g, 2)
    loads = [
        pltpu.make_async_copy(src, dst, ws.at[j])
        for j, (src, dst) in enumerate(((wg_h, wg), (wu_h, wu), (wd_h, wd)))
    ]
    for copy in kept + loads:
        copy.start()
    low_t[...] = att_t[...].astype(bf16)
    back, gain_two = norm_grad(hid[...], gains[1:2], gn[...])
    gh[...] = cot[...].astype(f32) + back
    ghl[...] = gh[...].astype(bf16)
    items = [(ghl, lambda g, at: ghl_g.at[g, at])]
    tokens_start(items, ts.at[0], tr.at[0], place)
    for copy in swaps():
        copy.start()
    n1_g[f] = n1_t[rows(f)]
    low_g[f] = low_t[rows(f)]
    do_t[...] = over_last(wo[...], ghl[...]).astype(bf16)
    key_width = KV * HD
    for g in range(KV):
        queries, grads = heads(q_t, g, group, HD), heads(do_t, g, group, HD)
        delta = jnp.sum(grads.astype(f32) * heads(att_t, g, group, HD), 0, keepdims=True)
        total = jnp.concatenate([lse[pl.ds(g * group + j, 1)] for j in range(group)], 1)

        @pl.loop(0, kv.shape[0] // step)
        def _(i):
            at = pl.ds(i * step, step)
            both = kv[at].reshape(step * tok, 2 * key_width)
            keys = both[:, g * HD : (g + 1) * HD]
            values = both[:, key_width + g * HD : key_width + (g + 1) * HD]
            bias = key_bias(i * step * tok, step * tok, c, pos)
            scores = plain_dot(keys, queries) * scale + jnp.concatenate([bias] * group, 1)
            probs = jnp.exp(scores - total)
            g_probs = plain_dot(values, grads)
            g_scores = (probs * (g_probs - delta)).astype(bf16)
            g_keys = over_last(g_scores, queries) * scale
            g_values = over_last(probs.astype(bf16), grads)
            part[at, :, g * HD : (g + 1) * HD] = g_keys.astype(bf16).reshape(step, tok, HD)
            part[at, :, key_width + g * HD : key_width + (g + 1) * HD] = g_values.astype(bf16).reshape(
                step, tok, HD
            )
            g_queries = over_first(keys, g_scores) * scale

            @pl.when(i == 0)
            def _():
                dq[g] = g_queries

            @pl.when(i > 0)
            def _():
                dq[g] += g_queries

    owners = [remote(part.at[p], held.at[k], ks.at[k], kr.at[k], (p, f)) for k, p in enumerate(peers)]
    for copy in owners:
        copy.start()
    tokens_finish(items, ts.at[0], tr.at[0], place)
    for copy in swaps():
        copy.wait()
    cos, sin = cos_r[...], sin_r[...]
    g_q = [
        turn_back(dq[g, :, j * tok : (j + 1) * tok], cos, sin, HD) for g in range(KV) for j in range(group)
    ]
    g_q = jnp.concatenate(g_q, 0)
    query_width = g_q.shape[0]
    gp[:, :query_width] = g_q.T.astype(bf16)
    columns = gp.shape[1]
    low_all = jnp.concatenate([low_g[g] for g in range(4)], 1)
    pay[pl.ds(0, depth), pl.ds(columns, width)] = plain_dot(low_all, ghl_g[...].reshape(4 * tok, width)).astype(
        bf16
    )
    pay[pl.ds(depth, pay.shape[0] - depth)] = jnp.zeros((pay.shape[0] - depth, pay.shape[1]), bf16)
    third = width // 7
    early = Total(
        place, ctx // 2, columns, 5 * third, 2 * third, pay, total_r, (p0, p1, p2, p3, p4, p5), sum_s.at[0], sum_r.at[0]
    )
    late = Total(
        place, ctx // 2, 0, 6 * third, 3 * third, pay, total_r, (q0, q1, q2, q3, q4, q5), sum_s.at[1], sum_r.at[1]
    )
    pairs = part[c].astype(f32)
    for k, copy in enumerate(owners):
        copy.wait()
        pairs = pairs + held[k].astype(f32)
    early.start(0)
    spread.lines_out(2)
    g_k = turn_back(pairs[:, :key_width].T, cos, sin, HD)
    gp[:, query_width : query_width + key_width] = g_k.T.astype(bf16)
    gp[:, query_width + key_width :] = pairs[:, key_width:].astype(bf16)
    items = [(gp, lambda g, at: gp_g.at[g, at])]
    tokens_start(items, ts.at[1], tr.at[1], place)
    spread.on_line(1, True)
    g_normed = over_last(gp[...], wp[...])
    values = inp[...].astype(f32)
    back, gain_one = norm_grad(values, gains[0:1], g_normed)
    inp_o[...] = (gh[...] + back).astype(bf16)
    vec[...] = jnp.zeros_like(vec)
    vec[0:1, :width] = gain_one
    vec[1:2, :width] = gain_two
    vec[2:3, :columns] = jnp.sum(gp[...].astype(f32), 0, keepdims=True)
    vectors = [remote(vec, vec_g.at[k], vs.at[k], vr.at[k], (c, g)) for k, g in enumerate((m, n, far))]
    for copy in vectors:
        copy.start()
    early.wait(0)
    early.start(1)
    tokens_finish(items, ts.at[1], tr.at[1], place)
    n1_all = jnp.concatenate([n1_g[g] for g in range(4)], 1)
    pay[pl.ds(0, depth), pl.ds(0, columns)] = plain_dot(n1_all, gp_g[...].reshape(4 * tok, columns)).astype(bf16)
    total = vec[...]
    for k, copy in enumerate(vectors):
        copy.wait()
        total = total + vec_g[k]
    pay[pl.ds(depth, 8), :columns] = total[:, :columns].astype(bf16)
    early.wait(1)
    early.start(2)
    late.start(0)
    spread.cross(0)
    spread.cross(1)
    for copy in loads:
        copy.wait()
    parts = (((x_a0, x_a1), (cot_a0, cot_a1)), ((x_b0, x_b1), (cot_b0, cot_b1)))
    blocks = wg.shape[0] // block
    per_part = ctx * tok // chunk
    for way, sides in enumerate(parts):
        if way == 1:
            spread.finish_line(1)
            kept[0].wait()
            spread.finish_pair(1)
        for i in range(per_part):
            count = chunk // tok // 2
            at = pl.ds(i * count, count)
            fetch = [
                pltpu.make_async_copy(sides[j][side].at[at], into.at[side], ins.at[j, side])
                for j, into in enumerate((xs, cs))
                for side in range(2)
            ]
            for copy in fetch:
                copy.start()
            for copy in fetch:
                copy.wait()
            tokens = xs[...].reshape(chunk, width), cs[...].reshape(chunk, width)
            first = way == 0 and i == 0
            last = way == 1 and i == per_part - 1

            @pl.loop(0, blocks)
            def _(b):
                at = pl.ds(pl.multiple_of(b * block, 16), block)
                act, g_gate, g_up = hidden_units(*tokens, wg[at], wu[at], wd[at])
                for j, (left, right) in enumerate(((g_gate, 0), (g_up, 0), (act, 1))):
                    value = plain_dot(left, tokens[right])
                    if first:
                        acc[j, at] = value
                    else:
                        acc[j, at] += value
                if first:

                    @pl.when(b == 0)
                    def _():
                        early.wait(2)
                        early.start(3)
                        rest.on_y(0)
                        rest.on_y(1)

                    @pl.when(b == 1)
                    def _():
                        late.wait(0)
                        late.start(1)

                    @pl.when(b == 2)
                    def _():
                        early.wait(3)
                        rest.on_pair(2)
                        spread.on_line(2, True)

                    @pl.when(b == 3)
                    def _():
                        late.wait(1)
                        late.start(2)

                if way == 0 and i == 0:

                    @pl.when(b == 2)
                    def _():
                        spread.on_pair(1)

                if way == 1 and i == 0:

                    @pl.when(b == 0)
                    def _():
                        spread.on_y(0)

                    @pl.when(b == 1)
                    def _():
                        late.wait(2)
                        late.start(3)
                        spread.on_y(1)

                    @pl.when(b == 3)
                    def _():
                        spread.on_pair(2)

                if last:
                    for j, out in enumerate((acc_g, acc_u, acc_d)):
                        pltpu.make_async_copy(acc.at[j, at], out.at[at], outs.at[b, j]).start()

    late.wait(3)
    grads_o[...] = total_r[...].astype(f32)
    spread.finish_line(2)
    spread.finish_pair(2)
    spread.finish_cross()
    rest.finish_pair(2)
    rest.finish_cross()
    for b in range(blocks):
        at = pl.ds(b * block, block)
        for j, out in enumerate((acc_g, acc_u, acc_d)):
            pltpu.make_async_copy(acc.at[j, at], out.at[at], outs.at[b, j]).wait()
    for copy in kept[1:]:
        copy.wait()


def over_last(a, b):
    return lax.dot_general(a, b, (((1,), (1,)), ((), ())), preferred_element_type=f32)


def over_first(a, b):
    return lax.dot_general(a, b, (((0,), (0,)), ((), ())), preferred_element_type=f32)


def plain_dot(a, b):
    return jnp.dot(a, b, preferred_element_type=f32)


def hidden_units(x, cot, wg, wu, wd):
    return gates(over_last(wg, x), over_last(wu, x), over_last(wd, cot))


def hidden_body(
    chunk, block, windows, x0_h, x1_h, x2_h, x3_h, c0_h, c1_h, c2_h, c3_h, wg_h, wu_h, wd_h, ig_h, iu_h, id_h, *refs
):
    passed, refs = refs[:4], refs[4:]
    og_h, ou_h, od_h = refs[:3]
    results_out, refs = refs[3 : 3 + len(windows)], refs[3 + len(windows) :]
    xs, cs, wg, wu, wd, acc, in_sem, w_sem, out_sem, init_sem, pass_sem = refs[:11]
    through = []
    for j, (which, at) in enumerate(windows):
        src = passed[which] if at is None else passed[which].at[at]
        buffer = refs[11 + j]
        through.append(
            (
                pltpu.make_async_copy(src, buffer, pass_sem.at[0, j]),
                pltpu.make_async_copy(buffer, results_out[j], pass_sem.at[1, j]),
            )
        )
    parts = (((x0_h, x1_h), (c0_h, c1_h)), ((x2_h, x3_h), (c2_h, c3_h)))
    rows = 4 * x0_h.shape[0]
    steps, blocks, held = rows // chunk, wg.shape[0] // block, xs.shape[0] // chunk
    def weights(b):
        at = pl.ds(b * block, block)
        return [
            pltpu.make_async_copy(src.at[at], dst.at[at], w_sem.at[b, j])
            for j, (src, dst) in enumerate(((wg_h, wg), (wu_h, wu), (wd_h, wd)))
        ]

    def fetch(i, begin, part):
        half = chunk // 2
        src = pl.ds(pl.multiple_of(begin * half, half), half)
        slot = i % held
        return [
            pltpu.make_async_copy(
                part[j][side].at[src],
                into.at[pl.ds(pl.multiple_of(slot * chunk + side * half, half), half)],
                in_sem.at[slot, j, side],
            )
            for j, into in enumerate((xs, cs))
            for side in range(2)
        ]

    def start_tokens(i):
        begin = 0
        for part in parts:
            count = 2 * x0_h.shape[0] // chunk

            def go(begin=begin, part=part):
                for copy in fetch(i, i - begin, part):
                    copy.start()

            if isinstance(i, int):
                if begin <= i < begin + count:
                    go()
            else:
                pl.when((i >= begin) & (i < begin + count))(go)
            begin += count

    def wait_tokens(i):
        for copy in fetch(i, 0, parts[0]):
            copy.wait()

    def results(b, slot):
        at = pl.ds(pl.multiple_of(b * block, 16), block)
        return [
            pltpu.make_async_copy(acc.at[slot, j], out.at[at], out_sem.at[slot, j])
            for j, out in enumerate((og_h, ou_h, od_h))
        ]

    def initial(b, slot):
        at = pl.ds(pl.multiple_of(b * block, 16), block)
        return [
            pltpu.make_async_copy(src.at[at], acc.at[slot, j], init_sem.at[slot, j])
            for j, src in enumerate((ig_h, iu_h, id_h))
        ]

    resident = held == steps
    slots = acc.shape[0]
    start_tokens(0)
    for copy in weights(0):
        copy.start()
    for copy in weights(0):
        copy.wait()
    for copy in initial(0, 0):
        copy.start()
    for i in range(1, held if resident else 1):
        start_tokens(i)
    for b in range(1, slots):
        for copy in weights(b) + initial(b, b):
            copy.start()
    for copy, _ in through:
        copy.start()

    @pl.loop(0, blocks)
    def _(b):
        slot = b % slots
        at = pl.ds(pl.multiple_of(b * block, 16), block)

        @pl.when(b == 1)
        def _():
            for copy in weights(1):
                copy.wait()
            for into, out in through:
                into.wait()
                out.start()

        @pl.loop(0, steps)
        def _(i):
            if resident:

                @pl.when(b == 0)
                def _():
                    wait_tokens(i)

            else:
                wait_tokens(i)

                @pl.when((i + 1 < steps) | (b + 1 < blocks))
                def _():
                    start_tokens(lax.rem(i + 1, steps))

            t = pl.ds(pl.multiple_of(i % held * chunk, chunk), chunk)
            x, cot = xs[t], cs[t]
            act, g_gate, g_up = hidden_units(x, cot, wg[at], wu[at], wd[at])

            @pl.when(i == 0)
            def _():
                for copy in initial(b, slot):
                    copy.wait()

            acc[slot, 0] += plain_dot(g_gate, x)
            acc[slot, 1] += plain_dot(g_up, x)
            acc[slot, 2] += plain_dot(act, cot)

        for copy in results(b, slot):
            copy.start()

    for b in range(max(0, blocks - slots), blocks):
        for copy in results(b, b % slots):
            copy.wait()
    for _, out in through:
        out.wait()


def hidden_grads(xs, cots, wg, wu, wd, initial, passed, windows):
    width = wg.shape[1]
    xs, cots = [[part.reshape(-1, width) for part in parts] for parts in (xs, cots)]
    rows = sum(part.shape[0] for part in xs)
    units = wg.shape[0]
    chunk = math.gcd(rows // 2, 1024)
    block = units // 2
    held = min(rows // chunk, 4)
    any_spec = pl.BlockSpec(memory_space=pl.ANY)
    dma = pltpu.SemaphoreType.DMA
    return pl.pallas_call(
        functools.partial(hidden_body, chunk, block, [window[:2] for window in windows]),
        out_shape=(jax.ShapeDtypeStruct((units, width), f32),) * 3
        + tuple(jax.ShapeDtypeStruct(shape, dtype) for _, _, shape, dtype in windows),
        in_specs=[any_spec] * 18,
        out_specs=(any_spec,) * (3 + len(windows)),
        scratch_shapes=[pltpu.VMEM((held * chunk, width), bf16)] * 2
        + [pltpu.VMEM((units, width), bf16)] * 3
        + [pltpu.VMEM((2, 3, block, width), f32), dma((held, 2, 2)), dma((2, 3)), dma((2, 3)), dma((2, 3))]
        + [dma((2, len(windows)))]
        + [pltpu.VMEM(shape, dtype) for _, _, shape, dtype in windows],
        compiler_params=pltpu.CompilerParams(vmem_limit_bytes=62 << 20),
        cost_estimate=pl.CostEstimate(
            flops=12 * rows * width * units, bytes_accessed=4 * rows * width + 18 * units * width, transcendentals=0
        ),
        name="hidden_grads",
    )(*xs, *cots, wg, wu, wd, *initial, *passed)


def shards(
    layer_input,
    seq_ids,
    positions,
    norm_gain,
    w_query,
    b_query,
    w_key,
    b_key,
    w_value,
    b_value,
    w_output,
    mlp_gain,
    w_gate,
    w_up,
    w_down,
    cotangent,
):
    tok = layer_input.shape[1]
    width = layer_input.shape[2]
    group = H // KV
    query_width = H * HD
    key_width = KV * HD
    score_scale = HD ** (-0.5)
    ctx = lax.axis_size("ctx")
    fsdp = lax.axis_size("fsdp")
    depth = width // fsdp
    lines = ctx // 2
    c, f = lax.axis_index("ctx"), lax.axis_index("fsdp")
    seq_length = ctx * tok
    dma = pltpu.SemaphoreType.DMA
    sds = jax.ShapeDtypeStruct
    input_rows = layer_input[0]
    grad_out = cotangent[0]
    own_segment = seq_ids[0]
    own_positions = positions[0]
    query_rows = c * tok + jnp.arange(tok, dtype=jnp.int32)

    cosine, sine_table = rope_tables(own_positions, HD)
    own_positions = own_positions[None]
    step = math.gcd(ctx, 4)
    columns = query_width + 2 * key_width
    hbm = pl.BlockSpec(memory_space=pltpu.HBM)
    half_blocks = sds((lines, 2, tok // 2, width), bf16)
    (w_project, wo_full, gains, n1_t, q_t, kv_all, cot_group, att_t, log_total, hidden_state, normed_second,
     cot_a0, cot_a1, cot_b0) = (
        staged_call(
            functools.partial(front_body, lines, step),
            (
                input_rows, grad_out, norm_gain, mlp_gain, b_query, b_key, b_value, own_positions, cosine, sine_table,
                w_query, w_key, w_value, w_output,
            ),
            (10, 11, 12, 13),
            (
                sds((width, columns), bf16),
                sds((query_width, width), bf16),
                sds((8, width), f32),
                sds((width, tok), bf16),
                sds((query_width, tok), bf16),
                sds((ctx, tok, 2 * key_width), bf16),
                sds((fsdp, tok, width), bf16),
                sds((query_width, tok), f32),
                sds((H, tok), f32),
                sds((tok, width), f32),
                sds((tok, width), bf16),
                half_blocks,
                half_blocks,
                half_blocks,
            ),
            (11, 12, 13),
            [
                pltpu.VMEM((tok, 2 * key_width), bf16),
                pltpu.VMEM((8, 256), f32),
                pltpu.VMEM((fsdp, 8, 256), f32),
                dma((3,)),
                dma((3,)),
            ]
            + gather_sems(4)
            + [dma((2, lines)), dma((2, lines))]
            + gather_sems(1)
            + spread_sems(lines),
            0,
            "front",
            pl.CostEstimate(flops=4 * 10**9, bytes_accessed=10**7, transcendentals=0),
        )
    )
    units = w_down.shape[0]
    wg_t, wu_t = w_gate.T, w_up.T
    grad_normed2, block_out, x_group, cot_b1, cot_fb0, x_a0, x_a1 = staged_call(
        functools.partial(mid_body, lines),
        (normed_second, cot_group, grad_out, cot_a0, cot_a1, cot_b0, hidden_state, wg_t, wu_t, w_down),
        (3, 4, 5, 7, 8, 9),
        (
            sds((tok, width), f32),
            sds((tok, width), bf16),
            sds((fsdp, tok, width), bf16),
        )
        + (half_blocks,) * 4,
        (3, 4, 5, 6),
        [pltpu.VMEM((units, width), bf16)] * 3
        + [
            pltpu.VMEM((3, 2 * tok, units), bf16),
            pltpu.VMEM((2, tok, width), f32),
            pltpu.VMEM((8, tok, width), bf16),
            pltpu.VMEM((2, tok, width), bf16),
            pltpu.VMEM((2, tok, width), bf16),
            dma((3,)),
            dma((5,)),
            dma((5,)),
            dma((6,)),
            dma((6,)),
        ]
        + spread_sems(lines)
        + spread_sems(lines),
        2,
        "mid",
        pl.CostEstimate(
            flops=12 * fsdp * tok * width * units, bytes_accessed=6 * units * width, transcendentals=0
        ),
    )
    tall, everything = max(256, 16 * ctx), columns + width
    third = width // 7
    block = units // 4
    chunk = math.gcd(ctx * tok, 1024)
    big = sds((units, width), f32)
    (
        input_grad, weight_grads, acc_g, acc_u, acc_d, x_b0, x_b1, x_fa0, x_fa1, x_fb0, x_fb1, cot_fa0, cot_fa1,
        cot_fb1,
    ) = staged_call(
        functools.partial(back_body, ctx, step, block, chunk),
        (
            grad_normed2, hidden_state, gains, grad_out, wo_full, att_t, q_t, kv_all, own_positions, log_total,
            cosine, sine_table, n1_t, input_rows, w_project, normed_second, x_group, cot_group, cot_a0,
            cot_a1, cot_b0, cot_b1, cot_fb0, x_a0, x_a1, wg_t, wu_t, w_down,
        ),
        (18, 19, 20, 21, 22, 23, 24, 25, 26, 27),
        (sds((tok, width), bf16), sds((tall, everything), f32), big, big, big) + (half_blocks,) * 9,
        tuple(range(2, 14)),
        [
            pltpu.VMEM((tok, width), f32),
            pltpu.VMEM((query_width, tok), bf16),
            pltpu.VMEM((ctx, tok, 2 * key_width), bf16),
            pltpu.VMEM((KV, HD, group * tok), f32),
            pltpu.VMEM((ctx - 1, tok, 2 * key_width), bf16),
            pltpu.VMEM((tok, width), bf16),
            pltpu.VMEM((fsdp, tok, width), bf16),
            pltpu.VMEM((query_width, tok), bf16),
            pltpu.VMEM((fsdp, depth, tok), bf16),
            pltpu.VMEM((fsdp, depth, tok), bf16),
            pltpu.VMEM((tok, columns), bf16),
            pltpu.VMEM((fsdp, tok, columns), bf16),
            pltpu.VMEM((8, everything), f32),
            pltpu.VMEM((3, 8, everything), f32),
            pltpu.VMEM((tall, everything), bf16),
            pltpu.VMEM((tall, everything), bf16),
            *sum_buffers(lines, tall, 5 * third, 2 * third),
            *sum_buffers(lines, tall, 6 * third, 3 * third),
            pltpu.VMEM((2, chunk // tok // 2, 2, tok // 2, width), bf16),
            pltpu.VMEM((2, chunk // tok // 2, 2, tok // 2, width), bf16),
            pltpu.VMEM((units, width), bf16),
            pltpu.VMEM((units, width), bf16),
            pltpu.VMEM((units, width), bf16),
            pltpu.VMEM((3, units, width), f32),
            dma((ctx - 1,)),
            dma((ctx - 1,)),
            dma((2, 1, 6)),
            dma((2, 1, 6)),
            dma((2, 3)),
            dma((2, 3)),
            dma((3,)),
            dma((3,)),
            dma((2, 2, 4, lines)),
            dma((2, 2, 4, lines)),
            dma((3,)),
            dma((2, 2)),
            dma((4, 3)),
        ]
        + spread_sems(lines)
        + spread_sems(lines),
        3,
        "back",
        pl.CostEstimate(flops=4 * 10**10, bytes_accessed=6 * 10**7, transcendentals=0),
    )
    starts = ((0, 0, width), (1, 0, width), (2, 0, query_width), (2, query_width, key_width),
              (2, query_width + key_width, key_width))

    def piece(row, start, size):
        share = size // fsdp
        return lax.dynamic_slice_in_dim(weight_grads[depth + row], start + f * share, share, 0)

    own = [piece(*at) for at in starts]

    ends = (0, query_width, query_width + key_width, columns, columns + width)
    windows = [
        (0, (slice(0, depth), slice(ends[j], ends[j + 1])), (depth, ends[j + 1] - ends[j]), f32) for j in range(4)
    ]
    windows += [(1, None, (tok, width), bf16), (2, None, (tok, width), bf16), (3, None, (H, tok), f32)]
    gate_grad, up_grad, down_grad, query_grad, key_grad, value_grad, output_grad, block_out, input_grad, lse = (
        hidden_grads(
            (x_fa0, x_fa1, x_fb0, x_fb1), (cot_fa0, cot_fa1, cot_fb0, cot_fb1), wg_t, wu_t, w_down,
            (acc_g, acc_u, acc_d), (weight_grads, block_out, input_grad, log_total), windows,
        )
    )
    return (
        block_out[None],
        input_grad[None],
        own[0],
        query_grad,
        own[2],
        key_grad,
        own[3],
        value_grad,
        own[4],
        output_grad,
        own[1],
        gate_grad.T,
        up_grad.T,
        down_grad,
        lse[None],
    )


def solution(mesh):
    in_specs = (
        P("fsdp", "ctx", None),
        P("fsdp", "ctx"),
        P("fsdp", "ctx"),
        P("fsdp"),
        P("fsdp", None),
        P("fsdp"),
        P("fsdp", None),
        P("fsdp"),
        P("fsdp", None),
        P("fsdp"),
        P("fsdp", None),
        P("fsdp"),
        P(None, "fsdp"),
        P(None, "fsdp"),
        P("fsdp", None),
        P("fsdp", "ctx", None),
    )
    out_specs = (
        P("fsdp", "ctx", None),
        P("fsdp", "ctx", None),
        P("fsdp"),
        P("fsdp", None),
        P("fsdp"),
        P("fsdp", None),
        P("fsdp"),
        P("fsdp", None),
        P("fsdp"),
        P("fsdp", None),
        P("fsdp"),
        P(None, "fsdp"),
        P(None, "fsdp"),
        P("fsdp", None),
        P("fsdp", None, "ctx"),
    )

    return jax.shard_map(shards, mesh=mesh, in_specs=in_specs, out_specs=out_specs, check_vma=False)
```

```python
import functools
import math

import jax
import jax.numpy as jnp
from jax import lax
from jax.experimental import pallas as pl
from jax.experimental.pallas import tpu as pltpu
from jax.sharding import PartitionSpec as P

H = 14
KV = 2
HD = 64


EPSILON = 1e-06
ROPE_BASE = 1000000.0
MASK_FILL = -1e30
MESH = pl.DeviceIdType.MESH
VMEM = pl.BlockSpec(memory_space=pltpu.VMEM)
f32 = jnp.float32
bf16 = jnp.bfloat16


def rope_tables(positions, head_dim):
    half = head_dim // 2
    freq = ROPE_BASE ** (-(jnp.arange(half, dtype=jnp.float32) * 2.0 / head_dim))
    angle = positions.astype(jnp.float32)[None, :] * freq[:, None]
    return jnp.cos(angle), jnp.sin(angle)


def remote(src, dst, send_sem, recv_sem, device):
    return pltpu.make_async_remote_copy(
        src_ref=src, dst_ref=dst, send_sem=send_sem, recv_sem=recv_sem, device_id=device,
        device_id_type=MESH,
    )


def where_am_i():
    c, f = lax.axis_index("ctx"), lax.axis_index("fsdp")
    c2 = c + 1 - 2 * (c % 2)
    m = f + 1 - 2 * (f % 2)
    n = (f + 2) % 4
    return c, f, c2, m, n


def greet(devices):
    barrier = pltpu.get_barrier_semaphore()
    for device in devices:
        pl.semaphore_signal(barrier, inc=1, device_id=device, device_id_type=MESH)
    pl.semaphore_wait(barrier, len(devices))


def gather_start(items, ss, rs, place):
    c, f, c2, m, n = place
    h = c % 2
    for i, (src, dst) in enumerate(items):
        half = src.shape[0] // 2
        rows = pl.ds(h * half, half)
        remote(src.at[rows], dst(f).at[rows], ss.at[i, 1], rs.at[i, 1], (c, n)).start()
    for i, (src, dst) in enumerate(items):
        remote(src, dst(f), ss.at[i, 0], rs.at[i, 0], (c, m)).start()
        pltpu.make_async_copy(src, dst(f), ss.at[i, 5]).start()


def gather_finish(items, ss, rs, place):
    c, f, c2, m, n = place
    h = c % 2
    far = (m + 2) % 4
    for i, (src, dst) in enumerate(items):
        half = src.shape[0] // 2
        mine = dst(n).at[pl.ds(h * half, half)]
        remote(mine, mine, ss.at[i, 1], rs.at[i, 1], (c, n)).wait_recv()
        remote(mine, mine, ss.at[i, 2], rs.at[i, 2], (c2, f)).start()
        remote(mine, mine, ss.at[i, 3], rs.at[i, 3], (c, m)).start()
    for i, (src, dst) in enumerate(items):
        half = src.shape[0] // 2
        other = dst(n).at[pl.ds((1 - h) * half, half)]
        remote(other, other, ss.at[i, 2], rs.at[i, 2], (c2, f)).wait_recv()
        remote(other, other, ss.at[i, 4], rs.at[i, 4], (c, m)).start()
    for i, (src, dst) in enumerate(items):
        half = src.shape[0] // 2
        mine, other = pl.ds(h * half, half), pl.ds((1 - h) * half, half)
        remote(src, dst(m), ss.at[i, 0], rs.at[i, 0], (c, m)).wait()
        remote(src.at[mine], dst(f).at[mine], ss.at[i, 1], rs.at[i, 1], (c, n)).wait_send()
        remote(src.at[mine], dst(n).at[mine], ss.at[i, 2], rs.at[i, 2], (c2, f)).wait_send()
        remote(src.at[mine], dst(far).at[mine], ss.at[i, 3], rs.at[i, 3], (c, m)).wait()
        remote(src.at[other], dst(far).at[other], ss.at[i, 4], rs.at[i, 4], (c, m)).wait()
        pltpu.make_async_copy(src, dst(f), ss.at[i, 5]).wait()


def tokens_start(items, ss, rs, place):
    c, f, c2, m, n = place
    for i, (src, dst) in enumerate(items):
        half = src.shape[0] // 2
        for j in range(2):
            rows = pl.ds(j * half, half)
            remote(src.at[rows], dst(f, rows), ss.at[i, 1 + j], rs.at[i, 1 + j], (c, n)).start()
    for i, (src, dst) in enumerate(items):
        rows = pl.ds(0, src.shape[0])
        remote(src, dst(f, rows), ss.at[i, 0], rs.at[i, 0], (c, m)).start()
        dst(f, rows)[...] = src[...]


def tokens_finish(items, ss, rs, place):
    c, f, c2, m, n = place
    far = (m + 2) % 4
    for i, (src, dst) in enumerate(items):
        half = src.shape[0] // 2
        for j in range(2):
            here = dst(n, pl.ds(j * half, half))
            remote(here, here, ss.at[i, 1 + j], rs.at[i, 1 + j], (c, n)).wait_recv()
            remote(here, here, ss.at[i, 3 + j], rs.at[i, 3 + j], (c, m)).start()
    for i, (src, dst) in enumerate(items):
        half = src.shape[0] // 2
        remote(src, dst(m, pl.ds(0, src.shape[0])), ss.at[i, 0], rs.at[i, 0], (c, m)).wait()
        for j in range(2):
            rows = pl.ds(j * half, half)
            remote(src.at[rows], dst(f, rows), ss.at[i, 1 + j], rs.at[i, 1 + j], (c, n)).wait_send()
            remote(src.at[rows], dst(far, rows), ss.at[i, 3 + j], rs.at[i, 3 + j], (c, m)).wait()


def gather_sems(count):
    return [pltpu.SemaphoreType.DMA((count, 6)), pltpu.SemaphoreType.DMA((count, 6))]


def staged_call(body, args, in_hbm, out_shape, out_hbm, scratch, ident, name, cost):
    hbm = pl.BlockSpec(memory_space=pltpu.HBM)
    staged_in = [i for i in range(len(args)) if i not in in_hbm]
    staged_out = [i for i in range(len(out_shape)) if i not in out_hbm]

    def kernel(*refs):
        ins, outs = list(refs[: len(args)]), list(refs[len(args) : len(args) + len(out_shape)])
        rest = list(refs[len(args) + len(out_shape) :])
        own, rest = rest[: len(scratch)], rest[len(scratch) :]
        in_sem, out_sem = rest[-2:]
        copies_in, copies_out = [], []
        for j, i in enumerate(staged_in):
            buffer = rest.pop(0)
            copies_in.append(pltpu.make_async_copy(ins[i], buffer, in_sem.at[j]))
            ins[i] = buffer
        for j, i in enumerate(staged_out):
            buffer = rest.pop(0)
            copies_out.append(pltpu.make_async_copy(buffer, outs[i], out_sem.at[j]))
            outs[i] = buffer
        for copy in copies_in:
            copy.start()

        def ready():
            for copy in copies_in:
                copy.wait()

        body(ready, *ins, *outs, *own)
        for copy in copies_out:
            copy.start()
        for copy in copies_out:
            copy.wait()

    buffers = [pltpu.VMEM(args[i].shape, args[i].dtype) for i in staged_in]
    buffers += [pltpu.VMEM(out_shape[i].shape, out_shape[i].dtype) for i in staged_out]
    sems = [pltpu.SemaphoreType.DMA((len(staged_in),)), pltpu.SemaphoreType.DMA((len(staged_out),))]
    return pl.pallas_call(
        kernel,
        out_shape=out_shape,
        in_specs=[hbm] * len(args),
        out_specs=(hbm,) * len(out_shape),
        scratch_shapes=scratch + buffers + sems,
        compiler_params=pltpu.CompilerParams(
            collective_id=ident, has_side_effects=True, vmem_limit_bytes=67_043_328
        ),
        cost_estimate=cost,
        name=name,
    )(*args)


def spread_start(src, dst, ss, rs, place, lines):
    c, f, c2, m, n = place
    for k in range(1, lines):
        p = lax.rem(c // 2 + k, lines) * 2 + c % 2
        remote(src, dst.at[c], ss.at[0, k], rs.at[0, k], (p, f)).start()
    remote(src, dst.at[c], ss.at[1, 0], rs.at[1, 0], (c2, f)).start()


def spread_finish(src, dst, ss, rs, place, lines):
    c, f, c2, m, n = place
    for k in range(1, lines):
        giver = lax.rem(c // 2 + lines - k, lines) * 2 + c % 2
        block = dst.at[giver]
        remote(block, block, ss.at[0, k], rs.at[0, k], (c2, f)).wait_recv()
        remote(block, block, ss.at[1, k], rs.at[1, k], (c2, f)).start()
    for k in range(lines):
        giver = lax.rem(c2 // 2 + lines - k, lines) * 2 + c2 % 2
        remote(src, dst.at[giver], ss.at[1, k], rs.at[1, k], (c2, f)).wait()
        if k:
            remote(src, dst.at[c], ss.at[0, k], rs.at[0, k], (c2, f)).wait_send()


def line_devices(place, lines):
    c, f, c2, m, n = place
    return [(lax.rem(c // 2 + k, lines) * 2 + c % 2, f) for k in range(1, lines)] + [(c2, f)]


def gates(gate, up, g_act):
    sg = jax.nn.sigmoid(gate)
    silu = gate * sg
    act = (silu * up).astype(bf16)
    g_gate = (g_act * up * (sg * (1.0 + gate * (1.0 - sg)))).astype(bf16)
    g_up = (g_act * silu).astype(bf16)
    return act, g_gate, g_up


class Spread:
    def __init__(self, place, lines, x, group, into, sems):
        self.place, self.lines, self.x, self.group, self.into = place, lines, x, group, into
        self.half = x.shape[0] // 2
        self.core = place[1] % 2
        self.line_s, self.line_r, self.pair_s, self.pair_r, self.y_s, self.y_r, self.mate_s, self.mate_r, self.own = sems

    def at(self, k):
        return lax.rem(self.place[0] // 2 + self.lines - k, self.lines)

    def each(self, first, act):
        pl.loop(first, self.lines)(act)

    def source(self, way):
        n = self.place[4]
        rows = pl.ds((0 if way == 0 else 1) * self.half, self.half)
        return self.x.at[rows] if way < 2 else self.group.at[n, rows]

    def slot(self, way, side, k, core=None):
        return self.into[(0, 1, 3, 2)[way]][side].at[self.at(k), self.core if core is None else core]

    def line(self, way, k):
        c, f = self.place[:2]
        sems = self.line_s.at[way, k], self.line_r.at[way, k]
        device = (lax.rem(c // 2 + k, self.lines) * 2 + c % 2, f)
        return remote(self.source(way), self.slot(way, 0, 0), *sems, device)

    def arrived(self, way, k):
        here = self.slot(way, 0, k)
        c, f, c2 = self.place[:3]
        return remote(here, here, self.line_s.at[way, k], self.line_r.at[way, k], (c2, f))

    def pair(self, way, k):
        c, f, c2 = self.place[:3]
        src = self.source(way) if isinstance(k, int) and k == 0 else self.slot(way, 0, k)
        return remote(src, self.slot(way, 1, k), self.pair_s.at[way, k], self.pair_r.at[way, k], (c2, f))

    def across(self, side, k):
        c, n = self.place[0], self.place[4]
        sems = self.y_s.at[side, k], self.y_r.at[side, k]
        return remote(self.slot(0, side, k), self.slot(3, side, k), *sems, (c, n))

    def hand(self, way, side, k, core=None):
        c, m = self.place[0], self.place[3]
        here = self.slot(way, side, k, core)
        return remote(here, here, self.mate_s.at[way, side, k], self.mate_r.at[way, side, k], (c, m))

    def lines_out(self, way):
        self.each(1, lambda k: self.line(way, k).start())

    def on_line(self, way, forward):
        def act(k):
            self.arrived(way, k).wait_recv()
            if forward:
                self.pair(way, k).start()
            self.hand(way, 0, k).start()

        if forward:
            self.pair(way, 0).start()
        self.each(1, act)

    def pairs_out(self, way):
        self.pair(way, 0).start()
        self.each(1, lambda k: self.pair(way, k).start())

    def on_pair(self, way):
        def act(k):
            self.pair(way, k).wait_recv()
            self.hand(way, 1, k).start()

        self.each(0, act)

    def cross(self, side):
        self.each(1 - side, lambda k: self.across(side, k).start())

    def on_y(self, side):
        def act(k):
            self.across(side, k).wait_recv()
            self.hand(3, side, k).start()

        self.each(1 - side, act)

    def keep(self, group, *parts):
        c, f = self.place[:2]
        copies = []
        for part in parts:
            pair = pl.ds((f // 2 if part < 2 else 1 - f // 2) * 2, 2)
            rows = pl.ds(part % 2 * self.half, self.half)
            into = self.into[part][0].at[c // 2]
            copies.append(pltpu.make_async_copy(group.at[pair, rows], into, self.own.at[part]))
        return copies

    def handed(self, way, side):
        def act(k):
            self.hand(way, side, k).wait_send()
            self.hand(way, side, k, 1 - self.core).wait_recv()

        self.each(1 - side, act)

    def finish_line(self, way):
        self.each(1, lambda k: self.line(way, k).wait_send())
        self.handed(way, 0)

    def finish_pair(self, way):
        self.each(0, lambda k: self.pair(way, k).wait_send())
        self.handed(way, 1)

    def finish_cross(self):
        for side in range(2):
            self.each(1 - side, lambda k: self.across(side, k).wait_send())
            self.handed(3, side)


def spread_sems(lines):
    dma = pltpu.SemaphoreType.DMA
    return [dma(shape) for shape in ((3, lines), (3, lines), (2, lines), (4, 2, lines)) for _ in range(2)] + [dma((4,))]


def mid_body(
    lines, ready, x, cot, own_cot, a0, a1, b0, hid, wg_h, wu_h, wd_h,
    gn_o, block_o, xg, b1_o, fb0_o, xa0_o, xa1_o,
    wg, wu, wd, act, back, near, sums, far_in, ws, ss, rs, ns, nr, *sems
):
    place = where_am_i()
    c, f, c2, m, n = place
    far = (m + 2) % 4
    tok, width = x.shape
    loads = [
        pltpu.make_async_copy(src, dst, ws.at[j])
        for j, (src, dst) in enumerate(((wg_h, wg), (wu_h, wu), (wd_h, wd)))
    ]
    for copy in loads:
        copy.start()
    greet(line_devices(place, lines) + [(c, m), (c, n)])
    ready()
    half = tok // 2
    own = remote(x, xg.at[f], ss.at[0], rs.at[0], (c, m))
    own.start()
    for j in range(2):
        rows = pl.ds(j * half, half)
        remote(x.at[rows], xg.at[f, rows], ss.at[1 + j], rs.at[1 + j], (c, n)).start()
    rest = Spread(place, lines, own_cot, cot, ((a0, a1), (b0, b1_o), None, (fb0_o,)), sems[:9])
    spread = Spread(place, lines, x, xg, ((xa0_o, xa1_o),), sems[9:])
    rest.pairs_out(1)
    spread.lines_out(0)
    kept = rest.keep(cot, 3)
    for copy in kept:
        copy.start()
    xg[f] = x[...]
    for copy in loads:
        copy.wait()
    own.wait()

    def forward(pair):
        at = pl.ds(pair * 2, 2)
        xs = xg[at].reshape(2 * tok, width)
        cs = cot[at].reshape(2 * tok, width)
        parts = gates(over_last(xs, wg[...]), over_last(xs, wu[...]), over_last(cs, wd[...]))
        for j, part in enumerate(parts):
            act[j] = part

    def backward():
        return plain_dot(act[1], wg[...]) + plain_dot(act[2], wu[...])

    def down():
        return plain_dot(act[0], wd[...])

    y = f // 2
    core = f % 2

    def swap(j):
        return remote(near.at[2 * j], near.at[2 * j + 1], ns.at[j], nr.at[j], (c, m))

    def give(j, value):
        back[...] = value.reshape(2, tok, width)
        near[2 * j] = back[1 - core].astype(bf16)
        swap(j).start()

    def cross(j):
        return remote(sums.at[j], far_in.at[j], ns.at[4 + j], nr.at[4 + j], (c, n))

    def send_over(j, j_swap):
        swap(j_swap).wait()
        sums[j] = (back[core] + near[2 * j_swap + 1].astype(f32)).astype(bf16)
        cross(j).start()

    forward(y)
    for j in range(2):
        here = xg.at[n, pl.ds(j * half, half)]
        remote(here, here, ss.at[1 + j], rs.at[1 + j], (c, n)).wait_recv()
        remote(here, here, ss.at[3 + j], rs.at[3 + j], (c, m)).start()
    rest.lines_out(2)
    give(0, backward())
    gn_o[...] = back[core]
    give(1, down())
    down_own = hid[...] + back[core]
    for j in range(2):
        rows = pl.ds(j * half, half)
        remote(x.at[rows], xg.at[far, rows], ss.at[3 + j], rs.at[3 + j], (c, m)).wait_recv()
    kept += spread.keep(xg, 0)
    kept[-1].start()
    forward(1 - y)
    give(2, backward())
    send_over(0, 2)
    spread.on_line(0, True)
    give(3, down())
    send_over(1, 3)
    rest.on_pair(1)
    cross(0).wait()
    swap(0).wait()
    gn_o[...] += near[1].astype(f32) + far_in[0].astype(f32)
    cross(1).wait()
    swap(1).wait()
    block_o[...] = (down_own + near[3].astype(f32) + far_in[1].astype(f32)).astype(bf16)
    rest.on_line(2, False)
    spread.on_pair(0)
    for j in range(2):
        rows = pl.ds(j * half, half)
        remote(x.at[rows], xg.at[f, rows], ss.at[1 + j], rs.at[1 + j], (c, n)).wait_send()
        remote(x.at[rows], xg.at[far, rows], ss.at[3 + j], rs.at[3 + j], (c, m)).wait_send()
    for copy in kept:
        copy.wait()
    rest.finish_pair(1)
    rest.finish_line(2)
    spread.finish_line(0)
    spread.finish_pair(0)


def turn(values, cos, sin, size):
    half = size // 2
    pieces = []
    for at in range(0, values.shape[0], size):
        lead, trail = values[at : at + half], values[at + half : at + size]
        pieces += [lead * cos - trail * sin, trail * cos + lead * sin]
    return jnp.concatenate(pieces, 0)


def key_bias(first, count, c, pos):
    tok = pos.shape[1]
    keys = lax.broadcasted_iota(jnp.int32, (count, tok), 0) + first
    queries = lax.broadcasted_iota(jnp.int32, (count, tok), 1) + c * tok
    allowed = (keys <= queries) & (keys >= queries - pos[...])
    return jnp.where(allowed, 0.0, MASK_FILL)


def front_body(
    lines, step, ready,
    inp, cot, v0, v1, v2, v3, v4, pos, cos_r, sin_r, wq, wk, wv, wo,
    wp_o, wo_o, gains_o, n1_o, q_o, kv_o, cot_o, att_o, lse_o, hid_o, n2_o, a0_o, a1_o, b0_o,
    kv, small, small_g, ms, mr, gs, gr, ks, kr, ts, tr, *sems
):
    place = where_am_i()
    c, f, c2, m, n = place
    far = (m + 2) % 4
    greet(line_devices(place, lines) + [(c, m), (c, n), (c, far)])
    tok, width = inp.shape
    depth, query_width = wq.shape
    key_width = wk.shape[1]
    group = H // KV
    scale = HD ** (-0.5)

    def rows(g):
        return pl.ds(pl.multiple_of(g * depth, 16), depth)

    project = [
        (wq, lambda g: wp_o.at[rows(g), pl.ds(0, query_width)]),
        (wk, lambda g: wp_o.at[rows(g), pl.ds(query_width, key_width)]),
        (wv, lambda g: wp_o.at[rows(g), pl.ds(query_width + key_width, key_width)]),
    ]
    output = [(wo, lambda g: wo_o.at[rows(g)])]
    gather_start(project, gs.at[pl.ds(0, 3)], gr.at[pl.ds(0, 3)], place)
    ready()
    small[...] = jnp.zeros_like(small)
    for k, v in enumerate((v0, v1, v2, v3, v4)):
        small[k : k + 1, : v.shape[0]] = v[...].astype(f32).reshape(1, v.shape[0])
    smalls = [remote(small, small_g.at[f], ms.at[k], mr.at[k], (c, g)) for k, g in enumerate((m, n, far))]
    for copy in smalls:
        copy.start()
    spread = Spread(place, lines, cot, cot_o, ((a0_o, a1_o), (b0_o,)), sems)
    spread.lines_out(0)
    values = inp[...].astype(f32)
    unit = values * lax.rsqrt(jnp.mean(values * values, -1, keepdims=True) + EPSILON)
    small_g[f] = small[...]
    for k, g in enumerate((m, n, far)):
        remote(small, small_g.at[g], ms.at[k], mr.at[k], (c, g)).wait()

    def vector(row, size):
        return jnp.concatenate([small_g[g, row : row + 1, :size] for g in range(4)], 1)

    gains_o[0:1] = vector(0, depth)
    gains_o[1:2] = vector(1, depth)
    bias = jnp.concatenate([vector(2, depth), vector(3, key_width // 4), vector(4, key_width // 4)], 1)
    normed = unit * gains_o[0:1]
    n1_o[...] = normed.T.astype(bf16)
    gather_start(output, gs.at[pl.ds(3, 1)], gr.at[pl.ds(3, 1)], place)
    gather_finish(project, gs.at[pl.ds(0, 3)], gr.at[pl.ds(0, 3)], place)
    projected = plain_dot(normed.astype(bf16), wp_o[...]) + bias
    cos, sin = cos_r[...], sin_r[...]
    keys = turn(projected[:, query_width : query_width + key_width].T, cos, sin, HD)
    kv[:, :key_width] = keys.T.astype(bf16)
    kv[:, key_width:] = projected[:, query_width + key_width :].astype(bf16)
    spread_start(kv, kv_o, ks, kr, place, lines)
    kv_o[c] = kv[...]
    q_o[...] = turn(projected[:, :query_width].T, cos, sin, HD).astype(bf16)
    items = [(cot, lambda g, at: cot_o.at[g, at])]
    tokens_start(items, ts, tr, place)
    gather_finish(output, gs.at[pl.ds(3, 1)], gr.at[pl.ds(3, 1)], place)
    spread_finish(kv, kv_o, ks, kr, place, lines)
    spread.lines_out(1)
    spread.on_line(0, True)
    for g in range(KV):
        queries = heads(q_o, g, group, HD)

        def visit(i, state):
            highest, total, acc = state
            at = pl.ds(i * step, step)
            both = kv_o[at].reshape(step * tok, 2 * key_width)
            seen = both[:, g * HD : (g + 1) * HD]
            carried = both[:, key_width + g * HD : key_width + (g + 1) * HD]
            mask = key_bias(i * step * tok, step * tok, c, pos)
            scores = plain_dot(seen, queries) * scale + jnp.concatenate([mask] * group, 1)
            top = jnp.maximum(highest, jnp.max(scores, 0, keepdims=True))
            exps = jnp.exp(scores - top)
            shrink = jnp.exp(highest - top)
            total = total * shrink + jnp.sum(exps, 0, keepdims=True)
            acc = acc * shrink + over_first(carried, exps.astype(bf16))
            return top, total, acc

        state = (
            jnp.full((1, group * tok), MASK_FILL, f32),
            jnp.zeros((1, group * tok), f32),
            jnp.zeros((HD, group * tok), f32),
        )
        blocks = kv_o.shape[0] // step
        if blocks <= 2:
            for i in range(blocks):
                state = visit(i, state)
        else:
            state = lax.fori_loop(0, blocks, visit, state)
        highest, total, acc = state
        attention = acc / total
        logs = highest + jnp.log(total)
        for j in range(group):
            at = slice(j * tok, (j + 1) * tok)
            h = g * group + j
            att_o[h * HD : (h + 1) * HD] = attention[:, at]
            lse_o[h] = logs[:, at]
    hidden = values + plain_dot(att_o[...].T.astype(bf16), wo_o[...])
    hid_o[...] = hidden
    inverse = lax.rsqrt(jnp.mean(hidden * hidden, -1, keepdims=True) + EPSILON)
    n2_o[...] = (hidden * inverse * gains_o[1:2]).astype(bf16)
    tokens_finish(items, ts, tr, place)
    kept = spread.keep(cot_o, 0, 1)
    for copy in kept:
        copy.start()
    spread.on_pair(0)
    spread.on_line(1, False)
    spread.finish_line(0)
    spread.finish_pair(0)
    spread.finish_line(1)
    for copy in kept:
        copy.wait()


def heads(ref, g, group, size):
    return jnp.concatenate([ref[pl.ds((g * group + j) * size, size)] for j in range(group)], 1)


def turn_back(grads, cos, sin, size):
    half = size // 2
    pieces = []
    for at in range(0, grads.shape[0], size):
        lead, trail = grads[at : at + half], grads[at + half : at + size]
        pieces += [lead * cos + trail * sin, trail * cos - lead * sin]
    return jnp.concatenate(pieces, 0)


def norm_grad(values, gain, grads):
    inverse = lax.rsqrt(jnp.mean(values * values, -1, keepdims=True) + EPSILON)
    scaled = values * inverse
    weighted = grads * gain
    back = inverse * (weighted - scaled * jnp.mean(weighted * scaled, -1, keepdims=True))
    return back, jnp.sum(grads * scaled, 0, keepdims=True)


class Total:
    def __init__(self, place, lines, low, wide, rest, pay, total, bufs, ss, rs):
        self.place, self.lines, self.pay, self.total = place, lines, pay, total
        self.a_in, self.a_sum, self.a_line, self.b_line, self.b_sum, self.b_in = bufs
        self.ss, self.rs = ss, rs
        self.p, self.x = place[0] // 2, place[0] % 2
        self.height = pay.shape[0] // (2 * lines)
        self.a, self.b = pl.ds(low, wide), pl.ds(low + wide, rest)

    def rows(self, first, count=1):
        return pl.ds(pl.multiple_of(first * self.height, 16), count * self.height)

    def ahead(self, k):
        return lax.rem(self.p + k, self.lines)

    def to_pair(self, way, stage, src, dst):
        c, f, c2 = self.place[:3]
        return remote(src, dst, self.ss.at[way, stage, 0], self.rs.at[way, stage, 0], (c2, f))

    def to_line(self, way, stage, k, src, dst):
        f = self.place[1]
        device = (self.ahead(k) * 2 + self.x, f)
        return remote(src, dst, self.ss.at[way, stage, k], self.rs.at[way, stage, k], device)

    def copies(self, way, stage):
        pay, total, p, x, n = self.pay, self.total, self.p, self.x, self.lines
        every = range(1, n)
        if way == 0:
            own = total.at[self.rows(x * n + p), self.a]
            group = total.at[self.rows(x * n, n), self.a]
            if stage == 0:
                return [self.to_pair(0, 0, pay.at[self.rows((1 - x) * n, n), self.a], self.a_in)]
            if stage == 1:
                return [
                    self.to_line(0, 1, k, self.a_sum.at[self.rows(self.ahead(k))], self.a_line.at[k - 1]) for k in every
                ]
            if stage == 2:
                return [self.to_line(0, 2, k, own, own) for k in every]
            return [self.to_pair(0, 3, group, group)]
        own = total.at[self.rows(p * 2 + x), self.b]
        both = total.at[self.rows(p * 2, 2), self.b]
        if stage == 0:
            return [
                self.to_line(1, 0, k, pay.at[self.rows(self.ahead(k) * 2, 2), self.b], self.b_line.at[k - 1])
                for k in every
            ]
        if stage == 1:
            return [self.to_pair(1, 1, self.b_sum.at[self.rows(1 - x)], self.b_in)]
        if stage == 2:
            return [self.to_pair(1, 2, own, own)]
        return [self.to_line(1, 3, k, both, both) for k in every]

    def start(self, stage):
        for way in range(2):
            for copy in self.copies(way, stage):
                copy.start()

    def wait(self, stage):
        pay, total, p, x, n = self.pay, self.total, self.p, self.x, self.lines
        for way in range(2):
            for copy in self.copies(way, stage):
                copy.wait()
        if stage == 0:
            value = pay[self.rows(x * n, n), self.a].astype(f32) + self.a_in[...].astype(f32)
            self.a_sum[...] = value.astype(bf16)
            value = pay[self.rows(p * 2, 2), self.b].astype(f32)
            for k in range(1, n):
                value = value + self.b_line[k - 1].astype(f32)
            self.b_sum[...] = value.astype(bf16)
        if stage == 1:
            value = self.a_sum[self.rows(p)].astype(f32)
            for k in range(1, n):
                value = value + self.a_line[k - 1].astype(f32)
            total[self.rows(x * n + p), self.a] = value.astype(bf16)
            value = self.b_sum[self.rows(x)].astype(f32) + self.b_in[...].astype(f32)
            total[self.rows(p * 2 + x), self.b] = value.astype(bf16)


def sum_buffers(lines, tall, wide, rest):
    height = tall // (2 * lines)
    shapes = (
        (lines * height, wide), (lines * height, wide), (lines - 1, height, wide),
        (lines - 1, 2 * height, rest), (2 * height, rest), (height, rest),
    )
    return [pltpu.VMEM(shape, bf16) for shape in shapes]


def back_body(
    ctx, step, block, chunk, ready,
    gn, hid, gains, cot, wo, att_t, q_t, kv, pos, lse, cos_r, sin_r, n1_t, inp, wp, n2, n2_g,
    cot_g, cot_a0, cot_a1, cot_b0, cot_b1, cot_fb0, x_a0, x_a1, wg_h, wu_h, wd_h,
    inp_o, grads_o, acc_g, acc_u, acc_d, x_b0, x_b1, x_fa0, x_fa1, x_fb0, x_fb1, cot_fa0, cot_fa1, cot_fb1,
    gh, do_t, part, dq, held, ghl, ghl_g, low_t, n1_g, low_g, gp, gp_g, vec, vec_g,
    pay, total_r, p0, p1, p2, p3, p4, p5, q0, q1, q2, q3, q4, q5,
    xs, cs, wg, wu, wd, acc,
    ks, kr, ts, tr, as_, ar, vs, vr, sum_s, sum_r, ws, ins, outs, *sems
):
    place = where_am_i()
    c, f, c2, m, n = place
    far = (m + 2) % 4
    peers = [lax.rem(c + k, ctx) for k in range(1, ctx)]
    greet([(p, f) for p in peers] + [(c, m), (c, n), (c, far)])
    tok, width = cot.shape
    group = H // KV
    depth = n1_g.shape[1]
    scale = HD ** (-0.5)

    def rows(g):
        return pl.ds(pl.multiple_of(g * depth, 16), depth)

    def swaps():
        return [
            remote(src.at[rows(g)], dst.at[f], as_.at[j, k], ar.at[j, k], (c, g))
            for j, (src, dst) in enumerate(((n1_t, n1_g), (low_t, low_g)))
            for k, g in enumerate((n, far, m))
        ]

    ready()
    spread = Spread(place, ctx // 2, n2, n2_g, ((x_a0, x_a1), (x_b0, x_b1), (x_fa0, x_fa1), (x_fb0, x_fb1)), sems[:9])
    rest = Spread(
        place, ctx // 2, cot, cot_g, ((cot_a0, cot_a1), None, (cot_fa0, cot_fa1), (cot_fb0, cot_fb1)), sems[9:]
    )
    rest.pairs_out(2)
    spread.lines_out(1)
    rest.cross(0)
    rest.cross(1)
    kept = spread.keep(n2_g, 1, 2, 3) + rest.keep(cot_g, 2)
    loads = [
        pltpu.make_async_copy(src, dst, ws.at[j])
        for j, (src, dst) in enumerate(((wg_h, wg), (wu_h, wu), (wd_h, wd)))
    ]
    for copy in kept + loads:
        copy.start()
    low_t[...] = att_t[...].astype(bf16)
    back, gain_two = norm_grad(hid[...], gains[1:2], gn[...])
    gh[...] = cot[...].astype(f32) + back
    ghl[...] = gh[...].astype(bf16)
    items = [(ghl, lambda g, at: ghl_g.at[g, at])]
    tokens_start(items, ts.at[0], tr.at[0], place)
    for copy in swaps():
        copy.start()
    n1_g[f] = n1_t[rows(f)]
    low_g[f] = low_t[rows(f)]
    do_t[...] = over_last(wo[...], ghl[...]).astype(bf16)
    key_width = KV * HD
    for g in range(KV):
        queries, grads = heads(q_t, g, group, HD), heads(do_t, g, group, HD)
        delta = jnp.sum(grads.astype(f32) * heads(att_t, g, group, HD), 0, keepdims=True)
        total = jnp.concatenate([lse[g * group + j] for j in range(group)], 1)

        @pl.loop(0, kv.shape[0] // step)
        def _(i):
            at = pl.ds(i * step, step)
            both = kv[at].reshape(step * tok, 2 * key_width)
            keys = both[:, g * HD : (g + 1) * HD]
            values = both[:, key_width + g * HD : key_width + (g + 1) * HD]
            bias = key_bias(i * step * tok, step * tok, c, pos)
            scores = plain_dot(keys, queries) * scale + jnp.concatenate([bias] * group, 1)
            probs = jnp.exp(scores - total)
            g_probs = plain_dot(values, grads)
            g_scores = (probs * (g_probs - delta)).astype(bf16)
            g_keys = over_last(g_scores, queries) * scale
            g_values = over_last(probs.astype(bf16), grads)
            part[at, :, g * HD : (g + 1) * HD] = g_keys.astype(bf16).reshape(step, tok, HD)
            part[at, :, key_width + g * HD : key_width + (g + 1) * HD] = g_values.astype(bf16).reshape(
                step, tok, HD
            )
            g_queries = over_first(keys, g_scores) * scale

            @pl.when(i == 0)
            def _():
                dq[g] = g_queries

            @pl.when(i > 0)
            def _():
                dq[g] += g_queries

    owners = [remote(part.at[p], held.at[k], ks.at[k], kr.at[k], (p, f)) for k, p in enumerate(peers)]
    for copy in owners:
        copy.start()
    tokens_finish(items, ts.at[0], tr.at[0], place)
    for copy in swaps():
        copy.wait()
    cos, sin = cos_r[...], sin_r[...]
    g_q = [
        turn_back(dq[g, :, j * tok : (j + 1) * tok], cos, sin, HD) for g in range(KV) for j in range(group)
    ]
    g_q = jnp.concatenate(g_q, 0)
    query_width = g_q.shape[0]
    gp[:, :query_width] = g_q.T.astype(bf16)
    columns = gp.shape[1]
    low_all = jnp.concatenate([low_g[g] for g in range(4)], 1)
    pay[pl.ds(0, depth), pl.ds(columns, width)] = plain_dot(low_all, ghl_g[...].reshape(4 * tok, width)).astype(
        bf16
    )
    pay[pl.ds(depth, pay.shape[0] - depth)] = jnp.zeros((pay.shape[0] - depth, pay.shape[1]), bf16)
    third = width // 7
    early = Total(
        place, ctx // 2, columns, 5 * third, 2 * third, pay, total_r, (p0, p1, p2, p3, p4, p5), sum_s.at[0], sum_r.at[0]
    )
    late = Total(
        place, ctx // 2, 0, 6 * third, 3 * third, pay, total_r, (q0, q1, q2, q3, q4, q5), sum_s.at[1], sum_r.at[1]
    )
    pairs = part[c].astype(f32)
    for k, copy in enumerate(owners):
        copy.wait()
        pairs = pairs + held[k].astype(f32)
    early.start(0)
    spread.lines_out(2)
    g_k = turn_back(pairs[:, :key_width].T, cos, sin, HD)
    gp[:, query_width : query_width + key_width] = g_k.T.astype(bf16)
    gp[:, query_width + key_width :] = pairs[:, key_width:].astype(bf16)
    items = [(gp, lambda g, at: gp_g.at[g, at])]
    tokens_start(items, ts.at[1], tr.at[1], place)
    spread.on_line(1, True)
    g_normed = over_last(gp[...], wp[...])
    values = inp[...].astype(f32)
    back, gain_one = norm_grad(values, gains[0:1], g_normed)
    inp_o[...] = (gh[...] + back).astype(bf16)
    vec[...] = jnp.zeros_like(vec)
    vec[0:1, :width] = gain_one
    vec[1:2, :width] = gain_two
    vec[2:3, :columns] = jnp.sum(gp[...].astype(f32), 0, keepdims=True)
    vectors = [remote(vec, vec_g.at[k], vs.at[k], vr.at[k], (c, g)) for k, g in enumerate((m, n, far))]
    for copy in vectors:
        copy.start()
    early.wait(0)
    early.start(1)
    tokens_finish(items, ts.at[1], tr.at[1], place)
    n1_all = jnp.concatenate([n1_g[g] for g in range(4)], 1)
    pay[pl.ds(0, depth), pl.ds(0, columns)] = plain_dot(n1_all, gp_g[...].reshape(4 * tok, columns)).astype(bf16)
    total = vec[...]
    for k, copy in enumerate(vectors):
        copy.wait()
        total = total + vec_g[k]
    pay[pl.ds(depth, 8), :columns] = total[:, :columns].astype(bf16)
    early.wait(1)
    early.start(2)
    late.start(0)
    spread.cross(0)
    spread.cross(1)
    for copy in loads:
        copy.wait()
    parts = (((x_a0, x_a1), (cot_a0, cot_a1)), ((x_b0, x_b1), (cot_b0, cot_b1)))
    blocks = wg.shape[0] // block
    per_part = ctx * tok // chunk
    for way, sides in enumerate(parts):
        if way == 1:
            spread.finish_line(1)
            kept[0].wait()
            spread.finish_pair(1)
        for i in range(per_part):
            count = chunk // tok // 2
            at = pl.ds(i * count, count)
            fetch = [
                pltpu.make_async_copy(sides[j][side].at[at], into.at[side], ins.at[j, side])
                for j, into in enumerate((xs, cs))
                for side in range(2)
            ]
            for copy in fetch:
                copy.start()
            for copy in fetch:
                copy.wait()
            tokens = xs[...].reshape(chunk, width), cs[...].reshape(chunk, width)
            first = way == 0 and i == 0
            last = way == 1 and i == per_part - 1

            @pl.loop(0, blocks)
            def _(b):
                at = pl.ds(pl.multiple_of(b * block, 16), block)
                act, g_gate, g_up = hidden_units(*tokens, wg[at], wu[at], wd[at])
                for j, (left, right) in enumerate(((g_gate, 0), (g_up, 0), (act, 1))):
                    value = plain_dot(left, tokens[right])
                    if first:
                        acc[j, at] = value
                    else:
                        acc[j, at] += value
                if first:

                    @pl.when(b == 0)
                    def _():
                        early.wait(2)
                        early.start(3)
                        rest.on_y(0)
                        rest.on_y(1)

                    @pl.when(b == 1)
                    def _():
                        late.wait(0)
                        late.start(1)

                    @pl.when(b == 2)
                    def _():
                        early.wait(3)
                        rest.on_pair(2)
                        spread.on_line(2, True)

                    @pl.when(b == 3)
                    def _():
                        late.wait(1)
                        late.start(2)

                if way == 0 and i == 0:

                    @pl.when(b == 2)
                    def _():
                        spread.on_pair(1)

                if way == 1 and i == 0:

                    @pl.when(b == 0)
                    def _():
                        spread.on_y(0)

                    @pl.when(b == 1)
                    def _():
                        late.wait(2)
                        late.start(3)
                        spread.on_y(1)

                    @pl.when(b == 3)
                    def _():
                        spread.on_pair(2)

                if last:
                    for j, out in enumerate((acc_g, acc_u, acc_d)):
                        pltpu.make_async_copy(acc.at[j, at], out.at[at], outs.at[b, j]).start()

    late.wait(3)
    grads_o[...] = total_r[...].astype(f32)
    spread.finish_line(2)
    spread.finish_pair(2)
    spread.finish_cross()
    rest.finish_pair(2)
    rest.finish_cross()
    for b in range(blocks):
        at = pl.ds(b * block, block)
        for j, out in enumerate((acc_g, acc_u, acc_d)):
            pltpu.make_async_copy(acc.at[j, at], out.at[at], outs.at[b, j]).wait()
    for copy in kept[1:]:
        copy.wait()


def over_last(a, b):
    return lax.dot_general(a, b, (((1,), (1,)), ((), ())), preferred_element_type=f32)


def over_first(a, b):
    return lax.dot_general(a, b, (((0,), (0,)), ((), ())), preferred_element_type=f32)


def plain_dot(a, b):
    return jnp.dot(a, b, preferred_element_type=f32)


def hidden_units(x, cot, wg, wu, wd):
    return gates(over_last(wg, x), over_last(wu, x), over_last(wd, cot))


def hidden_body(
    chunk, block, windows, x0_h, x1_h, x2_h, x3_h, c0_h, c1_h, c2_h, c3_h, wg_h, wu_h, wd_h, ig_h, iu_h, id_h, *refs
):
    passed, refs = refs[:4], refs[4:]
    og_h, ou_h, od_h = refs[:3]
    results_out, refs = refs[3 : 3 + len(windows)], refs[3 + len(windows) :]
    xs, cs, wg, wu, wd, acc, in_sem, w_sem, out_sem, init_sem, pass_sem = refs[:11]
    through = []
    for j, (which, at) in enumerate(windows):
        src = passed[which] if at is None else passed[which].at[at]
        buffer = refs[11 + j]
        through.append(
            (
                pltpu.make_async_copy(src, buffer, pass_sem.at[0, j]),
                pltpu.make_async_copy(buffer, results_out[j], pass_sem.at[1, j]),
            )
        )
    parts = (((x0_h, x1_h), (c0_h, c1_h)), ((x2_h, x3_h), (c2_h, c3_h)))
    rows = 4 * x0_h.shape[0]
    steps, blocks, held = rows // chunk, wg.shape[0] // block, xs.shape[0] // chunk
    def weights(b):
        at = pl.ds(b * block, block)
        return [
            pltpu.make_async_copy(src.at[at], dst.at[at], w_sem.at[b, j])
            for j, (src, dst) in enumerate(((wg_h, wg), (wu_h, wu), (wd_h, wd)))
        ]

    def fetch(i, begin, part):
        half = chunk // 2
        src = pl.ds(pl.multiple_of(begin * half, half), half)
        slot = i % held
        return [
            pltpu.make_async_copy(
                part[j][side].at[src],
                into.at[pl.ds(pl.multiple_of(slot * chunk + side * half, half), half)],
                in_sem.at[slot, j, side],
            )
            for j, into in enumerate((xs, cs))
            for side in range(2)
        ]

    def start_tokens(i):
        begin = 0
        for part in parts:
            count = 2 * x0_h.shape[0] // chunk

            def go(begin=begin, part=part):
                for copy in fetch(i, i - begin, part):
                    copy.start()

            if isinstance(i, int):
                if begin <= i < begin + count:
                    go()
            else:
                pl.when((i >= begin) & (i < begin + count))(go)
            begin += count

    def wait_tokens(i):
        for copy in fetch(i, 0, parts[0]):
            copy.wait()

    def results(b, slot):
        at = pl.ds(pl.multiple_of(b * block, 16), block)
        return [
            pltpu.make_async_copy(acc.at[slot, j], out.at[at], out_sem.at[slot, j])
            for j, out in enumerate((og_h, ou_h, od_h))
        ]

    def initial(b, slot):
        at = pl.ds(pl.multiple_of(b * block, 16), block)
        return [
            pltpu.make_async_copy(src.at[at], acc.at[slot, j], init_sem.at[slot, j])
            for j, src in enumerate((ig_h, iu_h, id_h))
        ]

    resident = held == steps
    slots = acc.shape[0]
    start_tokens(0)
    for copy in weights(0):
        copy.start()
    for copy in weights(0):
        copy.wait()
    for copy in initial(0, 0):
        copy.start()
    for i in range(1, held if resident else 1):
        start_tokens(i)
    for b in range(1, slots):
        for copy in weights(b) + initial(b, b):
            copy.start()
    for copy, _ in through:
        copy.start()

    @pl.loop(0, blocks)
    def _(b):
        slot = b % slots
        at = pl.ds(pl.multiple_of(b * block, 16), block)

        @pl.when(b == 1)
        def _():
            for copy in weights(1):
                copy.wait()
            for into, out in through:
                into.wait()
                out.start()

        @pl.loop(0, steps)
        def _(i):
            if resident:

                @pl.when(b == 0)
                def _():
                    wait_tokens(i)

            else:
                wait_tokens(i)

                @pl.when((i + 1 < steps) | (b + 1 < blocks))
                def _():
                    start_tokens(lax.rem(i + 1, steps))

            t = pl.ds(pl.multiple_of(i % held * chunk, chunk), chunk)
            x, cot = xs[t], cs[t]
            act, g_gate, g_up = hidden_units(x, cot, wg[at], wu[at], wd[at])

            @pl.when(i == 0)
            def _():
                for copy in initial(b, slot):
                    copy.wait()

            acc[slot, 0] += plain_dot(g_gate, x)
            acc[slot, 1] += plain_dot(g_up, x)
            acc[slot, 2] += plain_dot(act, cot)

        for copy in results(b, slot):
            copy.start()

    for b in range(max(0, blocks - slots), blocks):
        for copy in results(b, b % slots):
            copy.wait()
    for _, out in through:
        out.wait()


def hidden_grads(xs, cots, wg, wu, wd, initial, passed, windows):
    width = wg.shape[1]
    xs, cots = [[part.reshape(-1, width) for part in parts] for parts in (xs, cots)]
    rows = sum(part.shape[0] for part in xs)
    units = wg.shape[0]
    chunk = math.gcd(rows // 2, 1024)
    block = units // 2
    held = min(rows // chunk, 4)
    any_spec = pl.BlockSpec(memory_space=pl.ANY)
    dma = pltpu.SemaphoreType.DMA
    return pl.pallas_call(
        functools.partial(hidden_body, chunk, block, [window[:2] for window in windows]),
        out_shape=(jax.ShapeDtypeStruct((units, width), f32),) * 3
        + tuple(jax.ShapeDtypeStruct(shape, dtype) for _, _, shape, dtype in windows),
        in_specs=[any_spec] * 18,
        out_specs=(any_spec,) * (3 + len(windows)),
        scratch_shapes=[pltpu.VMEM((held * chunk, width), bf16)] * 2
        + [pltpu.VMEM((units, width), bf16)] * 3
        + [pltpu.VMEM((2, 3, block, width), f32), dma((held, 2, 2)), dma((2, 3)), dma((2, 3)), dma((2, 3))]
        + [dma((2, len(windows)))]
        + [pltpu.VMEM(shape, dtype) for _, _, shape, dtype in windows],
        compiler_params=pltpu.CompilerParams(vmem_limit_bytes=62 << 20),
        cost_estimate=pl.CostEstimate(
            flops=12 * rows * width * units, bytes_accessed=4 * rows * width + 18 * units * width, transcendentals=0
        ),
        name="hidden_grads",
    )(*xs, *cots, wg, wu, wd, *initial, *passed)


def shards(
    layer_input,
    seq_ids,
    positions,
    norm_gain,
    w_query,
    b_query,
    w_key,
    b_key,
    w_value,
    b_value,
    w_output,
    mlp_gain,
    w_gate,
    w_up,
    w_down,
    cotangent,
):
    tok = layer_input.shape[1]
    width = layer_input.shape[2]
    group = H // KV
    query_width = H * HD
    key_width = KV * HD
    score_scale = HD ** (-0.5)
    ctx = lax.axis_size("ctx")
    fsdp = lax.axis_size("fsdp")
    depth = width // fsdp
    lines = ctx // 2
    c, f = lax.axis_index("ctx"), lax.axis_index("fsdp")
    seq_length = ctx * tok
    dma = pltpu.SemaphoreType.DMA
    sds = jax.ShapeDtypeStruct
    input_rows = layer_input[0]
    grad_out = cotangent[0]
    own_segment = seq_ids[0]
    own_positions = positions[0]
    query_rows = c * tok + jnp.arange(tok, dtype=jnp.int32)

    cosine, sine_table = rope_tables(own_positions, HD)
    own_positions = own_positions[None]
    step = math.gcd(ctx, 4)
    columns = query_width + 2 * key_width
    hbm = pl.BlockSpec(memory_space=pltpu.HBM)
    half_blocks = sds((lines, 2, tok // 2, width), bf16)
    (w_project, wo_full, gains, n1_t, q_t, kv_all, cot_group, att_t, log_total, hidden_state, normed_second,
     cot_a0, cot_a1, cot_b0) = (
        staged_call(
            functools.partial(front_body, lines, step),
            (
                input_rows, grad_out, norm_gain, mlp_gain, b_query, b_key, b_value, own_positions, cosine, sine_table,
                w_query, w_key, w_value, w_output,
            ),
            (10, 11, 12, 13),
            (
                sds((width, columns), bf16),
                sds((query_width, width), bf16),
                sds((8, width), f32),
                sds((width, tok), bf16),
                sds((query_width, tok), bf16),
                sds((ctx, tok, 2 * key_width), bf16),
                sds((fsdp, tok, width), bf16),
                sds((query_width, tok), f32),
                sds((H, 1, tok), f32),
                sds((tok, width), f32),
                sds((tok, width), bf16),
                half_blocks,
                half_blocks,
                half_blocks,
            ),
            (11, 12, 13),
            [
                pltpu.VMEM((tok, 2 * key_width), bf16),
                pltpu.VMEM((8, 256), f32),
                pltpu.VMEM((fsdp, 8, 256), f32),
                dma((3,)),
                dma((3,)),
            ]
            + gather_sems(4)
            + [dma((2, lines)), dma((2, lines))]
            + gather_sems(1)
            + spread_sems(lines),
            0,
            "front",
            pl.CostEstimate(flops=4 * 10**9, bytes_accessed=10**7, transcendentals=0),
        )
    )
    units = w_down.shape[0]
    wg_t, wu_t = w_gate.T, w_up.T
    grad_normed2, block_out, x_group, cot_b1, cot_fb0, x_a0, x_a1 = staged_call(
        functools.partial(mid_body, lines),
        (normed_second, cot_group, grad_out, cot_a0, cot_a1, cot_b0, hidden_state, wg_t, wu_t, w_down),
        (3, 4, 5, 7, 8, 9),
        (
            sds((tok, width), f32),
            sds((tok, width), bf16),
            sds((fsdp, tok, width), bf16),
        )
        + (half_blocks,) * 4,
        (3, 4, 5, 6),
        [pltpu.VMEM((units, width), bf16)] * 3
        + [
            pltpu.VMEM((3, 2 * tok, units), bf16),
            pltpu.VMEM((2, tok, width), f32),
            pltpu.VMEM((8, tok, width), bf16),
            pltpu.VMEM((2, tok, width), bf16),
            pltpu.VMEM((2, tok, width), bf16),
            dma((3,)),
            dma((5,)),
            dma((5,)),
            dma((6,)),
            dma((6,)),
        ]
        + spread_sems(lines)
        + spread_sems(lines),
        2,
        "mid",
        pl.CostEstimate(
            flops=12 * fsdp * tok * width * units, bytes_accessed=6 * units * width, transcendentals=0
        ),
    )
    tall, everything = max(256, 16 * ctx), columns + width
    third = width // 7
    block = units // 4
    chunk = math.gcd(ctx * tok, 1024)
    big = sds((units, width), f32)
    (
        input_grad, weight_grads, acc_g, acc_u, acc_d, x_b0, x_b1, x_fa0, x_fa1, x_fb0, x_fb1, cot_fa0, cot_fa1,
        cot_fb1,
    ) = staged_call(
        functools.partial(back_body, ctx, step, block, chunk),
        (
            grad_normed2, hidden_state, gains, grad_out, wo_full, att_t, q_t, kv_all, own_positions, log_total,
            cosine, sine_table, n1_t, input_rows, w_project, normed_second, x_group, cot_group, cot_a0,
            cot_a1, cot_b0, cot_b1, cot_fb0, x_a0, x_a1, wg_t, wu_t, w_down,
        ),
        (18, 19, 20, 21, 22, 23, 24, 25, 26, 27),
        (sds((tok, width), bf16), sds((tall, everything), f32), big, big, big) + (half_blocks,) * 9,
        tuple(range(2, 14)),
        [
            pltpu.VMEM((tok, width), f32),
            pltpu.VMEM((query_width, tok), bf16),
            pltpu.VMEM((ctx, tok, 2 * key_width), bf16),
            pltpu.VMEM((KV, HD, group * tok), f32),
            pltpu.VMEM((ctx - 1, tok, 2 * key_width), bf16),
            pltpu.VMEM((tok, width), bf16),
            pltpu.VMEM((fsdp, tok, width), bf16),
            pltpu.VMEM((query_width, tok), bf16),
            pltpu.VMEM((fsdp, depth, tok), bf16),
            pltpu.VMEM((fsdp, depth, tok), bf16),
            pltpu.VMEM((tok, columns), bf16),
            pltpu.VMEM((fsdp, tok, columns), bf16),
            pltpu.VMEM((8, everything), f32),
            pltpu.VMEM((3, 8, everything), f32),
            pltpu.VMEM((tall, everything), bf16),
            pltpu.VMEM((tall, everything), bf16),
            *sum_buffers(lines, tall, 5 * third, 2 * third),
            *sum_buffers(lines, tall, 6 * third, 3 * third),
            pltpu.VMEM((2, chunk // tok // 2, 2, tok // 2, width), bf16),
            pltpu.VMEM((2, chunk // tok // 2, 2, tok // 2, width), bf16),
            pltpu.VMEM((units, width), bf16),
            pltpu.VMEM((units, width), bf16),
            pltpu.VMEM((units, width), bf16),
            pltpu.VMEM((3, units, width), f32),
            dma((ctx - 1,)),
            dma((ctx - 1,)),
            dma((2, 1, 6)),
            dma((2, 1, 6)),
            dma((2, 3)),
            dma((2, 3)),
            dma((3,)),
            dma((3,)),
            dma((2, 2, 4, lines)),
            dma((2, 2, 4, lines)),
            dma((3,)),
            dma((2, 2)),
            dma((4, 3)),
        ]
        + spread_sems(lines)
        + spread_sems(lines),
        3,
        "back",
        pl.CostEstimate(flops=4 * 10**10, bytes_accessed=6 * 10**7, transcendentals=0),
    )
    starts = ((0, 0, width), (1, 0, width), (2, 0, query_width), (2, query_width, key_width),
              (2, query_width + key_width, key_width))

    def piece(row, start, size):
        share = size // fsdp
        return lax.dynamic_slice_in_dim(weight_grads[depth + row], start + f * share, share, 0)

    own = [piece(*at) for at in starts]

    ends = (0, query_width, query_width + key_width, columns, columns + width)
    windows = [
        (0, (slice(0, depth), slice(ends[j], ends[j + 1])), (depth, ends[j + 1] - ends[j]), f32) for j in range(4)
    ]
    windows += [(1, None, (tok, width), bf16), (2, None, (tok, width), bf16), (3, None, (H, 1, tok), f32)]
    gate_grad, up_grad, down_grad, query_grad, key_grad, value_grad, output_grad, block_out, input_grad, lse = (
        hidden_grads(
            (x_fa0, x_fa1, x_fb0, x_fb1), (cot_fa0, cot_fa1, cot_fb0, cot_fb1), wg_t, wu_t, w_down,
            (acc_g, acc_u, acc_d), (weight_grads, block_out, input_grad, log_total), windows,
        )
    )
    return (
        block_out[None],
        input_grad[None],
        own[0],
        query_grad,
        own[2],
        key_grad,
        own[3],
        value_grad,
        own[4],
        output_grad,
        own[1],
        gate_grad.T,
        up_grad.T,
        down_grad,
        lse.transpose(1, 0, 2),
    )


def solution(mesh):
    in_specs = (
        P("fsdp", "ctx", None),
        P("fsdp", "ctx"),
        P("fsdp", "ctx"),
        P("fsdp"),
        P("fsdp", None),
        P("fsdp"),
        P("fsdp", None),
        P("fsdp"),
        P("fsdp", None),
        P("fsdp"),
        P("fsdp", None),
        P("fsdp"),
        P(None, "fsdp"),
        P(None, "fsdp"),
        P("fsdp", None),
        P("fsdp", "ctx", None),
    )
    out_specs = (
        P("fsdp", "ctx", None),
        P("fsdp", "ctx", None),
        P("fsdp"),
        P("fsdp", None),
        P("fsdp"),
        P("fsdp", None),
        P("fsdp"),
        P("fsdp", None),
        P("fsdp"),
        P("fsdp", None),
        P("fsdp"),
        P(None, "fsdp"),
        P(None, "fsdp"),
        P("fsdp", None),
        P("fsdp", None, "ctx"),
    )

    return jax.shard_map(shards, mesh=mesh, in_specs=in_specs, out_specs=out_specs, check_vma=False)
```
